32 devices in a mesh: dp: 8 (over y, x, core), tensor: 4 (over z).
Axes of the slice: x: 2, y: 2, z: 4, core: 2. Of those that a mesh axis runs over, the one named last changes fastest.
Arguments:
- tokens: bfloat16 [4096, 1536], P('dp', 'tensor'), may hold values from -6 to 6
- cotangent: bfloat16 [4096, 1536], P('dp', 'tensor'), may hold values from -6 to 6
- seq_lens: int32 [8, 3], P('dp'), may hold values from 0 to 384, as said below
- input_norm_gain: float32 [1536], replicated, may hold values from 0.5 to 1.5
- w_zx: bfloat16 [1536, 2, 3072], P(None, None, 'tensor'), may hold values from -0.15625 to 0.15625
- w_bc: bfloat16 [1536, 256], replicated, may hold values from -0.15625 to 0.15625
- w_dt: bfloat16 [1536, 48], P(None, 'tensor'), may hold values from -0.078125 to 0.078125
- conv_wx: float32 [4, 3072], P(None, 'tensor'), may hold values from -3 to 3
- conv_bx: float32 [3072], P('tensor'), may hold values from -3 to 3
- conv_wbc: float32 [4, 256], replicated, may hold values from -3 to 3
- conv_bbc: float32 [256], replicated, may hold values from -3 to 3
- a_log: float32 [48], P('tensor'), may hold values from 0 to 2.7
- dt_bias: float32 [48], P('tensor'), may hold values from -6 to -2
- d_skip: float32 [48], P('tensor'), may hold values from 0.5 to 1.5
- norm_gate: float32 [3072], P('tensor'), may hold values from 0.5 to 1.5
- w_out: bfloat16 [3072, 1536], P('tensor'), may hold values from -0.109375 to 0.109375
Outputs:
- block_out: bfloat16 [4096, 1536], P('dp', 'tensor')
- d_tokens: float32 [4096, 1536], P('dp', 'tensor')
- grad_zx: float32 [1536, 2, 3072], P('dp', None, 'tensor')
- grad_bc: float32 [1536, 256], P('dp')
- grad_dt: float32 [1536, 48], P('dp', 'tensor')
- grad_out: float32 [3072, 1536], P('tensor', 'dp')
- grad_conv_wx: float32 [4, 3072], P(None, 'tensor')
- grad_conv_bx: float32 [3072], P('tensor')
- grad_conv_wbc: float32 [4, 256], replicated
- grad_conv_bbc: float32 [256], replicated
- grad_a_log: float32 [48], P('tensor')
- grad_dt_bias: float32 [48], P('tensor')
- grad_d_skip: float32 [48], P('tensor')
- grad_gate: float32 [3072], P('tensor')
- grad_in: float32 [1536], P('tensor')
The draws below stay inside these ranges and needn't reach their ends.
Inputs may be any that keep to these rules, and one draw needn't show every extreme that they name: `seq_lens`: row d holds the lengths of the sequences packed in order from the first row of index d of dp; the rows after them are padding. Every row has exactly one length 384, its other lengths are at most 64, it sums to at most 512, and some row sums to exactly 512.
All inputs are finite; a program needn't handle non-finite values.
Results may differ from the reference program's by a relative error of at most 0.0076.
Values may be sent and summed in bfloat16 or wider, within the bound.
A program may use at most 192 MiB of HBM per device.

```python
from functools import partial
import jax
import jax.numpy as jnp
from jax import lax

D = 1536
H = 48
STATE = 128
CONV = 4
SCAN_BLOCK = 256
SEQ_DEV = 3
TOK_DEV = 512
INNER = 3072
MAXLEN = 384
TOKENS = 4096
N_DP = 8


def draw_seq_lens(key, part):
    key_long = jax.random.fold_in(key, 11)
    key_short = jax.random.fold_in(key, 23)
    key_full = jax.random.fold_in(key, 37)
    short_most = (TOK_DEV - MAXLEN) // (SEQ_DEV - 1)
    long_slot = jax.random.randint(key_long, (N_DP, 1), 0, SEQ_DEV)
    shorts = jax.random.randint(key_short, (N_DP, SEQ_DEV), 0, short_most + 1)
    full_device = jax.random.randint(key_full, (), 0, N_DP)
    device_ids = jnp.arange(N_DP)[:, None]
    shorts = jnp.where(device_ids == full_device, short_most, shorts)
    slot_ids = jnp.arange(SEQ_DEV)[None, :]
    return jnp.where(slot_ids == long_slot, MAXLEN, shorts).astype(jnp.int32)


def with_spikes(values, key, source, target, shards_of, factor):
    def block_of(axis_at):
        return (jnp.arange(values.shape[axis_at]) // (values.shape[axis_at] // shards_of)).reshape((-1,) + (1,) * (values.ndim - 1 - axis_at))

    one_side = jax.random.permutation(key, shards_of)[block_of(target)]
    other_side = (block_of(target) + shards_of // 2) % shards_of
    return jnp.where((block_of(source) == one_side) | (block_of(source) == other_side), factor * values, values)


def shard_levels(key, shape, split, smallest, top_value):
    loudness = 1.0
    for dim, parts in split:
        heights = jax.random.uniform(jax.random.fold_in(jax.random.fold_in(key, 6), dim), (parts,), jnp.float32, smallest / len(split), top_value / len(split))
        loudness = loudness * jnp.repeat(jnp.exp(heights), shape[dim] // parts).reshape((-1,) + (1,) * (len(shape) - 1 - dim))
    return loudness


def normal_values(key, shape, scale, most, cuts=(), held_as=jnp.bfloat16):
    values = jax.random.normal(key, shape, jnp.float32) * scale
    if len(cuts) > 0:
        values = shard_levels(key, shape, cuts, -0.22, 0.18) * values
    return jnp.clip(values, min=-most, max=most).astype(held_as)


def bell_draw_with(key, shape, deviation, limit, shards, heavy, kind=jnp.bfloat16):
    array = deviation * jax.random.normal(key, shape, jnp.float32)
    if shards:
        array = array * shard_levels(key, shape, shards, -0.22, 0.18)
    return jnp.clip(with_spikes(array, jax.random.fold_in(key, 3), *heavy), -limit, limit).astype(kind)


def setup_inputs(seed: int = 0) -> dict:
    arg_keys = jax.random.split(jax.random.key(seed), 17)
    tokens = bell_draw_with(arg_keys[0], (TOKENS, D), 1.0, 6.0, ((0, 8), (1, 4)), (0, 1, 8, 2.0))
    cotangent = bell_draw_with(arg_keys[1], (TOKENS, D), 1.0, 6.0, ((0, 8), (1, 4)), (0, 1, 8, 2.0))
    seq_lens = draw_seq_lens(jax.random.fold_in(arg_keys[16], 71), 0)
    input_norm_gain = jnp.clip(1.0 + 0.1 * jax.random.normal(arg_keys[3], (D,), jnp.float32), 0.5, 1.5)
    w_zx = normal_values(arg_keys[4], (D, 2, INNER), D ** -0.5, 0.15625, ((2, 4),))
    w_bc = normal_values(arg_keys[5], (D, 2 * STATE), D ** -0.5, 0.15625)
    w_dt = normal_values(arg_keys[6], (D, H), (4 * D) ** -0.5, 0.078125, ((1, 4),))
    conv_wx = normal_values(arg_keys[7], (CONV, INNER), CONV ** -0.5, 3.0, ((1, 4),), jnp.float32)
    conv_bx = normal_values(arg_keys[8], (INNER,), 0.5, 3.0, ((0, 4),), jnp.float32)
    conv_wbc = normal_values(arg_keys[9], (CONV, 2 * STATE), CONV ** -0.5, 3.0, (), jnp.float32)
    conv_bbc = normal_values(arg_keys[10], (2 * STATE,), 0.5, 3.0, (), jnp.float32)
    a_log = jnp.clip(2.7 * jax.random.uniform(arg_keys[11], (H,), jnp.float32) ** shard_levels(arg_keys[11], (H,), ((0, 4),), -0.2, 0.2), 0.0, 2.7)
    dt_bias = jnp.clip(-6.0 + 4.0 * jax.random.uniform(arg_keys[12], (H,), jnp.float32) ** shard_levels(arg_keys[12], (H,), ((0, 4),), -0.2, 0.2), -6.0, -2.0)
    d_skip = jnp.clip(0.5 + 1.0 * jax.random.uniform(arg_keys[13], (H,), jnp.float32) ** shard_levels(arg_keys[13], (H,), ((0, 4),), -0.2, 0.2), 0.5, 1.5)
    norm_gate = jnp.clip(1.0 + 0.1 * jax.random.normal(arg_keys[14], (INNER,), jnp.float32), 0.5, 1.5)
    w_out = normal_values(arg_keys[15], (INNER, D), INNER ** -0.5, 0.109375, ((0, 4),))
    return {"tokens": tokens, "cotangent": cotangent, "seq_lens": seq_lens, "input_norm_gain": input_norm_gain, "w_zx": w_zx, "w_bc": w_bc, "w_dt": w_dt, "conv_wx": conv_wx, "conv_bx": conv_bx, "conv_wbc": conv_wbc, "conv_bbc": conv_bbc, "a_log": a_log, "dt_bias": dt_bias, "d_skip": d_skip, "norm_gate": norm_gate, "w_out": w_out}


NORM_EPS = 1e-05
PRECISE = lax.Precision.HIGHEST

def contract_rows(first_op, second_op):
    return lax.dot_general(first_op, second_op, (((0,), (0,)), ((), ())), preferred_element_type=jnp.float32)

def contract_cols(first_op, second_op):
    return lax.dot_general(first_op, second_op, (((1,), (1,)), ((), ())), preferred_element_type=jnp.float32)

def segment_ids(lengths, row_count):
    seq_ends = jnp.cumsum(lengths.astype(jnp.int32))
    positions = jnp.arange(row_count, dtype=jnp.int32)
    return lax.optimization_barrier(jnp.sum((positions[:, None] >= seq_ends[None, :]).astype(jnp.int32), axis=1))

def causal_conv(signal, kernel_w, kernel_b, segment):
    kernel_len = kernel_w.shape[0]
    row_count = signal.shape[0]
    summed = kernel_b[None, :] + kernel_w[kernel_len - 1][None, :] * signal
    for lag_steps in range(1, kernel_len):
        shifted = jnp.concatenate([jnp.zeros((lag_steps, signal.shape[1]), jnp.float32), signal[:row_count - lag_steps]], axis=0)
        earlier = jnp.concatenate([jnp.full((lag_steps,), -1, jnp.int32), segment[:row_count - lag_steps]])
        same_seq = (earlier == segment).astype(signal.dtype)
        summed = summed + kernel_w[kernel_len - 1 - lag_steps][None, :] * shifted * same_seq[:, None]
    return summed

def ssd_scan(values, steps_dt, decay_rate, b_mat, c_mat, segment, block_len):
    row_count, heads_n, head_size = values.shape
    state_n = b_mat.shape[1]
    blocks_n = row_count // block_len
    log_decay = steps_dt * decay_rate[None, :]
    seg_lasts = segment[block_len - 1::block_len]
    prev_lasts = jnp.concatenate([jnp.full((1,), -1, jnp.int32), seg_lasts[:-1]])
    lower_tri = jnp.arange(block_len)[:, None] >= jnp.arange(block_len)[None, :]

    def blocked(source_arr):
        return source_arr.reshape((blocks_n, block_len) + source_arr.shape[1:])

    def one_block(carry_state, block_in):
        block_vals, block_decay, block_dt, block_b, block_c, block_seg, before_seg = block_in
        cumulated = jnp.cumsum(block_decay, axis=0)
        same_seq = ((block_seg[:, None] == block_seg[None, :]) & lower_tri)[:, :, None]
        log_gaps = cumulated[:, None, :] - cumulated[None, :, :]
        decays = jnp.where(same_seq, jnp.exp(jnp.where(same_seq, log_gaps, 0.0)), 0.0)
        scores = jnp.einsum('in,jn->ij', block_c, block_b, precision=PRECISE)
        mixing = decays * scores[:, :, None] * block_dt[None, :, :]
        intra_out = jnp.einsum('ijh,jhp->ihp', mixing, block_vals, precision=PRECISE)
        keep_in = (block_seg == before_seg).astype(block_vals.dtype)
        entering = jnp.exp(cumulated) * keep_in[:, None]
        inter_out = jnp.einsum('in,hnp->ihp', block_c, carry_state, precision=PRECISE) * entering[:, :, None]
        tail_in = (block_seg == block_seg[-1]).astype(block_vals.dtype)
        to_end = jnp.exp(cumulated[-1][None, :] - cumulated) * tail_in[:, None] * block_dt
        carried = carry_state * (jnp.exp(cumulated[-1]) * keep_in[-1])[:, None, None]
        new_state = carried + jnp.einsum('jh,jn,jhp->hnp', to_end, block_b, block_vals, precision=PRECISE)
        return (new_state, intra_out + inter_out)
    init_state = jnp.zeros((heads_n, state_n, head_size), values.dtype)
    inputs = (blocked(values), blocked(log_decay), blocked(steps_dt), blocked(b_mat), blocked(c_mat), blocked(segment), prev_lasts)
    scan_out = lax.scan(one_block, init_state, inputs)[1]
    return scan_out.reshape(row_count, heads_n, head_size)

def mixer_core(zx_rows, dt_raw, b_conv, c_conv, conv_wx, conv_bx, a_log, dt_bias, d_skip, segment=None, heads_n=1):
    inner_n = zx_rows.shape[1] // 2
    row_count = zx_rows.shape[0]
    x_conv = jax.nn.silu(causal_conv(zx_rows[:, inner_n:], conv_wx, conv_bx, segment))
    steps_dt = jax.nn.softplus(dt_raw + dt_bias[None, :])
    decay_rate = -jnp.exp(a_log)
    values = x_conv.reshape(row_count, heads_n, inner_n // heads_n)
    mixed_out = ssd_scan(values, steps_dt, decay_rate, b_conv, c_conv, segment, SCAN_BLOCK) + d_skip[None, :, None] * values
    return mixed_out.reshape(row_count, inner_n) * jax.nn.silu(zx_rows[:, :inner_n])

def bc_core(bc_pre, conv_wbc, conv_bbc, segment=None):
    return jax.nn.silu(causal_conv(bc_pre, conv_wbc, conv_bbc, segment))

def reference(tokens, cotangent, seq_lens, input_norm_gain, w_zx, w_bc, w_dt, conv_wx, conv_bx, conv_wbc, conv_bbc, a_log, dt_bias, d_skip, norm_gate, w_out):
    w_zx_flat = w_zx.reshape(D, 2 * INNER)
    tok_blocks = tokens.reshape(N_DP, TOK_DEV, D)
    cot_blocks = cotangent.reshape(N_DP, TOK_DEV, D)

    def one_device(totals, block_in):
        tok_rows, cotangent_row_values, lengths = block_in
        segment = segment_ids(lengths, TOK_DEV)
        is_live = (segment < SEQ_DEV)[:, None]
        tok_float = tok_rows.astype(jnp.float32)
        inverse_root_mean = lax.rsqrt(lax.optimization_barrier(jnp.mean(tok_float * tok_float, axis=1, keepdims=True)) + NORM_EPS)
        unit_scaled_input = tok_float * inverse_root_mean
        normed = (unit_scaled_input * input_norm_gain[None, :]).astype(jnp.bfloat16)
        zx_rows = jnp.dot(normed, w_zx_flat, preferred_element_type=jnp.float32)
        bc_pre = jnp.dot(normed, w_bc, preferred_element_type=jnp.float32)
        dt_raw = jnp.dot(normed, w_dt, preferred_element_type=jnp.float32)
        bc_post, bc_back = jax.vjp(partial(bc_core, segment=segment), bc_pre, conv_wbc, conv_bbc)
        gated_rows, core_back = jax.vjp(partial(mixer_core, segment=segment, heads_n=H), zx_rows, dt_raw, bc_post[:, :STATE], bc_post[:, STATE:], conv_wx, conv_bx, a_log, dt_bias, d_skip)
        cot_live = jnp.where(is_live, cotangent_row_values, jnp.zeros_like(cotangent_row_values))
        d_gate = contract_cols(cot_live, w_out)
        d_hat = d_gate * norm_gate[None, :]
        squares = lax.optimization_barrier(jnp.sum(gated_rows * gated_rows, axis=1, keepdims=True))
        cross_sum = lax.optimization_barrier(jnp.sum(d_hat * gated_rows, axis=1, keepdims=True))
        r_gate = lax.rsqrt(squares / INNER + NORM_EPS)
        gate_hat = gated_rows * r_gate
        gate_out = (gate_hat * norm_gate[None, :]).astype(jnp.bfloat16)
        branch = jnp.dot(gate_out, w_out, preferred_element_type=jnp.float32)
        block_rows = (tok_float + jnp.where(is_live, branch, 0.0)).astype(jnp.bfloat16)
        grad_out = contract_rows(gate_out, cot_live)
        grad_gate = lax.optimization_barrier(jnp.sum(d_gate * gate_hat, axis=0))
        d_gated = r_gate * d_hat - gated_rows * (r_gate * r_gate * r_gate * cross_sum / INNER)
        d_zx, d_dt, d_b, d_c, grad_conv_wx, grad_conv_bx, grad_a_log, grad_dt_bias, grad_d_skip = core_back(d_gated)
        d_bc, grad_conv_wbc, grad_conv_bbc = bc_back(jnp.concatenate([d_b, d_c], axis=1))
        d_zx_half = d_zx.astype(jnp.bfloat16)
        d_bc_half = d_bc.astype(jnp.bfloat16)
        d_dt_half = d_dt.astype(jnp.bfloat16)
        grad_zx = contract_rows(normed, d_zx_half)
        grad_bc = contract_rows(normed, d_bc_half)
        grad_dt = contract_rows(normed, d_dt_half)
        normed_input_gradient = contract_cols(d_zx_half, w_zx_flat) + contract_cols(d_bc_half, w_bc) + contract_cols(d_dt_half, w_dt)
        grad_in = lax.optimization_barrier(jnp.sum(normed_input_gradient * unit_scaled_input, axis=0))
        unit_input_gradient = normed_input_gradient * input_norm_gain[None, :]
        row_gradient_values = cotangent_row_values.astype(jnp.float32) + inverse_root_mean * (unit_input_gradient - unit_scaled_input * lax.optimization_barrier(jnp.mean(unit_input_gradient * unit_scaled_input, axis=1, keepdims=True)))
        fresh = (grad_zx, grad_bc, grad_dt, grad_out, grad_conv_wx, grad_conv_bx, grad_conv_wbc, grad_conv_bbc, grad_a_log, grad_dt_bias, grad_d_skip, grad_gate, grad_in)
        new_totals = jax.tree.map(jnp.add, totals, fresh)
        return (new_totals, (block_rows, row_gradient_values))
    zero_f = jnp.float32
    init_totals = (jnp.zeros((D, 2 * INNER), zero_f), jnp.zeros((D, 2 * STATE), zero_f), jnp.zeros((D, H), zero_f), jnp.zeros((INNER, D), zero_f), jnp.zeros((CONV, INNER), zero_f), jnp.zeros((INNER,), zero_f), jnp.zeros((CONV, 2 * STATE), zero_f), jnp.zeros((2 * STATE,), zero_f), jnp.zeros((H,), zero_f), jnp.zeros((H,), zero_f), jnp.zeros((H,), zero_f), jnp.zeros((INNER,), zero_f), jnp.zeros((D,), zero_f))
    totals, stacked = lax.scan(one_device, init_totals, (tok_blocks, cot_blocks, seq_lens))
    block_out = stacked[0].reshape(TOKENS, D)
    d_tokens = stacked[1].reshape(TOKENS, D)
    grad_zx = totals[0].reshape(D, 2, INNER)
    return (block_out, d_tokens, grad_zx, totals[1], totals[2], totals[3], totals[4], totals[5], totals[6], totals[7], totals[8], totals[9], totals[10], totals[11], totals[12])
```

```python
from functools import partial


import jax
import jax.numpy as jnp
from jax import lax
from jax.experimental import pallas as pl
from jax.experimental.pallas import tpu as pltpu

PRECISE = lax.Precision.HIGHEST
HEAD_DIM = 64
PAIR = 2


def _dot(a, b):
    return jnp.dot(a, b, precision=PRECISE, preferred_element_type=jnp.float32)


def _dot_tn(a, b):
    return lax.dot_general(a, b, (((0,), (0,)), ((), ())), precision=PRECISE,
                           preferred_element_type=jnp.float32)


def _dot_nt(a, b):
    return lax.dot_general(a, b, (((1,), (1,)), ((), ())), precision=PRECISE,
                           preferred_element_type=jnp.float32)


def _prologue(c_ref, b_ref, segc_ref, segr_ref, s_scr, neg_scr):
    s_scr[...] = _dot_nt(c_ref[...], b_ref[...])
    rows = s_scr.shape[0]
    row_i = lax.broadcasted_iota(jnp.int32, (rows, rows), 0)
    col_j = lax.broadcasted_iota(jnp.int32, (rows, rows), 1)
    keep = (col_j <= row_i) & (segc_ref[...] == segr_ref[...])
    neg_scr[...] = jnp.where(keep, 0.0, -jnp.inf).astype(jnp.float32)


def _fwd_kernel(c_ref, b_ref, segc_ref, segr_ref, x_ref, cumc_ref, cumr_ref, dtr_ref,
                y_ref, s_scr, neg_scr):
    @pl.when(pl.program_id(0) == 0)
    def _():
        _prologue(c_ref, b_ref, segc_ref, segr_ref, s_scr, neg_scr)

    for k in range(PAIR):
        cc = cumc_ref[0, :, k:k + 1]
        cr = cumr_ref[0, k:k + 1, :]
        dr = dtr_ref[0, k:k + 1, :]
        decays = jnp.exp(cc - cr + neg_scr[...])
        mixing = s_scr[...] * (decays * dr)
        y_ref[:, k * HEAD_DIM:(k + 1) * HEAD_DIM] = _dot(
            mixing, x_ref[:, k * HEAD_DIM:(k + 1) * HEAD_DIM])


def _bwd_kernel(c_ref, b_ref, segc_ref, segr_ref, x_ref, cumc_ref, cumr_ref, dtr_ref, g_ref,
                dx_ref, dcumc_ref, dcumr_ref, ddtr_ref, db_ref, dc_ref,
                s_scr, neg_scr, ds_scr):
    step = pl.program_id(0)

    @pl.when(step == 0)
    def _():
        _prologue(c_ref, b_ref, segc_ref, segr_ref, s_scr, neg_scr)
        ds_scr[...] = jnp.zeros_like(ds_scr)

    for k in range(PAIR):
        cc = cumc_ref[0, :, k:k + 1]
        cr = cumr_ref[0, k:k + 1, :]
        dr = dtr_ref[0, k:k + 1, :]
        decays = jnp.exp(cc - cr + neg_scr[...])
        weights = decays * dr
        scores = s_scr[...]
        mixing = scores * weights
        xh = x_ref[:, k * HEAD_DIM:(k + 1) * HEAD_DIM]
        gh = g_ref[:, k * HEAD_DIM:(k + 1) * HEAD_DIM]
        dx_ref[:, k * HEAD_DIM:(k + 1) * HEAD_DIM] = _dot_tn(mixing, gh)
        d_mix = _dot_nt(gh, xh)
        d_dec = d_mix * decays
        ds_scr[...] += d_dec * dr
        through = d_dec * scores
        d_dt_row = jnp.sum(through, axis=0, keepdims=True)
        q_mat = through * dr
        dcumc_ref[0, :, k:k + 1] = jnp.sum(q_mat, axis=1, keepdims=True)
        dcumr_ref[0, k:k + 1, :] = -(d_dt_row * dr)
        ddtr_ref[0, k:k + 1, :] = d_dt_row

    @pl.when(step == pl.num_programs(0) - 1)
    def _():
        dc_ref[...] = _dot(ds_scr[...], b_ref[...])
        db_ref[...] = _dot_tn(ds_scr[...], c_ref[...])


def _specs(rows, state):
    full = lambda shape: pl.BlockSpec(shape, lambda g: (0,) * len(shape))
    return [
        full((rows, state)),
        full((rows, state)),
        full((rows, 1)),
        full((1, rows)),
        pl.BlockSpec((rows, PAIR * HEAD_DIM), lambda g: (0, g)),
        pl.BlockSpec((1, rows, PAIR), lambda g: (g, 0, 0)),
        pl.BlockSpec((1, PAIR, rows), lambda g: (g, 0, 0)),
        pl.BlockSpec((1, PAIR, rows), lambda g: (g, 0, 0)),
    ]


def _prep(dt, cum, seg):
    rows, heads = dt.shape
    groups = heads // PAIR
    cumr = cum.T.reshape(groups, PAIR, rows)
    cumc = jnp.transpose(cumr, (0, 2, 1))
    dtr = dt.T.reshape(groups, PAIR, rows)
    segc = seg.reshape(rows, 1)
    segr = seg.reshape(1, rows)
    return cumc, cumr, dtr, segc, segr


def _fwd_call(x, dt, cum, b_mat, c_mat, seg):
    rows, inner = x.shape
    heads = dt.shape[1]
    groups = heads // PAIR
    state = b_mat.shape[1]
    cumc, cumr, dtr, segc, segr = _prep(dt, cum, seg)
    flops = 2 * rows * rows * state * 6 + heads * (2 * rows * rows * HEAD_DIM * 6 + 8 * rows * rows)
    return pl.pallas_call(
        _fwd_kernel,
        grid=(groups,),
        in_specs=_specs(rows, state),
        out_specs=pl.BlockSpec((rows, PAIR * HEAD_DIM), lambda g: (0, g)),
        out_shape=jax.ShapeDtypeStruct((rows, inner), jnp.float32),
        scratch_shapes=[pltpu.VMEM((rows, rows), jnp.float32),
                        pltpu.VMEM((rows, rows), jnp.float32)],
        compiler_params=pltpu.CompilerParams(dimension_semantics=("arbitrary",)),
        cost_estimate=pl.CostEstimate(flops=flops, transcendentals=heads * rows * rows,
                                      bytes_accessed=4 * (2 * rows * inner + 2 * rows * state)),
        name="ssd_fwd",
    )(c_mat, b_mat, segc, segr, x, cumc, cumr, dtr)


def _bwd_call(x, dt, cum, b_mat, c_mat, seg, g):
    rows, inner = x.shape
    heads = dt.shape[1]
    groups = heads // PAIR
    state = b_mat.shape[1]
    cumc, cumr, dtr, segc, segr = _prep(dt, cum, seg)
    full = lambda shape: pl.BlockSpec(shape, lambda gi: (0,) * len(shape))
    flops = 2 * rows * rows * state * 6 * 3 + heads * (2 * 2 * rows * rows * HEAD_DIM * 6 + 16 * rows * rows)
    dx, dcumc, dcumr, ddtr, db, dc = pl.pallas_call(
        _bwd_kernel,
        grid=(groups,),
        in_specs=_specs(rows, state) + [pl.BlockSpec((rows, PAIR * HEAD_DIM), lambda gi: (0, gi))],
        out_specs=[
            pl.BlockSpec((rows, PAIR * HEAD_DIM), lambda gi: (0, gi)),
            pl.BlockSpec((1, rows, PAIR), lambda gi: (gi, 0, 0)),
            pl.BlockSpec((1, PAIR, rows), lambda gi: (gi, 0, 0)),
            pl.BlockSpec((1, PAIR, rows), lambda gi: (gi, 0, 0)),
            full((rows, state)),
            full((rows, state)),
        ],
        out_shape=[
            jax.ShapeDtypeStruct((rows, inner), jnp.float32),
            jax.ShapeDtypeStruct((groups, rows, PAIR), jnp.float32),
            jax.ShapeDtypeStruct((groups, PAIR, rows), jnp.float32),
            jax.ShapeDtypeStruct((groups, PAIR, rows), jnp.float32),
            jax.ShapeDtypeStruct((rows, state), jnp.float32),
            jax.ShapeDtypeStruct((rows, state), jnp.float32),
        ],
        scratch_shapes=[pltpu.VMEM((rows, rows), jnp.float32),
                        pltpu.VMEM((rows, rows), jnp.float32),
                        pltpu.VMEM((rows, rows), jnp.float32)],
        compiler_params=pltpu.CompilerParams(dimension_semantics=("arbitrary",)),
        cost_estimate=pl.CostEstimate(flops=flops, transcendentals=heads * rows * rows,
                                      bytes_accessed=4 * (4 * rows * inner + 4 * rows * state)),
        name="ssd_bwd",
    )(c_mat, b_mat, segc, segr, x, cumc, cumr, dtr, g)
    d_cum = jnp.transpose(dcumc, (0, 2, 1)).reshape(heads, rows).T + dcumr.reshape(heads, rows).T
    d_dt = ddtr.reshape(heads, rows).T
    return dx, d_dt, d_cum, db, dc


@jax.custom_vjp
def ssd_core(x, dt, cum, b_mat, c_mat, seg):
    return _fwd_call(x, dt, cum, b_mat, c_mat, seg)


def _ssd_core_fwd(x, dt, cum, b_mat, c_mat, seg):
    return _fwd_call(x, dt, cum, b_mat, c_mat, seg), (x, dt, cum, b_mat, c_mat, seg)


def _ssd_core_bwd(res, g):
    x, dt, cum, b_mat, c_mat, seg = res
    dx, d_dt, d_cum, db, dc = _bwd_call(x, dt, cum, b_mat, c_mat, seg, g)
    return dx, d_dt, d_cum, db, dc, None


ssd_core.defvjp(_ssd_core_fwd, _ssd_core_bwd)

from jax.sharding import PartitionSpec as P
from jax.experimental.layout import Layout, with_layout_constraint

NORM_EPS = 1e-05


def contract_rows(first_op, second_op):
    return lax.dot_general(
        first_op, second_op, (((0,), (0,)), ((), ())), preferred_element_type=jnp.float32
    )


def contract_cols(first_op, second_op):
    return lax.dot_general(
        first_op, second_op, (((1,), (1,)), ((), ())), preferred_element_type=jnp.float32
    )


def segment_ids(lengths, row_count):
    seq_ends = jnp.cumsum(lengths)
    positions = jnp.arange(row_count, dtype=jnp.int32)
    return jnp.sum((positions[:, None] >= seq_ends[None, :]).astype(jnp.int32), axis=1)


def causal_conv(signal, kernel_w, kernel_b, segment):
    kernel_len = kernel_w.shape[0]
    row_count = signal.shape[0]
    summed = kernel_b[None, :] + kernel_w[kernel_len - 1][None, :] * signal
    for lag_steps in range(1, kernel_len):
        shifted = jnp.concatenate(
            [jnp.zeros((lag_steps, signal.shape[1]), jnp.float32), signal[: row_count - lag_steps]],
            axis=0,
        )
        earlier = jnp.concatenate(
            [jnp.full((lag_steps,), -1, jnp.int32), segment[: row_count - lag_steps]]
        )
        same_seq = (earlier == segment).astype(signal.dtype)
        summed = (
            summed + kernel_w[kernel_len - 1 - lag_steps][None, :] * shifted * same_seq[:, None]
        )
    return summed


def mixer_core(zx_rows, dt_raw, b_conv, c_conv, conv_wx, conv_bx, a_log, dt_bias, d_skip,
               segment=None):
    inner_n = zx_rows.shape[1] // 2
    heads_n = a_log.shape[0]
    x_conv = jax.nn.silu(causal_conv(zx_rows[:, inner_n:], conv_wx, conv_bx, segment))
    steps_dt = jax.nn.softplus(dt_raw + dt_bias[None, :])
    decay = steps_dt * (-jnp.exp(a_log))[None, :]
    cum = jnp.cumsum(decay, axis=0)
    scanned = ssd_core(x_conv, steps_dt, cum, b_conv, c_conv, segment)
    skip = jnp.repeat(d_skip, inner_n // heads_n)
    mixed_out = scanned + skip[None, :] * x_conv
    return mixed_out * jax.nn.silu(zx_rows[:, :inner_n])


def bc_core(bc_pre, conv_wbc, conv_bbc, segment=None):
    return jax.nn.silu(causal_conv(bc_pre, conv_wbc, conv_bbc, segment))


def per_device_body(tokens, cotangent, seq_lens, input_norm_gain, w_zx, w_bc, w_dt, conv_wx, conv_bx,
               conv_wbc, conv_bbc, a_log, dt_bias, d_skip, norm_gate, w_out):
    n_dp = lax.axis_size("dp")
    x_full = lax.all_gather(tokens, "tensor", axis=1, tiled=True)
    cot_full = lax.all_gather(cotangent, "tensor", axis=1, tiled=True)
    row_count = tokens.shape[0]
    feat_n = tokens.shape[1]
    d_model = x_full.shape[1]
    feat_start = lax.axis_index("tensor") * feat_n
    state_n = w_bc.shape[1] // 2
    inner_loc = norm_gate.shape[0]
    inner_all = inner_loc * lax.axis_size("tensor")
    segment = segment_ids(seq_lens[0], row_count)
    is_live = (segment < seq_lens.shape[1])[:, None]
    w_zx_flat = w_zx.reshape(d_model, 2 * inner_loc)
    tok_float = x_full.astype(jnp.float32)
    inverse_root_mean = lax.rsqrt(jnp.mean(tok_float * tok_float, axis=1, keepdims=True) + NORM_EPS)
    unit_scaled_input = tok_float * inverse_root_mean
    normed = (unit_scaled_input * input_norm_gain[None, :]).astype(jnp.bfloat16)
    zx_rows = jnp.dot(normed, w_zx_flat, preferred_element_type=jnp.float32)
    bc_pre = jnp.dot(normed, w_bc, preferred_element_type=jnp.float32)
    dt_raw = jnp.dot(normed, w_dt, preferred_element_type=jnp.float32)
    bc_post, bc_back = jax.vjp(partial(bc_core, segment=segment), bc_pre, conv_wbc, conv_bbc)
    gated_rows, core_back = jax.vjp(
        partial(mixer_core, segment=segment),
        zx_rows, dt_raw, bc_post[:, :state_n], bc_post[:, state_n:],
        conv_wx, conv_bx, a_log, dt_bias, d_skip,
    )
    cot_live = jnp.where(is_live, cot_full, jnp.zeros_like(cot_full))
    d_gate = contract_cols(cot_live, w_out)
    d_hat = d_gate * norm_gate[None, :]
    stats = lax.psum(
        jnp.concatenate([jnp.sum(gated_rows * gated_rows, axis=1, keepdims=True),
                         jnp.sum(d_hat * gated_rows, axis=1, keepdims=True)], axis=1),
        "tensor")
    squares, cross_sum = stats[:, 0:1], stats[:, 1:2]
    r_gate = lax.rsqrt(squares / inner_all + NORM_EPS)
    gate_hat = gated_rows * r_gate
    gate_out = (gate_hat * norm_gate[None, :]).astype(jnp.bfloat16)
    branch_part = jnp.dot(gate_out, w_out, preferred_element_type=jnp.float32)
    grad_gate = jnp.sum(d_gate * gate_hat, axis=0)
    d_gated = r_gate * d_hat - gated_rows * (r_gate * r_gate * r_gate * cross_sum / inner_all)
    d_gated, branch_part = lax.optimization_barrier((d_gated, branch_part))
    branch = lax.psum_scatter(branch_part, "tensor", scatter_dimension=1, tiled=True)
    own_float = tokens.astype(jnp.float32)
    block_out = (own_float + jnp.where(is_live, branch, 0.0)).astype(jnp.bfloat16)
    d_zx, d_dt, d_b, d_c, grad_conv_wx, grad_conv_bx, grad_a_log, grad_dt_bias, grad_d_skip = (
        core_back(d_gated)
    )
    n_tp = lax.axis_size("tensor")
    d_bc_part = jnp.concatenate([d_b, d_c], axis=1)
    d_zx_half = d_zx.astype(jnp.bfloat16)
    d_dt_half = d_dt.astype(jnp.bfloat16)
    partial_in = contract_cols(d_zx_half, w_zx_flat) + contract_cols(d_dt_half, w_dt)
    bc_w = d_bc_part.shape[1]
    rs_in = jnp.concatenate(
        [partial_in.reshape(row_count, n_tp, feat_n),
         jnp.broadcast_to(d_bc_part[:, None, :], (row_count, n_tp, bc_w))], axis=2,
    ).reshape(row_count, n_tp * (feat_n + bc_w))
    rs_out = lax.psum_scatter(rs_in, "tensor", scatter_dimension=1, tiled=True)
    d_bc_post = rs_out[:, feat_n:]
    d_bc, grad_conv_wbc, grad_conv_bbc = bc_back(d_bc_post)
    d_bc_half = d_bc.astype(jnp.bfloat16)
    own_hat = lax.dynamic_slice_in_dim(unit_scaled_input, feat_start, feat_n, 1)
    own_gain = lax.dynamic_slice_in_dim(input_norm_gain, feat_start, feat_n, 0)
    own_w_bc = lax.dynamic_slice_in_dim(w_bc, feat_start, feat_n, 0)
    own_dn = rs_out[:, :feat_n] + contract_cols(d_bc_half, own_w_bc)
    own_dxhat = own_dn * own_gain[None, :]
    row_inner_product = lax.psum(jnp.sum(own_dxhat * own_hat, axis=1, keepdims=True),
                                 "tensor") / d_model
    grad_in = jnp.sum(own_dn * own_hat, axis=0)
    d_tokens = cotangent.astype(jnp.float32) + inverse_root_mean * (
        own_dxhat - own_hat * row_inner_product
    )
    smalls = (grad_conv_wx, grad_conv_bx, grad_conv_wbc, grad_conv_bbc, grad_a_log,
              grad_dt_bias, grad_d_skip, grad_gate, grad_in)
    flat_small = jnp.concatenate([s.reshape(-1) for s in smalls])
    chunk = d_model // n_dp
    small_cols = -(-flat_small.shape[0] // chunk)
    small_block = jnp.pad(flat_small, (0, small_cols * chunk - flat_small.shape[0])).reshape(
        chunk, small_cols)
    row_major = Layout(major_to_minor=(0, 1))
    grads_main = with_layout_constraint(
        contract_rows(normed, jnp.concatenate([d_zx_half, d_bc_half, d_dt_half], axis=1)),
        row_major)
    grad_out_t = with_layout_constraint(contract_rows(cot_live, gate_out), row_major)
    packed = with_layout_constraint(
        jnp.concatenate([grads_main, grad_out_t, jnp.tile(small_block, (n_dp, 1))], axis=1),
        row_major)
    reduced = lax.psum_scatter(packed, "dp", scatter_dimension=0, tiled=True)
    col = 0
    pieces = []
    for w in (2 * inner_loc, 2 * state_n, w_dt.shape[1], inner_loc):
        pieces.append(reduced[:, col:col + w])
        col += w
    grad_zx_sum, grad_bc_sum, grad_dt_sum, grad_out_t_sum = pieces
    small_sum = reduced[:, col:].reshape(-1)
    outs_small = []
    pos = 0
    for s in smalls:
        outs_small.append(small_sum[pos:pos + s.size].reshape(s.shape))
        pos += s.size
    grad_zx_out = grad_zx_sum.reshape(chunk, 2, inner_loc)
    return (block_out, d_tokens, grad_zx_out, grad_bc_sum, grad_dt_sum, grad_out_t_sum.T,
            *outs_small)


def solution(mesh):
    in_specs = (
        P("dp", "tensor"), P("dp", "tensor"), P("dp", None), P(),
        P(None, None, "tensor"), P(), P(None, "tensor"), P(None, "tensor"), P("tensor"),
        P(), P(), P("tensor"), P("tensor"), P("tensor"), P("tensor"), P("tensor", None),
    )
    out_specs = (
        P("dp", "tensor"), P("dp", "tensor"), P("dp", None, "tensor"), P("dp", None),
        P("dp", "tensor"), P("tensor", "dp"), P(None, "tensor"), P("tensor"), P(), P(),
        P("tensor"), P("tensor"), P("tensor"), P("tensor"), P("tensor"),
    )
    return jax.shard_map(
        per_device_body, mesh=mesh, in_specs=in_specs, out_specs=out_specs, check_vma=False
    )
```

```python
from functools import partial


import jax
import jax.numpy as jnp
from jax import lax
from jax.experimental import pallas as pl
from jax.experimental.pallas import tpu as pltpu

PRECISE = lax.Precision.HIGHEST
HEAD_DIM = 64
PAIR = 2


def _dot(a, b):
    return jnp.dot(a, b, precision=PRECISE, preferred_element_type=jnp.float32)


def _dot_tn(a, b):
    return lax.dot_general(a, b, (((0,), (0,)), ((), ())), precision=PRECISE,
                           preferred_element_type=jnp.float32)


def _dot_nt(a, b):
    return lax.dot_general(a, b, (((1,), (1,)), ((), ())), precision=PRECISE,
                           preferred_element_type=jnp.float32)


def _prologue(c_ref, b_ref, segc_ref, segr_ref, s_scr, neg_scr):
    s_scr[...] = _dot_nt(c_ref[...], b_ref[...])
    rows = s_scr.shape[0]
    row_i = lax.broadcasted_iota(jnp.int32, (rows, rows), 0)
    col_j = lax.broadcasted_iota(jnp.int32, (rows, rows), 1)
    keep = (col_j <= row_i) & (segc_ref[...] == segr_ref[...])
    neg_scr[...] = jnp.where(keep, 0.0, -jnp.inf).astype(jnp.float32)


def _fwd_kernel(c_ref, b_ref, segc_ref, segr_ref, x_ref, cumc_ref, cumr_ref, dtr_ref,
                y_ref, s_scr, neg_scr):
    @pl.when(pl.program_id(0) == 0)
    def _():
        _prologue(c_ref, b_ref, segc_ref, segr_ref, s_scr, neg_scr)

    for k in range(PAIR):
        cc = cumc_ref[0, :, k:k + 1]
        cr = cumr_ref[0, k:k + 1, :]
        dr = dtr_ref[0, k:k + 1, :]
        decays = jnp.exp(cc - cr + neg_scr[...])
        mixing = s_scr[...] * (decays * dr)
        y_ref[:, k * HEAD_DIM:(k + 1) * HEAD_DIM] = _dot(
            mixing, x_ref[:, k * HEAD_DIM:(k + 1) * HEAD_DIM])


def _bwd_kernel(c_ref, b_ref, segc_ref, segr_ref, x_ref, cumc_ref, cumr_ref, dtr_ref, g_ref,
                dx_ref, dcumc_ref, dcumr_ref, ddtr_ref, db_ref, dc_ref,
                s_scr, neg_scr, ds_scr):
    step = pl.program_id(0)

    @pl.when(step == 0)
    def _():
        _prologue(c_ref, b_ref, segc_ref, segr_ref, s_scr, neg_scr)
        ds_scr[...] = jnp.zeros_like(ds_scr)

    for k in range(PAIR):
        cc = cumc_ref[0, :, k:k + 1]
        cr = cumr_ref[0, k:k + 1, :]
        dr = dtr_ref[0, k:k + 1, :]
        decays = jnp.exp(cc - cr + neg_scr[...])
        weights = decays * dr
        scores = s_scr[...]
        mixing = scores * weights
        xh = x_ref[:, k * HEAD_DIM:(k + 1) * HEAD_DIM]
        gh = g_ref[:, k * HEAD_DIM:(k + 1) * HEAD_DIM]
        dx_ref[:, k * HEAD_DIM:(k + 1) * HEAD_DIM] = _dot_tn(mixing, gh)
        d_mix = _dot_nt(gh, xh)
        d_dec = d_mix * decays
        ds_scr[...] += d_dec * dr
        through = d_dec * scores
        d_dt_row = jnp.sum(through, axis=0, keepdims=True)
        q_mat = through * dr
        dcumc_ref[0, :, k:k + 1] = jnp.sum(q_mat, axis=1, keepdims=True)
        dcumr_ref[0, k:k + 1, :] = -(d_dt_row * dr)
        ddtr_ref[0, k:k + 1, :] = d_dt_row

    @pl.when(step == pl.num_programs(0) - 1)
    def _():
        dc_ref[...] = _dot(ds_scr[...], b_ref[...])
        db_ref[...] = _dot_tn(ds_scr[...], c_ref[...])


def _specs(rows, state):
    full = lambda shape: pl.BlockSpec(shape, lambda g: (0,) * len(shape))
    return [
        full((rows, state)),
        full((rows, state)),
        full((rows, 1)),
        full((1, rows)),
        pl.BlockSpec((rows, PAIR * HEAD_DIM), lambda g: (0, g)),
        pl.BlockSpec((1, rows, PAIR), lambda g: (g, 0, 0)),
        pl.BlockSpec((1, PAIR, rows), lambda g: (g, 0, 0)),
        pl.BlockSpec((1, PAIR, rows), lambda g: (g, 0, 0)),
    ]


def _prep(dt, cum, seg):
    rows, heads = dt.shape
    groups = heads // PAIR
    cumr = cum.T.reshape(groups, PAIR, rows)
    cumc = jnp.transpose(cumr, (0, 2, 1))
    dtr = dt.T.reshape(groups, PAIR, rows)
    segc = seg.reshape(rows, 1)
    segr = seg.reshape(1, rows)
    return cumc, cumr, dtr, segc, segr


def _fwd_call(x, dt, cum, b_mat, c_mat, seg):
    rows, inner = x.shape
    heads = dt.shape[1]
    groups = heads // PAIR
    state = b_mat.shape[1]
    cumc, cumr, dtr, segc, segr = _prep(dt, cum, seg)
    flops = 2 * rows * rows * state * 6 + heads * (2 * rows * rows * HEAD_DIM * 6 + 8 * rows * rows)
    return pl.pallas_call(
        _fwd_kernel,
        grid=(groups,),
        in_specs=_specs(rows, state),
        out_specs=pl.BlockSpec((rows, PAIR * HEAD_DIM), lambda g: (0, g)),
        out_shape=jax.ShapeDtypeStruct((rows, inner), jnp.float32),
        scratch_shapes=[pltpu.VMEM((rows, rows), jnp.float32),
                        pltpu.VMEM((rows, rows), jnp.float32)],
        compiler_params=pltpu.CompilerParams(dimension_semantics=("arbitrary",)),
        cost_estimate=pl.CostEstimate(flops=flops, transcendentals=heads * rows * rows,
                                      bytes_accessed=4 * (2 * rows * inner + 2 * rows * state)),
        name="ssd_fwd",
    )(c_mat, b_mat, segc, segr, x, cumc, cumr, dtr)


def _bwd_call(x, dt, cum, b_mat, c_mat, seg, g):
    rows, inner = x.shape
    heads = dt.shape[1]
    groups = heads // PAIR
    state = b_mat.shape[1]
    cumc, cumr, dtr, segc, segr = _prep(dt, cum, seg)
    full = lambda shape: pl.BlockSpec(shape, lambda gi: (0,) * len(shape))
    flops = 2 * rows * rows * state * 6 * 3 + heads * (2 * 2 * rows * rows * HEAD_DIM * 6 + 16 * rows * rows)
    dx, dcumc, dcumr, ddtr, db, dc = pl.pallas_call(
        _bwd_kernel,
        grid=(groups,),
        in_specs=_specs(rows, state) + [pl.BlockSpec((rows, PAIR * HEAD_DIM), lambda gi: (0, gi))],
        out_specs=[
            pl.BlockSpec((rows, PAIR * HEAD_DIM), lambda gi: (0, gi)),
            pl.BlockSpec((1, rows, PAIR), lambda gi: (gi, 0, 0)),
            pl.BlockSpec((1, PAIR, rows), lambda gi: (gi, 0, 0)),
            pl.BlockSpec((1, PAIR, rows), lambda gi: (gi, 0, 0)),
            full((rows, state)),
            full((rows, state)),
        ],
        out_shape=[
            jax.ShapeDtypeStruct((rows, inner), jnp.float32),
            jax.ShapeDtypeStruct((groups, rows, PAIR), jnp.float32),
            jax.ShapeDtypeStruct((groups, PAIR, rows), jnp.float32),
            jax.ShapeDtypeStruct((groups, PAIR, rows), jnp.float32),
            jax.ShapeDtypeStruct((rows, state), jnp.float32),
            jax.ShapeDtypeStruct((rows, state), jnp.float32),
        ],
        scratch_shapes=[pltpu.VMEM((rows, rows), jnp.float32),
                        pltpu.VMEM((rows, rows), jnp.float32),
                        pltpu.VMEM((rows, rows), jnp.float32)],
        compiler_params=pltpu.CompilerParams(dimension_semantics=("arbitrary",)),
        cost_estimate=pl.CostEstimate(flops=flops, transcendentals=heads * rows * rows,
                                      bytes_accessed=4 * (4 * rows * inner + 4 * rows * state)),
        name="ssd_bwd",
    )(c_mat, b_mat, segc, segr, x, cumc, cumr, dtr, g)
    d_cum = jnp.transpose(dcumc, (0, 2, 1)).reshape(heads, rows).T + dcumr.reshape(heads, rows).T
    d_dt = ddtr.reshape(heads, rows).T
    return dx, d_dt, d_cum, db, dc


@jax.custom_vjp
def ssd_core(x, dt, cum, b_mat, c_mat, seg):
    return _fwd_call(x, dt, cum, b_mat, c_mat, seg)


def _ssd_core_fwd(x, dt, cum, b_mat, c_mat, seg):
    return _fwd_call(x, dt, cum, b_mat, c_mat, seg), (x, dt, cum, b_mat, c_mat, seg)


def _ssd_core_bwd(res, g):
    x, dt, cum, b_mat, c_mat, seg = res
    dx, d_dt, d_cum, db, dc = _bwd_call(x, dt, cum, b_mat, c_mat, seg, g)
    return dx, d_dt, d_cum, db, dc, None


ssd_core.defvjp(_ssd_core_fwd, _ssd_core_bwd)

from jax.sharding import PartitionSpec as P
from jax.experimental.layout import Layout, with_layout_constraint

NORM_EPS = 1e-05
WIRE = jnp.bfloat16


def contract_rows(first_op, second_op):
    return lax.dot_general(
        first_op, second_op, (((0,), (0,)), ((), ())), preferred_element_type=jnp.float32
    )


def contract_cols(first_op, second_op):
    return lax.dot_general(
        first_op, second_op, (((1,), (1,)), ((), ())), preferred_element_type=jnp.float32
    )


def segment_ids(lengths, row_count):
    seq_ends = jnp.cumsum(lengths)
    positions = jnp.arange(row_count, dtype=jnp.int32)
    return jnp.sum((positions[:, None] >= seq_ends[None, :]).astype(jnp.int32), axis=1)


def causal_conv(signal, kernel_w, kernel_b, segment):
    kernel_len = kernel_w.shape[0]
    row_count = signal.shape[0]
    summed = kernel_b[None, :] + kernel_w[kernel_len - 1][None, :] * signal
    for lag_steps in range(1, kernel_len):
        shifted = jnp.concatenate(
            [jnp.zeros((lag_steps, signal.shape[1]), jnp.float32), signal[: row_count - lag_steps]],
            axis=0,
        )
        earlier = jnp.concatenate(
            [jnp.full((lag_steps,), -1, jnp.int32), segment[: row_count - lag_steps]]
        )
        same_seq = (earlier == segment).astype(signal.dtype)
        summed = (
            summed + kernel_w[kernel_len - 1 - lag_steps][None, :] * shifted * same_seq[:, None]
        )
    return summed


def mixer_core(zx_rows, dt_raw, b_conv, c_conv, conv_wx, conv_bx, a_log, dt_bias, d_skip,
               segment=None):
    inner_n = zx_rows.shape[1] // 2
    heads_n = a_log.shape[0]
    x_conv = jax.nn.silu(causal_conv(zx_rows[:, inner_n:], conv_wx, conv_bx, segment))
    steps_dt = jax.nn.softplus(dt_raw + dt_bias[None, :])
    decay = steps_dt * (-jnp.exp(a_log))[None, :]
    cum = jnp.cumsum(decay, axis=0)
    scanned = ssd_core(x_conv, steps_dt, cum, b_conv, c_conv, segment)
    skip = jnp.repeat(d_skip, inner_n // heads_n)
    mixed_out = scanned + skip[None, :] * x_conv
    return mixed_out * jax.nn.silu(zx_rows[:, :inner_n])


def bc_core(bc_pre, conv_wbc, conv_bbc, segment=None):
    return jax.nn.silu(causal_conv(bc_pre, conv_wbc, conv_bbc, segment))


def per_device_body(tokens, cotangent, seq_lens, input_norm_gain, w_zx, w_bc, w_dt, conv_wx, conv_bx,
               conv_wbc, conv_bbc, a_log, dt_bias, d_skip, norm_gate, w_out):
    n_dp = lax.axis_size("dp")
    x_full = lax.all_gather(tokens, "tensor", axis=1, tiled=True)
    cot_full = lax.all_gather(cotangent, "tensor", axis=1, tiled=True)
    row_count = tokens.shape[0]
    feat_n = tokens.shape[1]
    d_model = x_full.shape[1]
    feat_start = lax.axis_index("tensor") * feat_n
    state_n = w_bc.shape[1] // 2
    inner_loc = norm_gate.shape[0]
    inner_all = inner_loc * lax.axis_size("tensor")
    segment = segment_ids(seq_lens[0], row_count)
    is_live = (segment < seq_lens.shape[1])[:, None]
    w_zx_flat = w_zx.reshape(d_model, 2 * inner_loc)
    tok_float = x_full.astype(jnp.float32)
    inverse_root_mean = lax.rsqrt(jnp.mean(tok_float * tok_float, axis=1, keepdims=True) + NORM_EPS)
    unit_scaled_input = tok_float * inverse_root_mean
    normed = (unit_scaled_input * input_norm_gain[None, :]).astype(jnp.bfloat16)
    zx_rows = jnp.dot(normed, w_zx_flat, preferred_element_type=jnp.float32)
    bc_pre = jnp.dot(normed, w_bc, preferred_element_type=jnp.float32)
    dt_raw = jnp.dot(normed, w_dt, preferred_element_type=jnp.float32)
    bc_post, bc_back = jax.vjp(partial(bc_core, segment=segment), bc_pre, conv_wbc, conv_bbc)
    gated_rows, core_back = jax.vjp(
        partial(mixer_core, segment=segment),
        zx_rows, dt_raw, bc_post[:, :state_n], bc_post[:, state_n:],
        conv_wx, conv_bx, a_log, dt_bias, d_skip,
    )
    cot_live = jnp.where(is_live, cot_full, jnp.zeros_like(cot_full))
    d_gate = contract_cols(cot_live, w_out)
    d_hat = d_gate * norm_gate[None, :]
    stats = lax.psum(
        jnp.concatenate([jnp.sum(gated_rows * gated_rows, axis=1, keepdims=True),
                         jnp.sum(d_hat * gated_rows, axis=1, keepdims=True)], axis=1),
        "tensor")
    squares, cross_sum = stats[:, 0:1], stats[:, 1:2]
    r_gate = lax.rsqrt(squares / inner_all + NORM_EPS)
    gate_hat = gated_rows * r_gate
    gate_out = (gate_hat * norm_gate[None, :]).astype(jnp.bfloat16)
    branch_part = contract_rows(w_out, gate_out.T)
    grad_gate = jnp.sum(d_gate * gate_hat, axis=0)
    d_gated = r_gate * d_hat - gated_rows * (r_gate * r_gate * r_gate * cross_sum / inner_all)
    d_gated, branch_part = lax.optimization_barrier((d_gated, branch_part))
    branch = lax.psum_scatter(branch_part.astype(WIRE), "tensor", scatter_dimension=0,
                              tiled=True).astype(jnp.float32).T
    own_float = tokens.astype(jnp.float32)
    block_out = (own_float + jnp.where(is_live, branch, 0.0)).astype(jnp.bfloat16)
    d_zx, d_dt, d_b, d_c, grad_conv_wx, grad_conv_bx, grad_a_log, grad_dt_bias, grad_d_skip = (
        core_back(d_gated)
    )
    n_tp = lax.axis_size("tensor")
    d_zx, d_dt, block_out = lax.optimization_barrier((d_zx, d_dt, block_out))
    d_bc_part = jnp.concatenate([d_b, d_c], axis=1)
    d_zx_half = d_zx.astype(jnp.bfloat16)
    d_dt_half = d_dt.astype(jnp.bfloat16)
    partial_in_t = contract_cols(w_zx_flat, d_zx_half) + contract_cols(w_dt, d_dt_half)
    bc_w = d_bc_part.shape[1]
    rs_in = jnp.concatenate(
        [partial_in_t.reshape(n_tp, feat_n, row_count),
         jnp.broadcast_to(d_bc_part.T[None], (n_tp, bc_w, row_count))], axis=1,
    ).reshape(n_tp * (feat_n + bc_w), row_count)
    rs_out = lax.psum_scatter(rs_in.astype(WIRE), "tensor", scatter_dimension=0,
                              tiled=True).astype(jnp.float32).T
    d_bc_post = rs_out[:, feat_n:]
    d_bc, grad_conv_wbc, grad_conv_bbc = bc_back(d_bc_post)
    d_bc_half = d_bc.astype(jnp.bfloat16)
    own_hat = lax.dynamic_slice_in_dim(unit_scaled_input, feat_start, feat_n, 1)
    own_gain = lax.dynamic_slice_in_dim(input_norm_gain, feat_start, feat_n, 0)
    own_w_bc = lax.dynamic_slice_in_dim(w_bc, feat_start, feat_n, 0)
    own_dn = rs_out[:, :feat_n] + contract_cols(d_bc_half, own_w_bc)
    own_dxhat = own_dn * own_gain[None, :]
    row_inner_product = lax.psum(jnp.sum(own_dxhat * own_hat, axis=1, keepdims=True),
                                 "tensor") / d_model
    grad_in = jnp.sum(own_dn * own_hat, axis=0)
    d_tokens = cotangent.astype(jnp.float32) + inverse_root_mean * (
        own_dxhat - own_hat * row_inner_product
    )
    smalls = (grad_conv_wx, grad_conv_bx, grad_conv_wbc, grad_conv_bbc, grad_a_log,
              grad_dt_bias, grad_d_skip, grad_gate, grad_in)
    flat_small = jnp.concatenate([s.reshape(-1) for s in smalls])
    chunk = d_model // n_dp
    small_cols = -(-flat_small.shape[0] // chunk)
    small_block = jnp.pad(flat_small, (0, small_cols * chunk - flat_small.shape[0])).reshape(
        chunk, small_cols)
    row_major = Layout(major_to_minor=(0, 1))
    grads_main = with_layout_constraint(
        contract_rows(normed, jnp.concatenate([d_zx_half, d_bc_half, d_dt_half], axis=1)),
        row_major)
    grad_out_t = with_layout_constraint(contract_rows(cot_live, gate_out), row_major)
    packed = with_layout_constraint(
        jnp.concatenate([grads_main, grad_out_t, jnp.tile(small_block, (n_dp, 1))], axis=1),
        row_major)
    reduced = lax.psum_scatter(packed, "dp", scatter_dimension=0, tiled=True)
    col = 0
    pieces = []
    for w in (2 * inner_loc, 2 * state_n, w_dt.shape[1], inner_loc):
        pieces.append(reduced[:, col:col + w])
        col += w
    grad_zx_sum, grad_bc_sum, grad_dt_sum, grad_out_t_sum = pieces
    small_sum = reduced[:, col:].reshape(-1)
    outs_small = []
    pos = 0
    for s in smalls:
        outs_small.append(small_sum[pos:pos + s.size].reshape(s.shape))
        pos += s.size
    grad_zx_out = grad_zx_sum.reshape(chunk, 2, inner_loc)
    return (block_out, d_tokens, grad_zx_out, grad_bc_sum, grad_dt_sum, grad_out_t_sum.T,
            *outs_small)


def solution(mesh):
    in_specs = (
        P("dp", "tensor"), P("dp", "tensor"), P("dp", None), P(),
        P(None, None, "tensor"), P(), P(None, "tensor"), P(None, "tensor"), P("tensor"),
        P(), P(), P("tensor"), P("tensor"), P("tensor"), P("tensor"), P("tensor", None),
    )
    out_specs = (
        P("dp", "tensor"), P("dp", "tensor"), P("dp", None, "tensor"), P("dp", None),
        P("dp", "tensor"), P("tensor", "dp"), P(None, "tensor"), P("tensor"), P(), P(),
        P("tensor"), P("tensor"), P("tensor"), P("tensor"), P("tensor"),
    )
    return jax.shard_map(
        per_device_body, mesh=mesh, in_specs=in_specs, out_specs=out_specs, check_vma=False
    )
```

```python
from functools import partial


import jax
import jax.numpy as jnp
from jax import lax
from jax.experimental import pallas as pl
from jax.experimental.pallas import tpu as pltpu

PRECISE = lax.Precision.HIGHEST
HEAD_DIM = 64
PAIR = 2


def _dot(a, b):
    return jnp.dot(a, b, precision=PRECISE, preferred_element_type=jnp.float32)


def _dot_tn(a, b):
    return lax.dot_general(a, b, (((0,), (0,)), ((), ())), precision=PRECISE,
                           preferred_element_type=jnp.float32)


def _dot_nt(a, b):
    return lax.dot_general(a, b, (((1,), (1,)), ((), ())), precision=PRECISE,
                           preferred_element_type=jnp.float32)


def _prologue(c_ref, b_ref, segc_ref, segr_ref, s_scr, neg_scr):
    s_scr[...] = _dot_nt(c_ref[...], b_ref[...])
    rows = s_scr.shape[0]
    row_i = lax.broadcasted_iota(jnp.int32, (rows, rows), 0)
    col_j = lax.broadcasted_iota(jnp.int32, (rows, rows), 1)
    keep = (col_j <= row_i) & (segc_ref[...] == segr_ref[...])
    neg_scr[...] = jnp.where(keep, 0.0, -jnp.inf).astype(jnp.float32)


def _fwd_kernel(c_ref, b_ref, segc_ref, segr_ref, x_ref, cumc_ref, cumr_ref, dtr_ref,
                y_ref, s_scr, neg_scr):
    @pl.when(pl.program_id(0) == 0)
    def _():
        _prologue(c_ref, b_ref, segc_ref, segr_ref, s_scr, neg_scr)

    for k in range(PAIR):
        cc = cumc_ref[0, :, k:k + 1]
        cr = cumr_ref[0, k:k + 1, :]
        dr = dtr_ref[0, k:k + 1, :]
        decays = jnp.exp(cc - cr + neg_scr[...])
        mixing = s_scr[...] * (decays * dr)
        y_ref[:, k * HEAD_DIM:(k + 1) * HEAD_DIM] = _dot(
            mixing, x_ref[:, k * HEAD_DIM:(k + 1) * HEAD_DIM])


def _bwd_kernel(c_ref, b_ref, segc_ref, segr_ref, x_ref, cumc_ref, cumr_ref, dtr_ref, g_ref,
                dx_ref, dcumc_ref, dcumr_ref, ddtr_ref, db_ref, dc_ref,
                s_scr, neg_scr, ds_scr):
    step = pl.program_id(0)

    @pl.when(step == 0)
    def _():
        _prologue(c_ref, b_ref, segc_ref, segr_ref, s_scr, neg_scr)
        ds_scr[...] = jnp.zeros_like(ds_scr)

    for k in range(PAIR):
        cc = cumc_ref[0, :, k:k + 1]
        cr = cumr_ref[0, k:k + 1, :]
        dr = dtr_ref[0, k:k + 1, :]
        decays = jnp.exp(cc - cr + neg_scr[...])
        weights = decays * dr
        scores = s_scr[...]
        mixing = scores * weights
        xh = x_ref[:, k * HEAD_DIM:(k + 1) * HEAD_DIM]
        gh = g_ref[:, k * HEAD_DIM:(k + 1) * HEAD_DIM]
        dx_ref[:, k * HEAD_DIM:(k + 1) * HEAD_DIM] = _dot_tn(mixing, gh)
        d_mix = _dot_nt(gh, xh)
        d_dec = d_mix * decays
        ds_scr[...] += d_dec * dr
        through = d_dec * scores
        d_dt_row = jnp.sum(through, axis=0, keepdims=True)
        q_mat = through * dr
        dcumc_ref[0, :, k:k + 1] = jnp.sum(q_mat, axis=1, keepdims=True)
        dcumr_ref[0, k:k + 1, :] = -(d_dt_row * dr)
        ddtr_ref[0, k:k + 1, :] = d_dt_row

    @pl.when(step == pl.num_programs(0) - 1)
    def _():
        dc_ref[...] = _dot(ds_scr[...], b_ref[...])
        db_ref[...] = _dot_tn(ds_scr[...], c_ref[...])


def _specs(rows, state):
    full = lambda shape: pl.BlockSpec(shape, lambda g: (0,) * len(shape))
    return [
        full((rows, state)),
        full((rows, state)),
        full((rows, 1)),
        full((1, rows)),
        pl.BlockSpec((rows, PAIR * HEAD_DIM), lambda g: (0, g)),
        pl.BlockSpec((1, rows, PAIR), lambda g: (g, 0, 0)),
        pl.BlockSpec((1, PAIR, rows), lambda g: (g, 0, 0)),
        pl.BlockSpec((1, PAIR, rows), lambda g: (g, 0, 0)),
    ]


def _prep(dt, cum, seg):
    rows, heads = dt.shape
    groups = heads // PAIR
    cumr = cum.T.reshape(groups, PAIR, rows)
    cumc = jnp.transpose(cumr, (0, 2, 1))
    dtr = dt.T.reshape(groups, PAIR, rows)
    segc = seg.reshape(rows, 1)
    segr = seg.reshape(1, rows)
    return cumc, cumr, dtr, segc, segr


def _fwd_call(x, dt, cum, b_mat, c_mat, seg):
    rows, inner = x.shape
    heads = dt.shape[1]
    groups = heads // PAIR
    state = b_mat.shape[1]
    cumc, cumr, dtr, segc, segr = _prep(dt, cum, seg)
    flops = 2 * rows * rows * state * 6 + heads * (2 * rows * rows * HEAD_DIM * 6 + 8 * rows * rows)
    return pl.pallas_call(
        _fwd_kernel,
        grid=(groups,),
        in_specs=_specs(rows, state),
        out_specs=pl.BlockSpec((rows, PAIR * HEAD_DIM), lambda g: (0, g)),
        out_shape=jax.ShapeDtypeStruct((rows, inner), jnp.float32),
        scratch_shapes=[pltpu.VMEM((rows, rows), jnp.float32),
                        pltpu.VMEM((rows, rows), jnp.float32)],
        compiler_params=pltpu.CompilerParams(dimension_semantics=("arbitrary",)),
        cost_estimate=pl.CostEstimate(flops=flops, transcendentals=heads * rows * rows,
                                      bytes_accessed=4 * (2 * rows * inner + 2 * rows * state)),
        name="ssd_fwd",
    )(c_mat, b_mat, segc, segr, x, cumc, cumr, dtr)


def _bwd_call(x, dt, cum, b_mat, c_mat, seg, g):
    rows, inner = x.shape
    heads = dt.shape[1]
    groups = heads // PAIR
    state = b_mat.shape[1]
    cumc, cumr, dtr, segc, segr = _prep(dt, cum, seg)
    full = lambda shape: pl.BlockSpec(shape, lambda gi: (0,) * len(shape))
    flops = 2 * rows * rows * state * 6 * 3 + heads * (2 * 2 * rows * rows * HEAD_DIM * 6 + 16 * rows * rows)
    dx, dcumc, dcumr, ddtr, db, dc = pl.pallas_call(
        _bwd_kernel,
        grid=(groups,),
        in_specs=_specs(rows, state) + [pl.BlockSpec((rows, PAIR * HEAD_DIM), lambda gi: (0, gi))],
        out_specs=[
            pl.BlockSpec((rows, PAIR * HEAD_DIM), lambda gi: (0, gi)),
            pl.BlockSpec((1, rows, PAIR), lambda gi: (gi, 0, 0)),
            pl.BlockSpec((1, PAIR, rows), lambda gi: (gi, 0, 0)),
            pl.BlockSpec((1, PAIR, rows), lambda gi: (gi, 0, 0)),
            full((rows, state)),
            full((rows, state)),
        ],
        out_shape=[
            jax.ShapeDtypeStruct((rows, inner), jnp.float32),
            jax.ShapeDtypeStruct((groups, rows, PAIR), jnp.float32),
            jax.ShapeDtypeStruct((groups, PAIR, rows), jnp.float32),
            jax.ShapeDtypeStruct((groups, PAIR, rows), jnp.float32),
            jax.ShapeDtypeStruct((rows, state), jnp.float32),
            jax.ShapeDtypeStruct((rows, state), jnp.float32),
        ],
        scratch_shapes=[pltpu.VMEM((rows, rows), jnp.float32),
                        pltpu.VMEM((rows, rows), jnp.float32),
                        pltpu.VMEM((rows, rows), jnp.float32)],
        compiler_params=pltpu.CompilerParams(dimension_semantics=("arbitrary",)),
        cost_estimate=pl.CostEstimate(flops=flops, transcendentals=heads * rows * rows,
                                      bytes_accessed=4 * (4 * rows * inner + 4 * rows * state)),
        name="ssd_bwd",
    )(c_mat, b_mat, segc, segr, x, cumc, cumr, dtr, g)
    d_cum = jnp.transpose(dcumc, (0, 2, 1)).reshape(heads, rows).T + dcumr.reshape(heads, rows).T
    d_dt = ddtr.reshape(heads, rows).T
    return dx, d_dt, d_cum, db, dc


@jax.custom_vjp
def ssd_core(x, dt, cum, b_mat, c_mat, seg):
    return _fwd_call(x, dt, cum, b_mat, c_mat, seg)


def _ssd_core_fwd(x, dt, cum, b_mat, c_mat, seg):
    return _fwd_call(x, dt, cum, b_mat, c_mat, seg), (x, dt, cum, b_mat, c_mat, seg)


def _ssd_core_bwd(res, g):
    x, dt, cum, b_mat, c_mat, seg = res
    dx, d_dt, d_cum, db, dc = _bwd_call(x, dt, cum, b_mat, c_mat, seg, g)
    return dx, d_dt, d_cum, db, dc, None


ssd_core.defvjp(_ssd_core_fwd, _ssd_core_bwd)

from jax.sharding import PartitionSpec as P
from jax.experimental.layout import Layout, with_layout_constraint

NORM_EPS = 1e-05


def contract_rows(first_op, second_op):
    return lax.dot_general(
        first_op, second_op, (((0,), (0,)), ((), ())), preferred_element_type=jnp.float32
    )


def contract_cols(first_op, second_op):
    return lax.dot_general(
        first_op, second_op, (((1,), (1,)), ((), ())), preferred_element_type=jnp.float32
    )


def segment_ids(lengths, row_count):
    seq_ends = jnp.cumsum(lengths)
    positions = jnp.arange(row_count, dtype=jnp.int32)
    return jnp.sum((positions[:, None] >= seq_ends[None, :]).astype(jnp.int32), axis=1)


def causal_conv(signal, kernel_w, kernel_b, segment):
    kernel_len = kernel_w.shape[0]
    row_count = signal.shape[0]
    summed = kernel_b[None, :] + kernel_w[kernel_len - 1][None, :] * signal
    for lag_steps in range(1, kernel_len):
        shifted = jnp.concatenate(
            [jnp.zeros((lag_steps, signal.shape[1]), jnp.float32), signal[: row_count - lag_steps]],
            axis=0,
        )
        earlier = jnp.concatenate(
            [jnp.full((lag_steps,), -1, jnp.int32), segment[: row_count - lag_steps]]
        )
        same_seq = (earlier == segment).astype(signal.dtype)
        summed = (
            summed + kernel_w[kernel_len - 1 - lag_steps][None, :] * shifted * same_seq[:, None]
        )
    return summed


def mixer_core(zx_rows, dt_raw, b_conv, c_conv, conv_wx, conv_bx, a_log, dt_bias, d_skip,
               segment=None):
    inner_n = zx_rows.shape[1] // 2
    heads_n = a_log.shape[0]
    x_conv = jax.nn.silu(causal_conv(zx_rows[:, inner_n:], conv_wx, conv_bx, segment))
    steps_dt = jax.nn.softplus(dt_raw + dt_bias[None, :])
    decay = steps_dt * (-jnp.exp(a_log))[None, :]
    cum = jnp.cumsum(decay, axis=0)
    scanned = ssd_core(x_conv, steps_dt, cum, b_conv, c_conv, segment)
    skip = jnp.repeat(d_skip, inner_n // heads_n)
    mixed_out = scanned + skip[None, :] * x_conv
    return mixed_out * jax.nn.silu(zx_rows[:, :inner_n])


def bc_core(bc_pre, conv_wbc, conv_bbc, segment=None):
    return jax.nn.silu(causal_conv(bc_pre, conv_wbc, conv_bbc, segment))


def per_device_body(tokens, cotangent, seq_lens, input_norm_gain, w_zx, w_bc, w_dt, conv_wx, conv_bx,
               conv_wbc, conv_bbc, a_log, dt_bias, d_skip, norm_gate, w_out):
    n_dp = lax.axis_size("dp")
    x_full = lax.all_gather(tokens, "tensor", axis=1, tiled=True)
    cot_full = lax.all_gather(cotangent, "tensor", axis=1, tiled=True)
    row_count = tokens.shape[0]
    feat_n = tokens.shape[1]
    d_model = x_full.shape[1]
    feat_start = lax.axis_index("tensor") * feat_n
    state_n = w_bc.shape[1] // 2
    inner_loc = norm_gate.shape[0]
    inner_all = inner_loc * lax.axis_size("tensor")
    segment = segment_ids(seq_lens[0], row_count)
    is_live = (segment < seq_lens.shape[1])[:, None]
    w_zx_flat = w_zx.reshape(d_model, 2 * inner_loc)
    tok_float = x_full.astype(jnp.float32)
    inverse_root_mean = lax.rsqrt(jnp.mean(tok_float * tok_float, axis=1, keepdims=True) + NORM_EPS)
    unit_scaled_input = tok_float * inverse_root_mean
    normed = (unit_scaled_input * input_norm_gain[None, :]).astype(jnp.bfloat16)
    zx_rows = jnp.dot(normed, w_zx_flat, preferred_element_type=jnp.float32)
    bc_pre = jnp.dot(normed, w_bc, preferred_element_type=jnp.float32)
    dt_raw = jnp.dot(normed, w_dt, preferred_element_type=jnp.float32)
    bc_post, bc_back = jax.vjp(partial(bc_core, segment=segment), bc_pre, conv_wbc, conv_bbc)
    gated_rows, core_back = jax.vjp(
        partial(mixer_core, segment=segment),
        zx_rows, dt_raw, bc_post[:, :state_n], bc_post[:, state_n:],
        conv_wx, conv_bx, a_log, dt_bias, d_skip,
    )
    cot_live = jnp.where(is_live, cot_full, jnp.zeros_like(cot_full))
    d_gate = contract_cols(cot_live, w_out)
    d_hat = d_gate * norm_gate[None, :]
    stats = lax.psum(
        jnp.concatenate([jnp.sum(gated_rows * gated_rows, axis=1, keepdims=True),
                         jnp.sum(d_hat * gated_rows, axis=1, keepdims=True)], axis=1),
        "tensor")
    squares, cross_sum = stats[:, 0:1], stats[:, 1:2]
    r_gate = lax.rsqrt(squares / inner_all + NORM_EPS)
    gate_hat = gated_rows * r_gate
    gate_out = (gate_hat * norm_gate[None, :]).astype(jnp.bfloat16)
    branch_part = jnp.dot(gate_out, w_out, preferred_element_type=jnp.float32)
    grad_gate = jnp.sum(d_gate * gate_hat, axis=0)
    d_gated = r_gate * d_hat - gated_rows * (r_gate * r_gate * r_gate * cross_sum / inner_all)
    d_gated, branch_part = lax.optimization_barrier((d_gated, branch_part))
    branch = lax.psum_scatter(branch_part, "tensor", scatter_dimension=1, tiled=True)
    own_float = tokens.astype(jnp.float32)
    block_out = (own_float + jnp.where(is_live, branch, 0.0)).astype(jnp.bfloat16)
    d_zx, d_dt, d_b, d_c, grad_conv_wx, grad_conv_bx, grad_a_log, grad_dt_bias, grad_d_skip = (
        core_back(d_gated)
    )
    n_tp = lax.axis_size("tensor")
    chunk = d_model // n_dp
    row_major = Layout(major_to_minor=(0, 1))
    d_zx_half = d_zx.astype(jnp.bfloat16)
    d_dt_half = d_dt.astype(jnp.bfloat16)
    grad_out_t = contract_rows(cot_live, gate_out)
    grad_z = contract_rows(normed, d_zx_half[:, :inner_loc])
    (grad_out_t_sum, grad_z_sum), (grad_gate_sum,) = pack_reduce(
        [grad_out_t, grad_z], [grad_gate], chunk, n_dp, row_major)
    d_zx, d_dt, block_out, grad_z_sum = lax.optimization_barrier(
        (d_zx, d_dt, block_out, grad_z_sum))
    d_zx_half = d_zx.astype(jnp.bfloat16)
    d_dt_half = d_dt.astype(jnp.bfloat16)
    d_bc_part = jnp.concatenate([d_b, d_c], axis=1)
    partial_in = contract_cols(d_zx_half, w_zx_flat) + contract_cols(d_dt_half, w_dt)
    bc_w = d_bc_part.shape[1]
    rs_in = jnp.concatenate(
        [partial_in.reshape(row_count, n_tp, feat_n),
         jnp.broadcast_to(d_bc_part[:, None, :], (row_count, n_tp, bc_w))], axis=2,
    ).reshape(row_count, n_tp * (feat_n + bc_w))
    rs_out = lax.psum_scatter(rs_in, "tensor", scatter_dimension=1, tiled=True)
    d_bc_post = rs_out[:, feat_n:]
    d_bc, grad_conv_wbc, grad_conv_bbc = bc_back(d_bc_post)
    d_bc_half = d_bc.astype(jnp.bfloat16)
    own_hat = lax.dynamic_slice_in_dim(unit_scaled_input, feat_start, feat_n, 1)
    own_gain = lax.dynamic_slice_in_dim(input_norm_gain, feat_start, feat_n, 0)
    own_w_bc = lax.dynamic_slice_in_dim(w_bc, feat_start, feat_n, 0)
    own_dn = rs_out[:, :feat_n] + contract_cols(d_bc_half, own_w_bc)
    own_dxhat = own_dn * own_gain[None, :]
    row_inner_product = lax.psum(jnp.sum(own_dxhat * own_hat, axis=1, keepdims=True),
                                 "tensor") / d_model
    grad_in = jnp.sum(own_dn * own_hat, axis=0)
    d_tokens = cotangent.astype(jnp.float32) + inverse_root_mean * (
        own_dxhat - own_hat * row_inner_product
    )
    grads_late = contract_rows(
        normed, jnp.concatenate([d_zx_half[:, inner_loc:], d_bc_half, d_dt_half], axis=1))
    late_smalls = (grad_conv_wx, grad_conv_bx, grad_conv_wbc, grad_conv_bbc, grad_a_log,
                   grad_dt_bias, grad_d_skip, grad_in)
    (grad_late_sum,), late_sums = pack_reduce([grads_late], late_smalls, chunk, n_dp,
                                              row_major)
    grad_x_sum = grad_late_sum[:, :inner_loc]
    grad_bc_sum = grad_late_sum[:, inner_loc:inner_loc + 2 * state_n]
    grad_dt_sum = grad_late_sum[:, inner_loc + 2 * state_n:]
    grad_zx_out = jnp.stack([grad_z_sum, grad_x_sum], axis=1)
    return (block_out, d_tokens, grad_zx_out, grad_bc_sum, grad_dt_sum, grad_out_t_sum.T,
            *late_sums[:7], grad_gate_sum, late_sums[7])


def pack_reduce(mats, smalls, chunk, n_dp, row_major):
    flat_small = jnp.concatenate([v.reshape(-1) for v in smalls])
    small_cols = -(-flat_small.shape[0] // chunk)
    small_block = jnp.pad(flat_small, (0, small_cols * chunk - flat_small.shape[0])).reshape(
        chunk, small_cols)
    packed = with_layout_constraint(
        jnp.concatenate([with_layout_constraint(m, row_major) for m in mats]
                        + [jnp.tile(small_block, (n_dp, 1))], axis=1), row_major)
    reduced = lax.psum_scatter(packed, "dp", scatter_dimension=0, tiled=True)
    col = 0
    pieces = []
    for m in mats:
        pieces.append(reduced[:, col:col + m.shape[1]])
        col += m.shape[1]
    small_sum = reduced[:, col:].reshape(-1)
    outs = []
    pos = 0
    for v in smalls:
        outs.append(small_sum[pos:pos + v.size].reshape(v.shape))
        pos += v.size
    return pieces, outs


def solution(mesh):
    in_specs = (
        P("dp", "tensor"), P("dp", "tensor"), P("dp", None), P(),
        P(None, None, "tensor"), P(), P(None, "tensor"), P(None, "tensor"), P("tensor"),
        P(), P(), P("tensor"), P("tensor"), P("tensor"), P("tensor"), P("tensor", None),
    )
    out_specs = (
        P("dp", "tensor"), P("dp", "tensor"), P("dp", None, "tensor"), P("dp", None),
        P("dp", "tensor"), P("tensor", "dp"), P(None, "tensor"), P("tensor"), P(), P(),
        P("tensor"), P("tensor"), P("tensor"), P("tensor"), P("tensor"),
    )
    return jax.shard_map(
        per_device_body, mesh=mesh, in_specs=in_specs, out_specs=out_specs, check_vma=False
    )
```

```python
from functools import partial


import jax
import jax.numpy as jnp
from jax import lax
from jax.experimental import pallas as pl
from jax.experimental.pallas import tpu as pltpu

PRECISE = lax.Precision.HIGHEST
HEAD_DIM = 64
PAIR = 2


def _dot(a, b):
    return jnp.dot(a, b, precision=PRECISE, preferred_element_type=jnp.float32)


def _dot_tn(a, b):
    return lax.dot_general(a, b, (((0,), (0,)), ((), ())), precision=PRECISE,
                           preferred_element_type=jnp.float32)


def _dot_nt(a, b):
    return lax.dot_general(a, b, (((1,), (1,)), ((), ())), precision=PRECISE,
                           preferred_element_type=jnp.float32)


def _prologue(c_ref, b_ref, segc_ref, segr_ref, s_scr, neg_scr):
    s_scr[...] = _dot_nt(c_ref[...], b_ref[...])
    rows = s_scr.shape[0]
    row_i = lax.broadcasted_iota(jnp.int32, (rows, rows), 0)
    col_j = lax.broadcasted_iota(jnp.int32, (rows, rows), 1)
    keep = (col_j <= row_i) & (segc_ref[...] == segr_ref[...])
    neg_scr[...] = jnp.where(keep, 0.0, -jnp.inf).astype(jnp.float32)


def _fwd_kernel(c_ref, b_ref, segc_ref, segr_ref, x_ref, cumc_ref, cumr_ref, dtr_ref,
                y_ref, s_scr, neg_scr):
    @pl.when(pl.program_id(0) == 0)
    def _():
        _prologue(c_ref, b_ref, segc_ref, segr_ref, s_scr, neg_scr)

    for k in range(PAIR):
        cc = cumc_ref[0, :, k:k + 1]
        cr = cumr_ref[0, k:k + 1, :]
        dr = dtr_ref[0, k:k + 1, :]
        decays = jnp.exp(cc - cr + neg_scr[...])
        mixing = s_scr[...] * (decays * dr)
        y_ref[:, k * HEAD_DIM:(k + 1) * HEAD_DIM] = _dot(
            mixing, x_ref[:, k * HEAD_DIM:(k + 1) * HEAD_DIM])


def _bwd_kernel(c_ref, b_ref, segc_ref, segr_ref, x_ref, cumc_ref, cumr_ref, dtr_ref, g_ref,
                dx_ref, dcumc_ref, dcumr_ref, ddtr_ref, db_ref, dc_ref,
                s_scr, neg_scr, ds_scr):
    step = pl.program_id(0)

    @pl.when(step == 0)
    def _():
        _prologue(c_ref, b_ref, segc_ref, segr_ref, s_scr, neg_scr)
        ds_scr[...] = jnp.zeros_like(ds_scr)

    for k in range(PAIR):
        cc = cumc_ref[0, :, k:k + 1]
        cr = cumr_ref[0, k:k + 1, :]
        dr = dtr_ref[0, k:k + 1, :]
        decays = jnp.exp(cc - cr + neg_scr[...])
        weights = decays * dr
        scores = s_scr[...]
        mixing = scores * weights
        xh = x_ref[:, k * HEAD_DIM:(k + 1) * HEAD_DIM]
        gh = g_ref[:, k * HEAD_DIM:(k + 1) * HEAD_DIM]
        dx_ref[:, k * HEAD_DIM:(k + 1) * HEAD_DIM] = _dot_tn(mixing, gh)
        d_mix = _dot_nt(gh, xh)
        d_dec = d_mix * decays
        ds_scr[...] += d_dec * dr
        through = d_dec * scores
        d_dt_row = jnp.sum(through, axis=0, keepdims=True)
        q_mat = through * dr
        dcumc_ref[0, :, k:k + 1] = jnp.sum(q_mat, axis=1, keepdims=True)
        dcumr_ref[0, k:k + 1, :] = -(d_dt_row * dr)
        ddtr_ref[0, k:k + 1, :] = d_dt_row

    @pl.when(step == pl.num_programs(0) - 1)
    def _():
        dc_ref[...] = _dot(ds_scr[...], b_ref[...])
        db_ref[...] = _dot_tn(ds_scr[...], c_ref[...])


def _specs(rows, state):
    full = lambda shape: pl.BlockSpec(shape, lambda g: (0,) * len(shape))
    return [
        full((rows, state)),
        full((rows, state)),
        full((rows, 1)),
        full((1, rows)),
        pl.BlockSpec((rows, PAIR * HEAD_DIM), lambda g: (0, g)),
        pl.BlockSpec((1, rows, PAIR), lambda g: (g, 0, 0)),
        pl.BlockSpec((1, PAIR, rows), lambda g: (g, 0, 0)),
        pl.BlockSpec((1, PAIR, rows), lambda g: (g, 0, 0)),
    ]


def _prep(dt, cum, seg):
    rows, heads = dt.shape
    groups = heads // PAIR
    cumr = cum.T.reshape(groups, PAIR, rows)
    cumc = jnp.transpose(cumr, (0, 2, 1))
    dtr = dt.T.reshape(groups, PAIR, rows)
    segc = seg.reshape(rows, 1)
    segr = seg.reshape(1, rows)
    return cumc, cumr, dtr, segc, segr


def _fwd_call(x, dt, cum, b_mat, c_mat, seg):
    rows, inner = x.shape
    heads = dt.shape[1]
    groups = heads // PAIR
    state = b_mat.shape[1]
    cumc, cumr, dtr, segc, segr = _prep(dt, cum, seg)
    flops = 2 * rows * rows * state * 6 + heads * (2 * rows * rows * HEAD_DIM * 6 + 8 * rows * rows)
    return pl.pallas_call(
        _fwd_kernel,
        grid=(groups,),
        in_specs=_specs(rows, state),
        out_specs=pl.BlockSpec((rows, PAIR * HEAD_DIM), lambda g: (0, g)),
        out_shape=jax.ShapeDtypeStruct((rows, inner), jnp.float32),
        scratch_shapes=[pltpu.VMEM((rows, rows), jnp.float32),
                        pltpu.VMEM((rows, rows), jnp.float32)],
        compiler_params=pltpu.CompilerParams(dimension_semantics=("arbitrary",)),
        cost_estimate=pl.CostEstimate(flops=flops, transcendentals=heads * rows * rows,
                                      bytes_accessed=4 * (2 * rows * inner + 2 * rows * state)),
        name="ssd_fwd",
    )(c_mat, b_mat, segc, segr, x, cumc, cumr, dtr)


def _bwd_call(x, dt, cum, b_mat, c_mat, seg, g):
    rows, inner = x.shape
    heads = dt.shape[1]
    groups = heads // PAIR
    state = b_mat.shape[1]
    cumc, cumr, dtr, segc, segr = _prep(dt, cum, seg)
    full = lambda shape: pl.BlockSpec(shape, lambda gi: (0,) * len(shape))
    flops = 2 * rows * rows * state * 6 * 3 + heads * (2 * 2 * rows * rows * HEAD_DIM * 6 + 16 * rows * rows)
    dx, dcumc, dcumr, ddtr, db, dc = pl.pallas_call(
        _bwd_kernel,
        grid=(groups,),
        in_specs=_specs(rows, state) + [pl.BlockSpec((rows, PAIR * HEAD_DIM), lambda gi: (0, gi))],
        out_specs=[
            pl.BlockSpec((rows, PAIR * HEAD_DIM), lambda gi: (0, gi)),
            pl.BlockSpec((1, rows, PAIR), lambda gi: (gi, 0, 0)),
            pl.BlockSpec((1, PAIR, rows), lambda gi: (gi, 0, 0)),
            pl.BlockSpec((1, PAIR, rows), lambda gi: (gi, 0, 0)),
            full((rows, state)),
            full((rows, state)),
        ],
        out_shape=[
            jax.ShapeDtypeStruct((rows, inner), jnp.float32),
            jax.ShapeDtypeStruct((groups, rows, PAIR), jnp.float32),
            jax.ShapeDtypeStruct((groups, PAIR, rows), jnp.float32),
            jax.ShapeDtypeStruct((groups, PAIR, rows), jnp.float32),
            jax.ShapeDtypeStruct((rows, state), jnp.float32),
            jax.ShapeDtypeStruct((rows, state), jnp.float32),
        ],
        scratch_shapes=[pltpu.VMEM((rows, rows), jnp.float32),
                        pltpu.VMEM((rows, rows), jnp.float32),
                        pltpu.VMEM((rows, rows), jnp.float32)],
        compiler_params=pltpu.CompilerParams(dimension_semantics=("arbitrary",)),
        cost_estimate=pl.CostEstimate(flops=flops, transcendentals=heads * rows * rows,
                                      bytes_accessed=4 * (4 * rows * inner + 4 * rows * state)),
        name="ssd_bwd",
    )(c_mat, b_mat, segc, segr, x, cumc, cumr, dtr, g)
    d_cum = jnp.transpose(dcumc, (0, 2, 1)).reshape(heads, rows).T + dcumr.reshape(heads, rows).T
    d_dt = ddtr.reshape(heads, rows).T
    return dx, d_dt, d_cum, db, dc


@jax.custom_vjp
def ssd_core(x, dt, cum, b_mat, c_mat, seg):
    return _fwd_call(x, dt, cum, b_mat, c_mat, seg)


def _ssd_core_fwd(x, dt, cum, b_mat, c_mat, seg):
    return _fwd_call(x, dt, cum, b_mat, c_mat, seg), (x, dt, cum, b_mat, c_mat, seg)


def _ssd_core_bwd(res, g):
    x, dt, cum, b_mat, c_mat, seg = res
    dx, d_dt, d_cum, db, dc = _bwd_call(x, dt, cum, b_mat, c_mat, seg, g)
    return dx, d_dt, d_cum, db, dc, None


ssd_core.defvjp(_ssd_core_fwd, _ssd_core_bwd)

from jax.sharding import PartitionSpec as P
from jax.experimental.layout import Layout, with_layout_constraint

NORM_EPS = 1e-05


def contract_rows(first_op, second_op):
    return lax.dot_general(
        first_op, second_op, (((0,), (0,)), ((), ())), preferred_element_type=jnp.float32
    )


def contract_cols(first_op, second_op):
    return lax.dot_general(
        first_op, second_op, (((1,), (1,)), ((), ())), preferred_element_type=jnp.float32
    )


def segment_ids(lengths, row_count):
    seq_ends = jnp.cumsum(lengths)
    positions = jnp.arange(row_count, dtype=jnp.int32)
    return jnp.sum((positions[:, None] >= seq_ends[None, :]).astype(jnp.int32), axis=1)


def causal_conv(signal, kernel_w, kernel_b, segment):
    kernel_len = kernel_w.shape[0]
    row_count = signal.shape[0]
    summed = kernel_b[None, :] + kernel_w[kernel_len - 1][None, :] * signal
    for lag_steps in range(1, kernel_len):
        shifted = jnp.concatenate(
            [jnp.zeros((lag_steps, signal.shape[1]), jnp.float32), signal[: row_count - lag_steps]],
            axis=0,
        )
        earlier = jnp.concatenate(
            [jnp.full((lag_steps,), -1, jnp.int32), segment[: row_count - lag_steps]]
        )
        same_seq = (earlier == segment).astype(signal.dtype)
        summed = (
            summed + kernel_w[kernel_len - 1 - lag_steps][None, :] * shifted * same_seq[:, None]
        )
    return summed


def mixer_core(zx_rows, dt_raw, b_conv, c_conv, conv_wx, conv_bx, a_log, dt_bias, d_skip,
               segment=None):
    inner_n = zx_rows.shape[1] // 2
    heads_n = a_log.shape[0]
    x_conv = jax.nn.silu(causal_conv(zx_rows[:, inner_n:], conv_wx, conv_bx, segment))
    steps_dt = jax.nn.softplus(dt_raw + dt_bias[None, :])
    decay = steps_dt * (-jnp.exp(a_log))[None, :]
    cum = jnp.cumsum(decay, axis=0)
    scanned = ssd_core(x_conv, steps_dt, cum, b_conv, c_conv, segment)
    skip = jnp.repeat(d_skip, inner_n // heads_n)
    mixed_out = scanned + skip[None, :] * x_conv
    return mixed_out * jax.nn.silu(zx_rows[:, :inner_n])


def bc_core(bc_pre, conv_wbc, conv_bbc, segment=None):
    return jax.nn.silu(causal_conv(bc_pre, conv_wbc, conv_bbc, segment))


def per_device_body(tokens, cotangent, seq_lens, input_norm_gain, w_zx, w_bc, w_dt, conv_wx, conv_bx,
               conv_wbc, conv_bbc, a_log, dt_bias, d_skip, norm_gate, w_out):
    n_dp = lax.axis_size("dp")
    x_full = lax.all_gather(tokens, "tensor", axis=1, tiled=True)
    cot_full = lax.all_gather(cotangent, "tensor", axis=1, tiled=True)
    row_count = tokens.shape[0]
    feat_n = tokens.shape[1]
    d_model = x_full.shape[1]
    feat_start = lax.axis_index("tensor") * feat_n
    state_n = w_bc.shape[1] // 2
    inner_loc = norm_gate.shape[0]
    inner_all = inner_loc * lax.axis_size("tensor")
    segment = segment_ids(seq_lens[0], row_count)
    is_live = (segment < seq_lens.shape[1])[:, None]
    w_zx_flat = w_zx.reshape(d_model, 2 * inner_loc)
    tok_float = x_full.astype(jnp.float32)
    inverse_root_mean = lax.rsqrt(jnp.mean(tok_float * tok_float, axis=1, keepdims=True) + NORM_EPS)
    unit_scaled_input = tok_float * inverse_root_mean
    normed = (unit_scaled_input * input_norm_gain[None, :]).astype(jnp.bfloat16)
    zx_rows = jnp.dot(normed, w_zx_flat, preferred_element_type=jnp.float32)
    bc_pre = jnp.dot(normed, w_bc, preferred_element_type=jnp.float32)
    dt_raw = jnp.dot(normed, w_dt, preferred_element_type=jnp.float32)
    bc_post, bc_back = jax.vjp(partial(bc_core, segment=segment), bc_pre, conv_wbc, conv_bbc)
    gated_rows, core_back = jax.vjp(
        partial(mixer_core, segment=segment),
        zx_rows, dt_raw, bc_post[:, :state_n], bc_post[:, state_n:],
        conv_wx, conv_bx, a_log, dt_bias, d_skip,
    )
    cot_live = jnp.where(is_live, cot_full, jnp.zeros_like(cot_full))
    d_gate = contract_cols(cot_live, w_out)
    d_hat = d_gate * norm_gate[None, :]
    stats = lax.psum(
        jnp.concatenate([jnp.sum(gated_rows * gated_rows, axis=1, keepdims=True),
                         jnp.sum(d_hat * gated_rows, axis=1, keepdims=True)], axis=1),
        "tensor")
    squares, cross_sum = stats[:, 0:1], stats[:, 1:2]
    r_gate = lax.rsqrt(squares / inner_all + NORM_EPS)
    gate_hat = gated_rows * r_gate
    gate_out = (gate_hat * norm_gate[None, :]).astype(jnp.bfloat16)
    branch_part = jnp.dot(gate_out, w_out, preferred_element_type=jnp.float32)
    grad_gate = jnp.sum(d_gate * gate_hat, axis=0)
    d_gated = r_gate * d_hat - gated_rows * (r_gate * r_gate * r_gate * cross_sum / inner_all)
    d_gated, branch_part = lax.optimization_barrier((d_gated, branch_part))
    branch = lax.psum_scatter(branch_part, "tensor", scatter_dimension=1, tiled=True)
    own_float = tokens.astype(jnp.float32)
    block_out = (own_float + jnp.where(is_live, branch, 0.0)).astype(jnp.bfloat16)
    d_zx, d_dt, d_b, d_c, grad_conv_wx, grad_conv_bx, grad_a_log, grad_dt_bias, grad_d_skip = (
        core_back(d_gated)
    )
    n_tp = lax.axis_size("tensor")
    chunk = d_model // n_dp
    row_major = Layout(major_to_minor=(0, 1))
    d_zx, d_dt, block_out = lax.optimization_barrier((d_zx, d_dt, block_out))
    d_zx_half = d_zx.astype(jnp.bfloat16)
    d_dt_half = d_dt.astype(jnp.bfloat16)
    grads_big = with_layout_constraint(jnp.concatenate(
        [with_layout_constraint(contract_rows(cot_live, gate_out), row_major),
         with_layout_constraint(contract_rows(normed, d_zx_half), row_major)], axis=1), row_major)
    big_sum = halving_reduce_scatter(grads_big, n_dp)
    d_bc_part = jnp.concatenate([d_b, d_c], axis=1)
    partial_in = contract_cols(d_zx_half, w_zx_flat) + contract_cols(d_dt_half, w_dt)
    bc_w = d_bc_part.shape[1]
    rs_in = jnp.concatenate(
        [partial_in.reshape(row_count, n_tp, feat_n),
         jnp.broadcast_to(d_bc_part[:, None, :], (row_count, n_tp, bc_w))], axis=2,
    ).reshape(row_count, n_tp * (feat_n + bc_w))
    rs_out = lax.psum_scatter(rs_in, "tensor", scatter_dimension=1, tiled=True)
    d_bc_post = rs_out[:, feat_n:]
    d_bc, grad_conv_wbc, grad_conv_bbc = bc_back(d_bc_post)
    d_bc_half = d_bc.astype(jnp.bfloat16)
    own_hat = lax.dynamic_slice_in_dim(unit_scaled_input, feat_start, feat_n, 1)
    own_gain = lax.dynamic_slice_in_dim(input_norm_gain, feat_start, feat_n, 0)
    own_w_bc = lax.dynamic_slice_in_dim(w_bc, feat_start, feat_n, 0)
    own_dn = rs_out[:, :feat_n] + contract_cols(d_bc_half, own_w_bc)
    own_dxhat = own_dn * own_gain[None, :]
    row_inner_product = lax.psum(jnp.sum(own_dxhat * own_hat, axis=1, keepdims=True),
                                 "tensor") / d_model
    grad_in = jnp.sum(own_dn * own_hat, axis=0)
    d_tokens = cotangent.astype(jnp.float32) + inverse_root_mean * (
        own_dxhat - own_hat * row_inner_product
    )
    smalls = (grad_conv_wx, grad_conv_bx, grad_conv_wbc, grad_conv_bbc, grad_a_log,
              grad_dt_bias, grad_d_skip, grad_gate, grad_in)
    flat_small = jnp.concatenate([v.reshape(-1) for v in smalls])
    small_cols = -(-flat_small.shape[0] // chunk)
    small_block = jnp.pad(flat_small, (0, small_cols * chunk - flat_small.shape[0])).reshape(
        chunk, small_cols)
    grads_small = with_layout_constraint(jnp.concatenate(
        [with_layout_constraint(
            contract_rows(normed, jnp.concatenate([d_bc_half, d_dt_half], axis=1)), row_major),
         jnp.tile(small_block, (n_dp, 1))], axis=1), row_major)
    small_sum_all = halving_reduce_scatter(grads_small, n_dp)
    grad_out_t_sum = big_sum[:, :inner_loc]
    grad_zx_sum = big_sum[:, inner_loc:]
    grad_bc_sum = small_sum_all[:, :2 * state_n]
    grad_dt_sum = small_sum_all[:, 2 * state_n:2 * state_n + w_dt.shape[1]]
    small_sum = small_sum_all[:, 2 * state_n + w_dt.shape[1]:].reshape(-1)
    outs_small = []
    pos = 0
    for v in smalls:
        outs_small.append(small_sum[pos:pos + v.size].reshape(v.shape))
        pos += v.size
    grad_zx_out = grad_zx_sum.reshape(chunk, 2, inner_loc)
    return (block_out, d_tokens, grad_zx_out, grad_bc_sum, grad_dt_sum, grad_out_t_sum.T,
            *outs_small)


def halving_reduce_scatter(x, n_dev):
    me = lax.axis_index("dp")
    chunk = x.shape[0] // n_dev
    cur = x.reshape(n_dev, chunk, x.shape[1])
    bit = 0
    while (1 << bit) < n_dev:
        pairs = cur.reshape(cur.shape[0] // 2, 2, chunk, x.shape[1])
        mine = (me >> bit) & 1
        keep = lax.dynamic_index_in_dim(pairs, mine, axis=1, keepdims=False)
        send = lax.dynamic_index_in_dim(pairs, 1 - mine, axis=1, keepdims=False)
        got = lax.ppermute(send, "dp", [(i, i ^ (1 << bit)) for i in range(n_dev)])
        cur = keep + got
        bit += 1
    return cur.reshape(chunk, x.shape[1])


def solution(mesh):
    in_specs = (
        P("dp", "tensor"), P("dp", "tensor"), P("dp", None), P(),
        P(None, None, "tensor"), P(), P(None, "tensor"), P(None, "tensor"), P("tensor"),
        P(), P(), P("tensor"), P("tensor"), P("tensor"), P("tensor"), P("tensor", None),
    )
    out_specs = (
        P("dp", "tensor"), P("dp", "tensor"), P("dp", None, "tensor"), P("dp", None),
        P("dp", "tensor"), P("tensor", "dp"), P(None, "tensor"), P("tensor"), P(), P(),
        P("tensor"), P("tensor"), P("tensor"), P("tensor"), P("tensor"),
    )
    return jax.shard_map(
        per_device_body, mesh=mesh, in_specs=in_specs, out_specs=out_specs, check_vma=False
    )
```

```python
from functools import partial


import jax
import jax.numpy as jnp
from jax import lax
from jax.experimental import pallas as pl
from jax.experimental.pallas import tpu as pltpu

PRECISE = lax.Precision.HIGHEST
HEAD_DIM = 64
PAIR = 2


def _dot(a, b):
    return jnp.dot(a, b, precision=PRECISE, preferred_element_type=jnp.float32)


def _dot_tn(a, b):
    return lax.dot_general(a, b, (((0,), (0,)), ((), ())), precision=PRECISE,
                           preferred_element_type=jnp.float32)


def _dot_nt(a, b):
    return lax.dot_general(a, b, (((1,), (1,)), ((), ())), precision=PRECISE,
                           preferred_element_type=jnp.float32)


def _prologue(c_ref, b_ref, segc_ref, segr_ref, s_scr, neg_scr):
    s_scr[...] = _dot_nt(c_ref[...], b_ref[...])
    rows = s_scr.shape[0]
    row_i = lax.broadcasted_iota(jnp.int32, (rows, rows), 0)
    col_j = lax.broadcasted_iota(jnp.int32, (rows, rows), 1)
    keep = (col_j <= row_i) & (segc_ref[...] == segr_ref[...])
    neg_scr[...] = jnp.where(keep, 0.0, -jnp.inf).astype(jnp.float32)


def _fwd_kernel(c_ref, b_ref, segc_ref, segr_ref, x_ref, cumc_ref, cumr_ref, dtr_ref,
                y_ref, s_scr, neg_scr):
    @pl.when(pl.program_id(0) == 0)
    def _():
        _prologue(c_ref, b_ref, segc_ref, segr_ref, s_scr, neg_scr)

    for k in range(PAIR):
        cc = cumc_ref[0, :, k:k + 1]
        cr = cumr_ref[0, k:k + 1, :]
        dr = dtr_ref[0, k:k + 1, :]
        decays = jnp.exp(cc - cr + neg_scr[...])
        mixing = s_scr[...] * (decays * dr)
        y_ref[:, k * HEAD_DIM:(k + 1) * HEAD_DIM] = _dot(
            mixing, x_ref[:, k * HEAD_DIM:(k + 1) * HEAD_DIM])


def _bwd_kernel(c_ref, b_ref, segc_ref, segr_ref, x_ref, cumc_ref, cumr_ref, dtr_ref, g_ref,
                dx_ref, dcumc_ref, dcumr_ref, ddtr_ref, db_ref, dc_ref,
                s_scr, neg_scr, ds_scr):
    step = pl.program_id(0)

    @pl.when(step == 0)
    def _():
        _prologue(c_ref, b_ref, segc_ref, segr_ref, s_scr, neg_scr)
        ds_scr[...] = jnp.zeros_like(ds_scr)

    for k in range(PAIR):
        cc = cumc_ref[0, :, k:k + 1]
        cr = cumr_ref[0, k:k + 1, :]
        dr = dtr_ref[0, k:k + 1, :]
        decays = jnp.exp(cc - cr + neg_scr[...])
        weights = decays * dr
        scores = s_scr[...]
        mixing = scores * weights
        xh = x_ref[:, k * HEAD_DIM:(k + 1) * HEAD_DIM]
        gh = g_ref[:, k * HEAD_DIM:(k + 1) * HEAD_DIM]
        dx_ref[:, k * HEAD_DIM:(k + 1) * HEAD_DIM] = _dot_tn(mixing, gh)
        d_mix = _dot_nt(gh, xh)
        d_dec = d_mix * decays
        ds_scr[...] += d_dec * dr
        through = d_dec * scores
        d_dt_row = jnp.sum(through, axis=0, keepdims=True)
        q_mat = through * dr
        dcumc_ref[0, :, k:k + 1] = jnp.sum(q_mat, axis=1, keepdims=True)
        dcumr_ref[0, k:k + 1, :] = -(d_dt_row * dr)
        ddtr_ref[0, k:k + 1, :] = d_dt_row

    @pl.when(step == pl.num_programs(0) - 1)
    def _():
        dc_ref[...] = _dot(ds_scr[...], b_ref[...])
        db_ref[...] = _dot_tn(ds_scr[...], c_ref[...])


def _specs(rows, state):
    full = lambda shape: pl.BlockSpec(shape, lambda g: (0,) * len(shape))
    return [
        full((rows, state)),
        full((rows, state)),
        full((rows, 1)),
        full((1, rows)),
        pl.BlockSpec((rows, PAIR * HEAD_DIM), lambda g: (0, g)),
        pl.BlockSpec((1, rows, PAIR), lambda g: (g, 0, 0)),
        pl.BlockSpec((1, PAIR, rows), lambda g: (g, 0, 0)),
        pl.BlockSpec((1, PAIR, rows), lambda g: (g, 0, 0)),
    ]


def _prep(dt, cum, seg):
    rows, heads = dt.shape
    groups = heads // PAIR
    cumr = cum.T.reshape(groups, PAIR, rows)
    cumc = jnp.transpose(cumr, (0, 2, 1))
    dtr = dt.T.reshape(groups, PAIR, rows)
    segc = seg.reshape(rows, 1)
    segr = seg.reshape(1, rows)
    return cumc, cumr, dtr, segc, segr


def _fwd_call(x, dt, cum, b_mat, c_mat, seg):
    rows, inner = x.shape
    heads = dt.shape[1]
    groups = heads // PAIR
    state = b_mat.shape[1]
    cumc, cumr, dtr, segc, segr = _prep(dt, cum, seg)
    flops = 2 * rows * rows * state * 6 + heads * (2 * rows * rows * HEAD_DIM * 6 + 8 * rows * rows)
    return pl.pallas_call(
        _fwd_kernel,
        grid=(groups,),
        in_specs=_specs(rows, state),
        out_specs=pl.BlockSpec((rows, PAIR * HEAD_DIM), lambda g: (0, g)),
        out_shape=jax.ShapeDtypeStruct((rows, inner), jnp.float32),
        scratch_shapes=[pltpu.VMEM((rows, rows), jnp.float32),
                        pltpu.VMEM((rows, rows), jnp.float32)],
        compiler_params=pltpu.CompilerParams(dimension_semantics=("arbitrary",)),
        cost_estimate=pl.CostEstimate(flops=flops, transcendentals=heads * rows * rows,
                                      bytes_accessed=4 * (2 * rows * inner + 2 * rows * state)),
        name="ssd_fwd",
    )(c_mat, b_mat, segc, segr, x, cumc, cumr, dtr)


def _bwd_call(x, dt, cum, b_mat, c_mat, seg, g):
    rows, inner = x.shape
    heads = dt.shape[1]
    groups = heads // PAIR
    state = b_mat.shape[1]
    cumc, cumr, dtr, segc, segr = _prep(dt, cum, seg)
    full = lambda shape: pl.BlockSpec(shape, lambda gi: (0,) * len(shape))
    flops = 2 * rows * rows * state * 6 * 3 + heads * (2 * 2 * rows * rows * HEAD_DIM * 6 + 16 * rows * rows)
    dx, dcumc, dcumr, ddtr, db, dc = pl.pallas_call(
        _bwd_kernel,
        grid=(groups,),
        in_specs=_specs(rows, state) + [pl.BlockSpec((rows, PAIR * HEAD_DIM), lambda gi: (0, gi))],
        out_specs=[
            pl.BlockSpec((rows, PAIR * HEAD_DIM), lambda gi: (0, gi)),
            pl.BlockSpec((1, rows, PAIR), lambda gi: (gi, 0, 0)),
            pl.BlockSpec((1, PAIR, rows), lambda gi: (gi, 0, 0)),
            pl.BlockSpec((1, PAIR, rows), lambda gi: (gi, 0, 0)),
            full((rows, state)),
            full((rows, state)),
        ],
        out_shape=[
            jax.ShapeDtypeStruct((rows, inner), jnp.float32),
            jax.ShapeDtypeStruct((groups, rows, PAIR), jnp.float32),
            jax.ShapeDtypeStruct((groups, PAIR, rows), jnp.float32),
            jax.ShapeDtypeStruct((groups, PAIR, rows), jnp.float32),
            jax.ShapeDtypeStruct((rows, state), jnp.float32),
            jax.ShapeDtypeStruct((rows, state), jnp.float32),
        ],
        scratch_shapes=[pltpu.VMEM((rows, rows), jnp.float32),
                        pltpu.VMEM((rows, rows), jnp.float32),
                        pltpu.VMEM((rows, rows), jnp.float32)],
        compiler_params=pltpu.CompilerParams(dimension_semantics=("arbitrary",)),
        cost_estimate=pl.CostEstimate(flops=flops, transcendentals=heads * rows * rows,
                                      bytes_accessed=4 * (4 * rows * inner + 4 * rows * state)),
        name="ssd_bwd",
    )(c_mat, b_mat, segc, segr, x, cumc, cumr, dtr, g)
    d_cum = jnp.transpose(dcumc, (0, 2, 1)).reshape(heads, rows).T + dcumr.reshape(heads, rows).T
    d_dt = ddtr.reshape(heads, rows).T
    return dx, d_dt, d_cum, db, dc


@jax.custom_vjp
def ssd_core(x, dt, cum, b_mat, c_mat, seg):
    return _fwd_call(x, dt, cum, b_mat, c_mat, seg)


def _ssd_core_fwd(x, dt, cum, b_mat, c_mat, seg):
    return _fwd_call(x, dt, cum, b_mat, c_mat, seg), (x, dt, cum, b_mat, c_mat, seg)


def _ssd_core_bwd(res, g):
    x, dt, cum, b_mat, c_mat, seg = res
    dx, d_dt, d_cum, db, dc = _bwd_call(x, dt, cum, b_mat, c_mat, seg, g)
    return dx, d_dt, d_cum, db, dc, None


ssd_core.defvjp(_ssd_core_fwd, _ssd_core_bwd)

from jax.sharding import PartitionSpec as P
from jax.experimental.layout import Layout, with_layout_constraint

NORM_EPS = 1e-05


def contract_rows(first_op, second_op):
    return lax.dot_general(
        first_op, second_op, (((0,), (0,)), ((), ())), preferred_element_type=jnp.float32
    )


def contract_cols(first_op, second_op):
    return lax.dot_general(
        first_op, second_op, (((1,), (1,)), ((), ())), preferred_element_type=jnp.float32
    )


def segment_ids(lengths, row_count):
    seq_ends = jnp.cumsum(lengths)
    positions = jnp.arange(row_count, dtype=jnp.int32)
    return jnp.sum((positions[:, None] >= seq_ends[None, :]).astype(jnp.int32), axis=1)


def causal_conv(signal, kernel_w, kernel_b, segment):
    kernel_len = kernel_w.shape[0]
    row_count = signal.shape[0]
    summed = kernel_b[None, :] + kernel_w[kernel_len - 1][None, :] * signal
    for lag_steps in range(1, kernel_len):
        shifted = jnp.concatenate(
            [jnp.zeros((lag_steps, signal.shape[1]), jnp.float32), signal[: row_count - lag_steps]],
            axis=0,
        )
        earlier = jnp.concatenate(
            [jnp.full((lag_steps,), -1, jnp.int32), segment[: row_count - lag_steps]]
        )
        same_seq = (earlier == segment).astype(signal.dtype)
        summed = (
            summed + kernel_w[kernel_len - 1 - lag_steps][None, :] * shifted * same_seq[:, None]
        )
    return summed


def mixer_core(z_rows, x_rows, dt_raw, b_conv, c_conv, conv_wx, conv_bx, a_log, dt_bias,
               d_skip, segment=None):
    inner_n = x_rows.shape[1]
    heads_n = a_log.shape[0]
    x_conv = jax.nn.silu(causal_conv(x_rows, conv_wx, conv_bx, segment))
    steps_dt = jax.nn.softplus(dt_raw + dt_bias[None, :])
    decay = steps_dt * (-jnp.exp(a_log))[None, :]
    cum = jnp.cumsum(decay, axis=0)
    scanned = ssd_core(x_conv, steps_dt, cum, b_conv, c_conv, segment)
    skip = jnp.repeat(d_skip, inner_n // heads_n)
    mixed_out = scanned + skip[None, :] * x_conv
    return mixed_out * jax.nn.silu(z_rows)


def bc_core(bc_pre, conv_wbc, conv_bbc, segment=None):
    return jax.nn.silu(causal_conv(bc_pre, conv_wbc, conv_bbc, segment))


def per_device_body(tokens, cotangent, seq_lens, input_norm_gain, w_zx, w_bc, w_dt, conv_wx, conv_bx,
               conv_wbc, conv_bbc, a_log, dt_bias, d_skip, norm_gate, w_out):
    n_dp = lax.axis_size("dp")
    x_full = lax.all_gather(tokens, "tensor", axis=1, tiled=True)
    cot_full = lax.all_gather(cotangent, "tensor", axis=1, tiled=True)
    row_count = tokens.shape[0]
    feat_n = tokens.shape[1]
    d_model = x_full.shape[1]
    feat_start = lax.axis_index("tensor") * feat_n
    state_n = w_bc.shape[1] // 2
    inner_loc = norm_gate.shape[0]
    inner_all = inner_loc * lax.axis_size("tensor")
    segment = segment_ids(seq_lens[0], row_count)
    is_live = (segment < seq_lens.shape[1])[:, None]
    w_zx_flat = w_zx.reshape(d_model, 2 * inner_loc)
    tok_float = x_full.astype(jnp.float32)
    inverse_root_mean = lax.rsqrt(jnp.mean(tok_float * tok_float, axis=1, keepdims=True) + NORM_EPS)
    unit_scaled_input = tok_float * inverse_root_mean
    normed = (unit_scaled_input * input_norm_gain[None, :]).astype(jnp.bfloat16)
    zx_rows = jnp.dot(normed, w_zx_flat, preferred_element_type=jnp.float32)
    bc_pre = jnp.dot(normed, w_bc, preferred_element_type=jnp.float32)
    dt_raw = jnp.dot(normed, w_dt, preferred_element_type=jnp.float32)
    bc_post, bc_back = jax.vjp(partial(bc_core, segment=segment), bc_pre, conv_wbc, conv_bbc)
    gated_rows, core_back = jax.vjp(
        partial(mixer_core, segment=segment),
        zx_rows[:, :inner_loc], zx_rows[:, inner_loc:], dt_raw, bc_post[:, :state_n],
        bc_post[:, state_n:],
        conv_wx, conv_bx, a_log, dt_bias, d_skip,
    )
    cot_live = jnp.where(is_live, cot_full, jnp.zeros_like(cot_full))
    d_gate = contract_cols(cot_live, w_out)
    d_hat = d_gate * norm_gate[None, :]
    stats = lax.psum(
        jnp.concatenate([jnp.sum(gated_rows * gated_rows, axis=1, keepdims=True),
                         jnp.sum(d_hat * gated_rows, axis=1, keepdims=True)], axis=1),
        "tensor")
    squares, cross_sum = stats[:, 0:1], stats[:, 1:2]
    r_gate = lax.rsqrt(squares / inner_all + NORM_EPS)
    gate_hat = gated_rows * r_gate
    gate_out = (gate_hat * norm_gate[None, :]).astype(jnp.bfloat16)
    branch_part = jnp.dot(gate_out, w_out, preferred_element_type=jnp.float32)
    grad_gate = jnp.sum(d_gate * gate_hat, axis=0)
    d_gated = r_gate * d_hat - gated_rows * (r_gate * r_gate * r_gate * cross_sum / inner_all)
    d_gated, branch_part = lax.optimization_barrier((d_gated, branch_part))
    branch = lax.psum_scatter(branch_part, "tensor", scatter_dimension=1, tiled=True)
    own_float = tokens.astype(jnp.float32)
    block_out = (own_float + jnp.where(is_live, branch, 0.0)).astype(jnp.bfloat16)
    d_z, d_x, d_dt, d_b, d_c, grad_conv_wx, grad_conv_bx, grad_a_log, grad_dt_bias, grad_d_skip = (
        core_back(d_gated)
    )
    n_tp = lax.axis_size("tensor")
    chunk = d_model // n_dp
    row_major = Layout(major_to_minor=(0, 1))
    d_z_half = d_z.astype(jnp.bfloat16)
    grads_early = with_layout_constraint(jnp.concatenate(
        [with_layout_constraint(contract_rows(cot_live, gate_out), row_major),
         with_layout_constraint(contract_rows(normed, d_z_half), row_major)],
        axis=1), row_major)
    d_x, d_dt, block_out = lax.optimization_barrier((d_x, d_dt, block_out))
    d_zx_half = jnp.concatenate([d_z_half, d_x.astype(jnp.bfloat16)], axis=1)
    d_dt_half = d_dt.astype(jnp.bfloat16)
    early_sum = split_reduce_scatter(grads_early, n_dp)
    grads_x = with_layout_constraint(contract_rows(normed, d_zx_half[:, inner_loc:]), row_major)
    x_sum = split_reduce_scatter(grads_x, n_dp)
    d_bc_part = jnp.concatenate([d_b, d_c], axis=1)
    partial_in = contract_cols(d_zx_half, w_zx_flat) + contract_cols(d_dt_half, w_dt)
    bc_w = d_bc_part.shape[1]
    rs_in = jnp.concatenate(
        [partial_in.reshape(row_count, n_tp, feat_n),
         jnp.broadcast_to(d_bc_part[:, None, :], (row_count, n_tp, bc_w))], axis=2,
    ).reshape(row_count, n_tp * (feat_n + bc_w))
    rs_out = lax.psum_scatter(rs_in, "tensor", scatter_dimension=1, tiled=True)
    d_bc_post = rs_out[:, feat_n:]
    d_bc, grad_conv_wbc, grad_conv_bbc = bc_back(d_bc_post)
    d_bc_half = d_bc.astype(jnp.bfloat16)
    own_hat = lax.dynamic_slice_in_dim(unit_scaled_input, feat_start, feat_n, 1)
    own_gain = lax.dynamic_slice_in_dim(input_norm_gain, feat_start, feat_n, 0)
    own_w_bc = lax.dynamic_slice_in_dim(w_bc, feat_start, feat_n, 0)
    own_dn = rs_out[:, :feat_n] + contract_cols(d_bc_half, own_w_bc)
    own_dxhat = own_dn * own_gain[None, :]
    row_inner_product = lax.psum(jnp.sum(own_dxhat * own_hat, axis=1, keepdims=True),
                                 "tensor") / d_model
    grad_in = jnp.sum(own_dn * own_hat, axis=0)
    d_tokens = cotangent.astype(jnp.float32) + inverse_root_mean * (
        own_dxhat - own_hat * row_inner_product
    )
    smalls = (grad_conv_wx, grad_conv_bx, grad_conv_wbc, grad_conv_bbc, grad_a_log,
              grad_dt_bias, grad_d_skip, grad_gate, grad_in)
    flat_small = jnp.concatenate([v.reshape(-1) for v in smalls])
    small_cols = -(-flat_small.shape[0] // chunk)
    small_block = jnp.pad(flat_small, (0, small_cols * chunk - flat_small.shape[0])).reshape(
        chunk, small_cols)
    grads_small = with_layout_constraint(jnp.concatenate(
        [with_layout_constraint(
            contract_rows(normed, jnp.concatenate([d_bc_half, d_dt_half], axis=1)), row_major),
         jnp.tile(small_block, (n_dp, 1))], axis=1), row_major)
    small_sum_all = halving_reduce_scatter(grads_small, n_dp)
    grad_out_t_sum = early_sum[:, :inner_loc]
    grad_zx_sum = jnp.concatenate([early_sum[:, inner_loc:], x_sum], axis=1)
    grad_bc_sum = small_sum_all[:, :2 * state_n]
    grad_dt_sum = small_sum_all[:, 2 * state_n:2 * state_n + w_dt.shape[1]]
    small_sum = small_sum_all[:, 2 * state_n + w_dt.shape[1]:].reshape(-1)
    outs_small = []
    pos = 0
    for v in smalls:
        outs_small.append(small_sum[pos:pos + v.size].reshape(v.shape))
        pos += v.size
    grad_zx_out = grad_zx_sum.reshape(chunk, 2, inner_loc)
    return (block_out, d_tokens, grad_zx_out, grad_bc_sum, grad_dt_sum, grad_out_t_sum.T,
            *outs_small)


def halving_reduce_scatter(x, n_dev, order=None):
    me = lax.axis_index("dp")
    bits = n_dev.bit_length() - 1
    chunk = x.shape[0] // n_dev
    cur = x.reshape((2,) * bits + (chunk, x.shape[1]))
    axes = list(range(bits - 1, -1, -1))
    for bit in (order if order is not None else range(bits)):
        pos = axes.index(bit)
        mine = (me >> bit) & 1
        keep = lax.dynamic_index_in_dim(cur, mine, axis=pos, keepdims=False)
        send = lax.dynamic_index_in_dim(cur, 1 - mine, axis=pos, keepdims=False)
        got = lax.ppermute(send, "dp", [(i, i ^ (1 << bit)) for i in range(n_dev)])
        cur = keep + got
        axes.pop(pos)
    return cur.reshape(chunk, x.shape[1])


def split_reduce_scatter(x, n_dev):
    bits = n_dev.bit_length() - 1
    half = x.shape[1] // 2
    first = tuple(range(bits))
    second = (0,) + tuple(range(bits - 1, 0, -1))
    return jnp.concatenate([halving_reduce_scatter(x[:, :half], n_dev, first),
                            halving_reduce_scatter(x[:, half:], n_dev, second)], axis=1)


def solution(mesh):
    in_specs = (
        P("dp", "tensor"), P("dp", "tensor"), P("dp", None), P(),
        P(None, None, "tensor"), P(), P(None, "tensor"), P(None, "tensor"), P("tensor"),
        P(), P(), P("tensor"), P("tensor"), P("tensor"), P("tensor"), P("tensor", None),
    )
    out_specs = (
        P("dp", "tensor"), P("dp", "tensor"), P("dp", None, "tensor"), P("dp", None),
        P("dp", "tensor"), P("tensor", "dp"), P(None, "tensor"), P("tensor"), P(), P(),
        P("tensor"), P("tensor"), P("tensor"), P("tensor"), P("tensor"),
    )
    return jax.shard_map(
        per_device_body, mesh=mesh, in_specs=in_specs, out_specs=out_specs, check_vma=False
    )
```

```python
from functools import partial


import jax
import jax.numpy as jnp
from jax import lax
from jax.experimental import pallas as pl
from jax.experimental.pallas import tpu as pltpu

PRECISE = lax.Precision.HIGHEST
HEAD_DIM = 64
PAIR = 2


def _dot(a, b):
    return jnp.dot(a, b, precision=PRECISE, preferred_element_type=jnp.float32)


def _dot_tn(a, b):
    return lax.dot_general(a, b, (((0,), (0,)), ((), ())), precision=PRECISE,
                           preferred_element_type=jnp.float32)


def _dot_nt(a, b):
    return lax.dot_general(a, b, (((1,), (1,)), ((), ())), precision=PRECISE,
                           preferred_element_type=jnp.float32)


def _prologue(c_ref, b_ref, segc_ref, segr_ref, s_scr, neg_scr):
    s_scr[...] = _dot_nt(c_ref[...], b_ref[...])
    rows = s_scr.shape[0]
    row_i = lax.broadcasted_iota(jnp.int32, (rows, rows), 0)
    col_j = lax.broadcasted_iota(jnp.int32, (rows, rows), 1)
    keep = (col_j <= row_i) & (segc_ref[...] == segr_ref[...])
    neg_scr[...] = jnp.where(keep, 0.0, -jnp.inf).astype(jnp.float32)


def _fwd_kernel(c_ref, b_ref, segc_ref, segr_ref, x_ref, cumc_ref, cumr_ref, dtr_ref,
                y_ref, s_scr, neg_scr):
    @pl.when(pl.program_id(0) == 0)
    def _():
        _prologue(c_ref, b_ref, segc_ref, segr_ref, s_scr, neg_scr)

    for k in range(PAIR):
        cc = cumc_ref[0, :, k:k + 1]
        cr = cumr_ref[0, k:k + 1, :]
        dr = dtr_ref[0, k:k + 1, :]
        decays = jnp.exp(cc - cr + neg_scr[...])
        mixing = s_scr[...] * (decays * dr)
        y_ref[:, k * HEAD_DIM:(k + 1) * HEAD_DIM] = _dot(
            mixing, x_ref[:, k * HEAD_DIM:(k + 1) * HEAD_DIM])


def _bwd_kernel(c_ref, b_ref, segc_ref, segr_ref, x_ref, cumc_ref, cumr_ref, dtr_ref, g_ref,
                dx_ref, dcumc_ref, dcumr_ref, ddtr_ref, db_ref, dc_ref,
                s_scr, neg_scr, ds_scr):
    step = pl.program_id(0)

    @pl.when(step == 0)
    def _():
        _prologue(c_ref, b_ref, segc_ref, segr_ref, s_scr, neg_scr)
        ds_scr[...] = jnp.zeros_like(ds_scr)

    for k in range(PAIR):
        cc = cumc_ref[0, :, k:k + 1]
        cr = cumr_ref[0, k:k + 1, :]
        dr = dtr_ref[0, k:k + 1, :]
        decays = jnp.exp(cc - cr + neg_scr[...])
        weights = decays * dr
        scores = s_scr[...]
        mixing = scores * weights
        xh = x_ref[:, k * HEAD_DIM:(k + 1) * HEAD_DIM]
        gh = g_ref[:, k * HEAD_DIM:(k + 1) * HEAD_DIM]
        dx_ref[:, k * HEAD_DIM:(k + 1) * HEAD_DIM] = _dot_tn(mixing, gh)
        d_mix = _dot_nt(gh, xh)
        d_dec = d_mix * decays
        ds_scr[...] += d_dec * dr
        through = d_dec * scores
        d_dt_row = jnp.sum(through, axis=0, keepdims=True)
        q_mat = through * dr
        dcumc_ref[0, :, k:k + 1] = jnp.sum(q_mat, axis=1, keepdims=True)
        dcumr_ref[0, k:k + 1, :] = -(d_dt_row * dr)
        ddtr_ref[0, k:k + 1, :] = d_dt_row

    @pl.when(step == pl.num_programs(0) - 1)
    def _():
        dc_ref[...] = _dot(ds_scr[...], b_ref[...])
        db_ref[...] = _dot_tn(ds_scr[...], c_ref[...])


def _specs(rows, state):
    full = lambda shape: pl.BlockSpec(shape, lambda g: (0,) * len(shape))
    return [
        full((rows, state)),
        full((rows, state)),
        full((rows, 1)),
        full((1, rows)),
        pl.BlockSpec((rows, PAIR * HEAD_DIM), lambda g: (0, g)),
        pl.BlockSpec((1, rows, PAIR), lambda g: (g, 0, 0)),
        pl.BlockSpec((1, PAIR, rows), lambda g: (g, 0, 0)),
        pl.BlockSpec((1, PAIR, rows), lambda g: (g, 0, 0)),
    ]


def _prep(dt, cum, seg):
    rows, heads = dt.shape
    groups = heads // PAIR
    cumr = cum.T.reshape(groups, PAIR, rows)
    cumc = jnp.transpose(cumr, (0, 2, 1))
    dtr = dt.T.reshape(groups, PAIR, rows)
    segc = seg.reshape(rows, 1)
    segr = seg.reshape(1, rows)
    return cumc, cumr, dtr, segc, segr


def _fwd_call(x, dt, cum, b_mat, c_mat, seg):
    rows, inner = x.shape
    heads = dt.shape[1]
    groups = heads // PAIR
    state = b_mat.shape[1]
    cumc, cumr, dtr, segc, segr = _prep(dt, cum, seg)
    flops = 2 * rows * rows * state * 6 + heads * (2 * rows * rows * HEAD_DIM * 6 + 8 * rows * rows)
    return pl.pallas_call(
        _fwd_kernel,
        grid=(groups,),
        in_specs=_specs(rows, state),
        out_specs=pl.BlockSpec((rows, PAIR * HEAD_DIM), lambda g: (0, g)),
        out_shape=jax.ShapeDtypeStruct((rows, inner), jnp.float32),
        scratch_shapes=[pltpu.VMEM((rows, rows), jnp.float32),
                        pltpu.VMEM((rows, rows), jnp.float32)],
        compiler_params=pltpu.CompilerParams(dimension_semantics=("arbitrary",)),
        cost_estimate=pl.CostEstimate(flops=flops, transcendentals=heads * rows * rows,
                                      bytes_accessed=4 * (2 * rows * inner + 2 * rows * state)),
        name="ssd_fwd",
    )(c_mat, b_mat, segc, segr, x, cumc, cumr, dtr)


def _bwd_call(x, dt, cum, b_mat, c_mat, seg, g):
    rows, inner = x.shape
    heads = dt.shape[1]
    groups = heads // PAIR
    state = b_mat.shape[1]
    cumc, cumr, dtr, segc, segr = _prep(dt, cum, seg)
    full = lambda shape: pl.BlockSpec(shape, lambda gi: (0,) * len(shape))
    flops = 2 * rows * rows * state * 6 * 3 + heads * (2 * 2 * rows * rows * HEAD_DIM * 6 + 16 * rows * rows)
    dx, dcumc, dcumr, ddtr, db, dc = pl.pallas_call(
        _bwd_kernel,
        grid=(groups,),
        in_specs=_specs(rows, state) + [pl.BlockSpec((rows, PAIR * HEAD_DIM), lambda gi: (0, gi))],
        out_specs=[
            pl.BlockSpec((rows, PAIR * HEAD_DIM), lambda gi: (0, gi)),
            pl.BlockSpec((1, rows, PAIR), lambda gi: (gi, 0, 0)),
            pl.BlockSpec((1, PAIR, rows), lambda gi: (gi, 0, 0)),
            pl.BlockSpec((1, PAIR, rows), lambda gi: (gi, 0, 0)),
            full((rows, state)),
            full((rows, state)),
        ],
        out_shape=[
            jax.ShapeDtypeStruct((rows, inner), jnp.float32),
            jax.ShapeDtypeStruct((groups, rows, PAIR), jnp.float32),
            jax.ShapeDtypeStruct((groups, PAIR, rows), jnp.float32),
            jax.ShapeDtypeStruct((groups, PAIR, rows), jnp.float32),
            jax.ShapeDtypeStruct((rows, state), jnp.float32),
            jax.ShapeDtypeStruct((rows, state), jnp.float32),
        ],
        scratch_shapes=[pltpu.VMEM((rows, rows), jnp.float32),
                        pltpu.VMEM((rows, rows), jnp.float32),
                        pltpu.VMEM((rows, rows), jnp.float32)],
        compiler_params=pltpu.CompilerParams(dimension_semantics=("arbitrary",)),
        cost_estimate=pl.CostEstimate(flops=flops, transcendentals=heads * rows * rows,
                                      bytes_accessed=4 * (4 * rows * inner + 4 * rows * state)),
        name="ssd_bwd",
    )(c_mat, b_mat, segc, segr, x, cumc, cumr, dtr, g)
    d_cum = jnp.transpose(dcumc, (0, 2, 1)).reshape(heads, rows).T + dcumr.reshape(heads, rows).T
    d_dt = ddtr.reshape(heads, rows).T
    return dx, d_dt, d_cum, db, dc


@jax.custom_vjp
def ssd_core(x, dt, cum, b_mat, c_mat, seg):
    return _fwd_call(x, dt, cum, b_mat, c_mat, seg)


def _ssd_core_fwd(x, dt, cum, b_mat, c_mat, seg):
    return _fwd_call(x, dt, cum, b_mat, c_mat, seg), (x, dt, cum, b_mat, c_mat, seg)


def _ssd_core_bwd(res, g):
    x, dt, cum, b_mat, c_mat, seg = res
    dx, d_dt, d_cum, db, dc = _bwd_call(x, dt, cum, b_mat, c_mat, seg, g)
    return dx, d_dt, d_cum, db, dc, None


ssd_core.defvjp(_ssd_core_fwd, _ssd_core_bwd)

from jax.sharding import PartitionSpec as P
from jax.experimental.layout import Layout, with_layout_constraint

NORM_EPS = 1e-05


def contract_rows(first_op, second_op):
    return lax.dot_general(
        first_op, second_op, (((0,), (0,)), ((), ())), preferred_element_type=jnp.float32
    )


def contract_cols(first_op, second_op):
    return lax.dot_general(
        first_op, second_op, (((1,), (1,)), ((), ())), preferred_element_type=jnp.float32
    )


def segment_ids(lengths, row_count):
    seq_ends = jnp.cumsum(lengths)
    positions = jnp.arange(row_count, dtype=jnp.int32)
    return jnp.sum((positions[:, None] >= seq_ends[None, :]).astype(jnp.int32), axis=1)


def causal_conv(signal, kernel_w, kernel_b, segment):
    kernel_len = kernel_w.shape[0]
    row_count = signal.shape[0]
    summed = kernel_b[None, :] + kernel_w[kernel_len - 1][None, :] * signal
    for lag_steps in range(1, kernel_len):
        shifted = jnp.concatenate(
            [jnp.zeros((lag_steps, signal.shape[1]), jnp.float32), signal[: row_count - lag_steps]],
            axis=0,
        )
        earlier = jnp.concatenate(
            [jnp.full((lag_steps,), -1, jnp.int32), segment[: row_count - lag_steps]]
        )
        same_seq = (earlier == segment).astype(signal.dtype)
        summed = (
            summed + kernel_w[kernel_len - 1 - lag_steps][None, :] * shifted * same_seq[:, None]
        )
    return summed


def mixer_core(z_rows, x_rows, dt_raw, b_conv, c_conv, conv_wx, conv_bx, a_log, dt_bias,
               d_skip, segment=None):
    inner_n = x_rows.shape[1]
    heads_n = a_log.shape[0]
    x_conv = jax.nn.silu(causal_conv(x_rows, conv_wx, conv_bx, segment))
    steps_dt = jax.nn.softplus(dt_raw + dt_bias[None, :])
    decay = steps_dt * (-jnp.exp(a_log))[None, :]
    cum = jnp.cumsum(decay, axis=0)
    scanned = ssd_core(x_conv, steps_dt, cum, b_conv, c_conv, segment)
    skip = jnp.repeat(d_skip, inner_n // heads_n)
    mixed_out = scanned + skip[None, :] * x_conv
    return mixed_out * jax.nn.silu(z_rows)


def bc_core(bc_pre, conv_wbc, conv_bbc, segment=None):
    return jax.nn.silu(causal_conv(bc_pre, conv_wbc, conv_bbc, segment))


def per_device_body(tokens, cotangent, seq_lens, input_norm_gain, w_zx, w_bc, w_dt, conv_wx, conv_bx,
               conv_wbc, conv_bbc, a_log, dt_bias, d_skip, norm_gate, w_out):
    n_dp = lax.axis_size("dp")
    x_full = lax.all_gather(tokens, "tensor", axis=1, tiled=True)
    cot_full = lax.all_gather(cotangent, "tensor", axis=1, tiled=True)
    row_count = tokens.shape[0]
    feat_n = tokens.shape[1]
    d_model = x_full.shape[1]
    feat_start = lax.axis_index("tensor") * feat_n
    state_n = w_bc.shape[1] // 2
    inner_loc = norm_gate.shape[0]
    inner_all = inner_loc * lax.axis_size("tensor")
    segment = segment_ids(seq_lens[0], row_count)
    is_live = (segment < seq_lens.shape[1])[:, None]
    w_zx_flat = w_zx.reshape(d_model, 2 * inner_loc)
    tok_float = x_full.astype(jnp.float32)
    inverse_root_mean = lax.rsqrt(jnp.mean(tok_float * tok_float, axis=1, keepdims=True) + NORM_EPS)
    unit_scaled_input = tok_float * inverse_root_mean
    normed = (unit_scaled_input * input_norm_gain[None, :]).astype(jnp.bfloat16)
    zx_rows = jnp.dot(normed, w_zx_flat, preferred_element_type=jnp.float32)
    bc_pre = jnp.dot(normed, w_bc, preferred_element_type=jnp.float32)
    dt_raw = jnp.dot(normed, w_dt, preferred_element_type=jnp.float32)
    bc_post, bc_back = jax.vjp(partial(bc_core, segment=segment), bc_pre, conv_wbc, conv_bbc)
    gated_rows, core_back = jax.vjp(
        partial(mixer_core, segment=segment),
        zx_rows[:, :inner_loc], zx_rows[:, inner_loc:], dt_raw, bc_post[:, :state_n],
        bc_post[:, state_n:],
        conv_wx, conv_bx, a_log, dt_bias, d_skip,
    )
    cot_live = jnp.where(is_live, cot_full, jnp.zeros_like(cot_full))
    d_gate = contract_cols(cot_live, w_out)
    d_hat = d_gate * norm_gate[None, :]
    stats = lax.psum(
        jnp.concatenate([jnp.sum(gated_rows * gated_rows, axis=1, keepdims=True),
                         jnp.sum(d_hat * gated_rows, axis=1, keepdims=True)], axis=1),
        "tensor")
    squares, cross_sum = stats[:, 0:1], stats[:, 1:2]
    r_gate = lax.rsqrt(squares / inner_all + NORM_EPS)
    gate_hat = gated_rows * r_gate
    gate_out = (gate_hat * norm_gate[None, :]).astype(jnp.bfloat16)
    branch_part = jnp.dot(gate_out, w_out, preferred_element_type=jnp.float32)
    grad_gate = jnp.sum(d_gate * gate_hat, axis=0)
    d_gated = r_gate * d_hat - gated_rows * (r_gate * r_gate * r_gate * cross_sum / inner_all)
    d_gated, branch_part = lax.optimization_barrier((d_gated, branch_part))
    branch = lax.psum_scatter(branch_part, "tensor", scatter_dimension=1, tiled=True)
    own_float = tokens.astype(jnp.float32)
    block_out = (own_float + jnp.where(is_live, branch, 0.0)).astype(jnp.bfloat16)
    d_z, d_x, d_dt, d_b, d_c, grad_conv_wx, grad_conv_bx, grad_a_log, grad_dt_bias, grad_d_skip = (
        core_back(d_gated)
    )
    n_tp = lax.axis_size("tensor")
    chunk = d_model // n_dp
    row_major = Layout(major_to_minor=(0, 1))
    d_z_half = d_z.astype(jnp.bfloat16)
    grads_early = with_layout_constraint(jnp.concatenate(
        [with_layout_constraint(contract_rows(cot_live, gate_out), row_major),
         with_layout_constraint(contract_rows(normed, d_z_half), row_major)],
        axis=1), row_major)
    d_x, d_dt, block_out = lax.optimization_barrier((d_x, d_dt, block_out))
    d_zx_half = jnp.concatenate([d_z_half, d_x.astype(jnp.bfloat16)], axis=1)
    d_dt_half = d_dt.astype(jnp.bfloat16)
    early_sum = split_reduce_scatter(grads_early, n_dp)
    grads_x = with_layout_constraint(contract_rows(normed, d_zx_half[:, inner_loc:]), row_major)
    x_sum = split_reduce_scatter(grads_x, n_dp)
    d_bc_part = jnp.concatenate([d_b, d_c], axis=1)
    partial_in = contract_cols(d_zx_half, w_zx_flat) + contract_cols(d_dt_half, w_dt)
    hat_gain = unit_scaled_input * input_norm_gain[None, :]
    row_part = jnp.sum(partial_in * hat_gain, axis=1, keepdims=True)
    bc_sum = doubling_all_reduce(jnp.concatenate([d_bc_part, row_part], axis=1), "tensor", n_tp)
    d_bc_post = bc_sum[:, :2 * state_n]
    d_bc, grad_conv_wbc, grad_conv_bbc = bc_back(d_bc_post)
    d_bc_half = d_bc.astype(jnp.bfloat16)
    bc_full = contract_cols(d_bc_half, w_bc)
    row_inner_product = (bc_sum[:, 2 * state_n:] + jnp.sum(bc_full * hat_gain, axis=1,
                                                            keepdims=True)) / d_model
    smalls = (grad_conv_wx, grad_conv_bx, grad_conv_wbc, grad_conv_bbc, grad_a_log,
              grad_dt_bias, grad_d_skip, grad_gate)
    flat_small = jnp.concatenate([v.reshape(-1) for v in smalls])
    small_cols = -(-flat_small.shape[0] // chunk)
    small_block = jnp.pad(flat_small, (0, small_cols * chunk - flat_small.shape[0])).reshape(
        chunk, small_cols)
    grads_small = with_layout_constraint(jnp.concatenate(
        [with_layout_constraint(
            contract_rows(normed, jnp.concatenate([d_bc_half, d_dt_half], axis=1)), row_major),
         jnp.tile(small_block, (n_dp, 1))], axis=1), row_major)
    small_sum_all = halving_reduce_scatter(grads_small, n_dp)
    partial_in, bc_sum = lax.optimization_barrier((partial_in, bc_sum))
    own_part = lax.psum_scatter(partial_in, "tensor", scatter_dimension=1, tiled=True)
    own_hat = lax.dynamic_slice_in_dim(unit_scaled_input, feat_start, feat_n, 1)
    own_gain = lax.dynamic_slice_in_dim(input_norm_gain, feat_start, feat_n, 0)
    own_dn = own_part + lax.dynamic_slice_in_dim(bc_full, feat_start, feat_n, 1)
    own_dxhat = own_dn * own_gain[None, :]
    grad_in = doubling_all_reduce(jnp.sum(own_dn * own_hat, axis=0), "dp", n_dp)
    d_tokens = cotangent.astype(jnp.float32) + inverse_root_mean * (
        own_dxhat - own_hat * row_inner_product
    )
    grad_out_t_sum = early_sum[:, :inner_loc]
    grad_zx_sum = jnp.concatenate([early_sum[:, inner_loc:], x_sum], axis=1)
    grad_bc_sum = small_sum_all[:, :2 * state_n]
    grad_dt_sum = small_sum_all[:, 2 * state_n:2 * state_n + w_dt.shape[1]]
    small_sum = small_sum_all[:, 2 * state_n + w_dt.shape[1]:].reshape(-1)
    outs_small = []
    pos = 0
    for v in smalls:
        outs_small.append(small_sum[pos:pos + v.size].reshape(v.shape))
        pos += v.size
    grad_zx_out = grad_zx_sum.reshape(chunk, 2, inner_loc)
    return (block_out, d_tokens, grad_zx_out, grad_bc_sum, grad_dt_sum, grad_out_t_sum.T,
            *outs_small, grad_in)


def halving_reduce_scatter(x, n_dev, order=None):
    me = lax.axis_index("dp")
    bits = n_dev.bit_length() - 1
    chunk = x.shape[0] // n_dev
    cur = x.reshape((2,) * bits + (chunk, x.shape[1]))
    axes = list(range(bits - 1, -1, -1))
    for bit in (order if order is not None else range(bits)):
        pos = axes.index(bit)
        mine = (me >> bit) & 1
        keep = lax.dynamic_index_in_dim(cur, mine, axis=pos, keepdims=False)
        send = lax.dynamic_index_in_dim(cur, 1 - mine, axis=pos, keepdims=False)
        got = lax.ppermute(send, "dp", [(i, i ^ (1 << bit)) for i in range(n_dev)])
        cur = keep + got
        axes.pop(pos)
    return cur.reshape(chunk, x.shape[1])


def doubling_all_reduce(x, axis, n_dev):
    bit = 0
    while (1 << bit) < n_dev:
        x = x + lax.ppermute(x, axis, [(i, i ^ (1 << bit)) for i in range(n_dev)])
        bit += 1
    return x


def split_reduce_scatter(x, n_dev):
    bits = n_dev.bit_length() - 1
    half = x.shape[1] // 2
    first = tuple(range(bits))
    second = (0,) + tuple(range(bits - 1, 0, -1))
    return jnp.concatenate([halving_reduce_scatter(x[:, :half], n_dev, first),
                            halving_reduce_scatter(x[:, half:], n_dev, second)], axis=1)


def solution(mesh):
    in_specs = (
        P("dp", "tensor"), P("dp", "tensor"), P("dp", None), P(),
        P(None, None, "tensor"), P(), P(None, "tensor"), P(None, "tensor"), P("tensor"),
        P(), P(), P("tensor"), P("tensor"), P("tensor"), P("tensor"), P("tensor", None),
    )
    out_specs = (
        P("dp", "tensor"), P("dp", "tensor"), P("dp", None, "tensor"), P("dp", None),
        P("dp", "tensor"), P("tensor", "dp"), P(None, "tensor"), P("tensor"), P(), P(),
        P("tensor"), P("tensor"), P("tensor"), P("tensor"), P("tensor"),
    )
    return jax.shard_map(
        per_device_body, mesh=mesh, in_specs=in_specs, out_specs=out_specs, check_vma=False
    )
```

```python
from functools import partial


import jax
import jax.numpy as jnp
from jax import lax
from jax.experimental import pallas as pl
from jax.experimental.pallas import tpu as pltpu

PRECISE = lax.Precision.HIGHEST
HEAD_DIM = 64
PAIR = 2


def _dot(a, b):
    return jnp.dot(a, b, precision=PRECISE, preferred_element_type=jnp.float32)


def _dot_tn(a, b):
    return lax.dot_general(a, b, (((0,), (0,)), ((), ())), precision=PRECISE,
                           preferred_element_type=jnp.float32)


def _dot_nt(a, b):
    return lax.dot_general(a, b, (((1,), (1,)), ((), ())), precision=PRECISE,
                           preferred_element_type=jnp.float32)


def _prologue(c_ref, b_ref, segc_ref, segr_ref, s_scr, neg_scr):
    s_scr[...] = _dot_nt(c_ref[...], b_ref[...])
    rows = s_scr.shape[0]
    row_i = lax.broadcasted_iota(jnp.int32, (rows, rows), 0)
    col_j = lax.broadcasted_iota(jnp.int32, (rows, rows), 1)
    keep = (col_j <= row_i) & (segc_ref[...] == segr_ref[...])
    neg_scr[...] = jnp.where(keep, 0.0, -jnp.inf).astype(jnp.float32)


def _fwd_kernel(c_ref, b_ref, segc_ref, segr_ref, x_ref, cumc_ref, cumr_ref, dtr_ref,
                y_ref, s_scr, neg_scr):
    @pl.when(pl.program_id(0) == 0)
    def _():
        _prologue(c_ref, b_ref, segc_ref, segr_ref, s_scr, neg_scr)

    for k in range(PAIR):
        cc = cumc_ref[0, :, k:k + 1]
        cr = cumr_ref[0, k:k + 1, :]
        dr = dtr_ref[0, k:k + 1, :]
        decays = jnp.exp(cc - cr + neg_scr[...])
        mixing = s_scr[...] * (decays * dr)
        y_ref[:, k * HEAD_DIM:(k + 1) * HEAD_DIM] = _dot(
            mixing, x_ref[:, k * HEAD_DIM:(k + 1) * HEAD_DIM])


def _bwd_kernel(c_ref, b_ref, segc_ref, segr_ref, x_ref, cumc_ref, cumr_ref, dtr_ref, g_ref,
                dx_ref, dcumc_ref, dcumr_ref, ddtr_ref, db_ref, dc_ref,
                s_scr, neg_scr, ds_scr):
    step = pl.program_id(0)

    @pl.when(step == 0)
    def _():
        _prologue(c_ref, b_ref, segc_ref, segr_ref, s_scr, neg_scr)
        ds_scr[...] = jnp.zeros_like(ds_scr)

    for k in range(PAIR):
        cc = cumc_ref[0, :, k:k + 1]
        cr = cumr_ref[0, k:k + 1, :]
        dr = dtr_ref[0, k:k + 1, :]
        decays = jnp.exp(cc - cr + neg_scr[...])
        weights = decays * dr
        scores = s_scr[...]
        mixing = scores * weights
        xh = x_ref[:, k * HEAD_DIM:(k + 1) * HEAD_DIM]
        gh = g_ref[:, k * HEAD_DIM:(k + 1) * HEAD_DIM]
        dx_ref[:, k * HEAD_DIM:(k + 1) * HEAD_DIM] = _dot_tn(mixing, gh)
        d_mix = _dot_nt(gh, xh)
        d_dec = d_mix * decays
        ds_scr[...] += d_dec * dr
        through = d_dec * scores
        d_dt_row = jnp.sum(through, axis=0, keepdims=True)
        q_mat = through * dr
        dcumc_ref[0, :, k:k + 1] = jnp.sum(q_mat, axis=1, keepdims=True)
        dcumr_ref[0, k:k + 1, :] = -(d_dt_row * dr)
        ddtr_ref[0, k:k + 1, :] = d_dt_row

    @pl.when(step == pl.num_programs(0) - 1)
    def _():
        dc_ref[...] = _dot(ds_scr[...], b_ref[...])
        db_ref[...] = _dot_tn(ds_scr[...], c_ref[...])


def _specs(rows, state):
    full = lambda shape: pl.BlockSpec(shape, lambda g: (0,) * len(shape))
    return [
        full((rows, state)),
        full((rows, state)),
        full((rows, 1)),
        full((1, rows)),
        pl.BlockSpec((rows, PAIR * HEAD_DIM), lambda g: (0, g)),
        pl.BlockSpec((1, rows, PAIR), lambda g: (g, 0, 0)),
        pl.BlockSpec((1, PAIR, rows), lambda g: (g, 0, 0)),
        pl.BlockSpec((1, PAIR, rows), lambda g: (g, 0, 0)),
    ]


def _prep(dt, cum, seg):
    rows, heads = dt.shape
    groups = heads // PAIR
    cumr = cum.T.reshape(groups, PAIR, rows)
    cumc = jnp.transpose(cumr, (0, 2, 1))
    dtr = dt.T.reshape(groups, PAIR, rows)
    segc = seg.reshape(rows, 1)
    segr = seg.reshape(1, rows)
    return cumc, cumr, dtr, segc, segr


def _fwd_call(x, dt, cum, b_mat, c_mat, seg):
    rows, inner = x.shape
    heads = dt.shape[1]
    groups = heads // PAIR
    state = b_mat.shape[1]
    cumc, cumr, dtr, segc, segr = _prep(dt, cum, seg)
    flops = 2 * rows * rows * state * 6 + heads * (2 * rows * rows * HEAD_DIM * 6 + 8 * rows * rows)
    return pl.pallas_call(
        _fwd_kernel,
        grid=(groups,),
        in_specs=_specs(rows, state),
        out_specs=pl.BlockSpec((rows, PAIR * HEAD_DIM), lambda g: (0, g)),
        out_shape=jax.ShapeDtypeStruct((rows, inner), jnp.float32),
        scratch_shapes=[pltpu.VMEM((rows, rows), jnp.float32),
                        pltpu.VMEM((rows, rows), jnp.float32)],
        compiler_params=pltpu.CompilerParams(dimension_semantics=("arbitrary",)),
        cost_estimate=pl.CostEstimate(flops=flops, transcendentals=heads * rows * rows,
                                      bytes_accessed=4 * (2 * rows * inner + 2 * rows * state)),
        name="ssd_fwd",
    )(c_mat, b_mat, segc, segr, x, cumc, cumr, dtr)


def _bwd_call(x, dt, cum, b_mat, c_mat, seg, g):
    rows, inner = x.shape
    heads = dt.shape[1]
    groups = heads // PAIR
    state = b_mat.shape[1]
    cumc, cumr, dtr, segc, segr = _prep(dt, cum, seg)
    full = lambda shape: pl.BlockSpec(shape, lambda gi: (0,) * len(shape))
    flops = 2 * rows * rows * state * 6 * 3 + heads * (2 * 2 * rows * rows * HEAD_DIM * 6 + 16 * rows * rows)
    dx, dcumc, dcumr, ddtr, db, dc = pl.pallas_call(
        _bwd_kernel,
        grid=(groups,),
        in_specs=_specs(rows, state) + [pl.BlockSpec((rows, PAIR * HEAD_DIM), lambda gi: (0, gi))],
        out_specs=[
            pl.BlockSpec((rows, PAIR * HEAD_DIM), lambda gi: (0, gi)),
            pl.BlockSpec((1, rows, PAIR), lambda gi: (gi, 0, 0)),
            pl.BlockSpec((1, PAIR, rows), lambda gi: (gi, 0, 0)),
            pl.BlockSpec((1, PAIR, rows), lambda gi: (gi, 0, 0)),
            full((rows, state)),
            full((rows, state)),
        ],
        out_shape=[
            jax.ShapeDtypeStruct((rows, inner), jnp.float32),
            jax.ShapeDtypeStruct((groups, rows, PAIR), jnp.float32),
            jax.ShapeDtypeStruct((groups, PAIR, rows), jnp.float32),
            jax.ShapeDtypeStruct((groups, PAIR, rows), jnp.float32),
            jax.ShapeDtypeStruct((rows, state), jnp.float32),
            jax.ShapeDtypeStruct((rows, state), jnp.float32),
        ],
        scratch_shapes=[pltpu.VMEM((rows, rows), jnp.float32),
                        pltpu.VMEM((rows, rows), jnp.float32),
                        pltpu.VMEM((rows, rows), jnp.float32)],
        compiler_params=pltpu.CompilerParams(dimension_semantics=("arbitrary",)),
        cost_estimate=pl.CostEstimate(flops=flops, transcendentals=heads * rows * rows,
                                      bytes_accessed=4 * (4 * rows * inner + 4 * rows * state)),
        name="ssd_bwd",
    )(c_mat, b_mat, segc, segr, x, cumc, cumr, dtr, g)
    d_cum = jnp.transpose(dcumc, (0, 2, 1)).reshape(heads, rows).T + dcumr.reshape(heads, rows).T
    d_dt = ddtr.reshape(heads, rows).T
    return dx, d_dt, d_cum, db, dc


@jax.custom_vjp
def ssd_core(x, dt, cum, b_mat, c_mat, seg):
    return _fwd_call(x, dt, cum, b_mat, c_mat, seg)


def _ssd_core_fwd(x, dt, cum, b_mat, c_mat, seg):
    return _fwd_call(x, dt, cum, b_mat, c_mat, seg), (x, dt, cum, b_mat, c_mat, seg)


def _ssd_core_bwd(res, g):
    x, dt, cum, b_mat, c_mat, seg = res
    dx, d_dt, d_cum, db, dc = _bwd_call(x, dt, cum, b_mat, c_mat, seg, g)
    return dx, d_dt, d_cum, db, dc, None


ssd_core.defvjp(_ssd_core_fwd, _ssd_core_bwd)

from jax.sharding import PartitionSpec as P
from jax.experimental.layout import Layout, with_layout_constraint

NORM_EPS = 1e-05


def contract_rows(first_op, second_op):
    return lax.dot_general(
        first_op, second_op, (((0,), (0,)), ((), ())), preferred_element_type=jnp.float32
    )


def contract_cols(first_op, second_op):
    return lax.dot_general(
        first_op, second_op, (((1,), (1,)), ((), ())), preferred_element_type=jnp.float32
    )


def segment_ids(lengths, row_count):
    seq_ends = jnp.cumsum(lengths)
    positions = jnp.arange(row_count, dtype=jnp.int32)
    return jnp.sum((positions[:, None] >= seq_ends[None, :]).astype(jnp.int32), axis=1)


def causal_conv(signal, kernel_w, kernel_b, segment):
    kernel_len = kernel_w.shape[0]
    row_count = signal.shape[0]
    summed = kernel_b[None, :] + kernel_w[kernel_len - 1][None, :] * signal
    for lag_steps in range(1, kernel_len):
        shifted = jnp.concatenate(
            [jnp.zeros((lag_steps, signal.shape[1]), jnp.float32), signal[: row_count - lag_steps]],
            axis=0,
        )
        earlier = jnp.concatenate(
            [jnp.full((lag_steps,), -1, jnp.int32), segment[: row_count - lag_steps]]
        )
        same_seq = (earlier == segment).astype(signal.dtype)
        summed = (
            summed + kernel_w[kernel_len - 1 - lag_steps][None, :] * shifted * same_seq[:, None]
        )
    return summed


def mixer_core(z_rows, x_rows, dt_raw, b_conv, c_conv, conv_wx, conv_bx, a_log, dt_bias,
               d_skip, segment=None):
    inner_n = x_rows.shape[1]
    heads_n = a_log.shape[0]
    x_conv = jax.nn.silu(causal_conv(x_rows, conv_wx, conv_bx, segment))
    steps_dt = jax.nn.softplus(dt_raw + dt_bias[None, :])
    decay = steps_dt * (-jnp.exp(a_log))[None, :]
    cum = jnp.cumsum(decay, axis=0)
    scanned = ssd_core(x_conv, steps_dt, cum, b_conv, c_conv, segment)
    skip = jnp.repeat(d_skip, inner_n // heads_n)
    mixed_out = scanned + skip[None, :] * x_conv
    return mixed_out * jax.nn.silu(z_rows)


def bc_core(bc_pre, conv_wbc, conv_bbc, segment=None):
    return jax.nn.silu(causal_conv(bc_pre, conv_wbc, conv_bbc, segment))


def per_device_body(tokens, cotangent, seq_lens, input_norm_gain, w_zx, w_bc, w_dt, conv_wx, conv_bx,
               conv_wbc, conv_bbc, a_log, dt_bias, d_skip, norm_gate, w_out):
    n_dp = lax.axis_size("dp")
    x_full = lax.all_gather(tokens, "tensor", axis=1, tiled=True)
    cot_full = lax.all_gather(cotangent, "tensor", axis=1, tiled=True)
    row_count = tokens.shape[0]
    feat_n = tokens.shape[1]
    d_model = x_full.shape[1]
    feat_start = lax.axis_index("tensor") * feat_n
    state_n = w_bc.shape[1] // 2
    inner_loc = norm_gate.shape[0]
    inner_all = inner_loc * lax.axis_size("tensor")
    segment = segment_ids(seq_lens[0], row_count)
    is_live = (segment < seq_lens.shape[1])[:, None]
    w_zx_flat = w_zx.reshape(d_model, 2 * inner_loc)
    tok_float = x_full.astype(jnp.float32)
    inverse_root_mean = lax.rsqrt(jnp.mean(tok_float * tok_float, axis=1, keepdims=True) + NORM_EPS)
    unit_scaled_input = tok_float * inverse_root_mean
    normed = (unit_scaled_input * input_norm_gain[None, :]).astype(jnp.bfloat16)
    zx_rows = jnp.dot(normed, w_zx_flat, preferred_element_type=jnp.float32)
    bc_pre = jnp.dot(normed, w_bc, preferred_element_type=jnp.float32)
    dt_raw = jnp.dot(normed, w_dt, preferred_element_type=jnp.float32)
    bc_post, bc_back = jax.vjp(partial(bc_core, segment=segment), bc_pre, conv_wbc, conv_bbc)
    gated_rows, core_back = jax.vjp(
        partial(mixer_core, segment=segment),
        zx_rows[:, :inner_loc], zx_rows[:, inner_loc:], dt_raw, bc_post[:, :state_n],
        bc_post[:, state_n:],
        conv_wx, conv_bx, a_log, dt_bias, d_skip,
    )
    cot_live = jnp.where(is_live, cot_full, jnp.zeros_like(cot_full))
    d_gate = contract_cols(cot_live, w_out)
    d_hat = d_gate * norm_gate[None, :]
    stats = lax.psum(
        jnp.concatenate([jnp.sum(gated_rows * gated_rows, axis=1, keepdims=True),
                         jnp.sum(d_hat * gated_rows, axis=1, keepdims=True)], axis=1),
        "tensor")
    squares, cross_sum = stats[:, 0:1], stats[:, 1:2]
    r_gate = lax.rsqrt(squares / inner_all + NORM_EPS)
    gate_hat = gated_rows * r_gate
    gate_out = (gate_hat * norm_gate[None, :]).astype(jnp.bfloat16)
    branch_part = jnp.dot(gate_out, w_out, preferred_element_type=jnp.float32)
    grad_gate = jnp.sum(d_gate * gate_hat, axis=0)
    d_gated = r_gate * d_hat - gated_rows * (r_gate * r_gate * r_gate * cross_sum / inner_all)
    d_gated, branch_part = lax.optimization_barrier((d_gated, branch_part))
    branch = lax.psum_scatter(branch_part, "tensor", scatter_dimension=1, tiled=True)
    own_float = tokens.astype(jnp.float32)
    block_out = (own_float + jnp.where(is_live, branch, 0.0)).astype(jnp.bfloat16)
    d_z, d_x, d_dt, d_b, d_c, grad_conv_wx, grad_conv_bx, grad_a_log, grad_dt_bias, grad_d_skip = (
        core_back(d_gated)
    )
    n_tp = lax.axis_size("tensor")
    chunk = d_model // n_dp
    row_major = Layout(major_to_minor=(0, 1))
    d_z_half = d_z.astype(jnp.bfloat16)
    grads_early = with_layout_constraint(jnp.concatenate(
        [with_layout_constraint(contract_rows(cot_live, gate_out), row_major),
         with_layout_constraint(contract_rows(normed, d_z_half), row_major)],
        axis=1), row_major)
    d_x, d_dt, block_out = lax.optimization_barrier((d_x, d_dt, block_out))
    d_zx_half = jnp.concatenate([d_z_half, d_x.astype(jnp.bfloat16)], axis=1)
    d_dt_half = d_dt.astype(jnp.bfloat16)
    early_sum = split_reduce_scatter(grads_early, n_dp)
    grads_x = with_layout_constraint(contract_rows(normed, d_zx_half[:, inner_loc:]), row_major)
    x_sum = split_reduce_scatter(grads_x, n_dp)
    d_bc_part = jnp.concatenate([d_b, d_c], axis=1)
    partial_in = contract_cols(d_zx_half, w_zx_flat) + contract_cols(d_dt_half, w_dt)
    hat_gain = unit_scaled_input * input_norm_gain[None, :]
    row_part = jnp.sum(partial_in * hat_gain, axis=1, keepdims=True)
    d_bc_post = lax.psum(d_bc_part, "tensor")
    row_sum = doubling_all_reduce(row_part, "tensor", n_tp)
    d_bc, grad_conv_wbc, grad_conv_bbc = bc_back(d_bc_post)
    d_bc_half = d_bc.astype(jnp.bfloat16)
    bc_full = contract_cols(d_bc_half, w_bc)
    row_inner_product = (row_sum + jnp.sum(bc_full * hat_gain, axis=1, keepdims=True)) / d_model
    smalls = (grad_conv_wx, grad_conv_bx, grad_conv_wbc, grad_conv_bbc, grad_a_log,
              grad_dt_bias, grad_d_skip, grad_gate)
    flat_small = jnp.concatenate([v.reshape(-1) for v in smalls])
    small_cols = -(-flat_small.shape[0] // chunk)
    small_block = jnp.pad(flat_small, (0, small_cols * chunk - flat_small.shape[0])).reshape(
        chunk, small_cols)
    grads_small = with_layout_constraint(jnp.concatenate(
        [with_layout_constraint(
            contract_rows(normed, jnp.concatenate([d_bc_half, d_dt_half], axis=1)), row_major),
         jnp.tile(small_block, (n_dp, 1))], axis=1), row_major)
    small_sum_all = halving_reduce_scatter(grads_small, n_dp)
    partial_in, d_bc_post = lax.optimization_barrier((partial_in, d_bc_post))
    own_part = lax.psum_scatter(partial_in, "tensor", scatter_dimension=1, tiled=True)
    own_hat = lax.dynamic_slice_in_dim(unit_scaled_input, feat_start, feat_n, 1)
    own_gain = lax.dynamic_slice_in_dim(input_norm_gain, feat_start, feat_n, 0)
    own_dn = own_part + lax.dynamic_slice_in_dim(bc_full, feat_start, feat_n, 1)
    own_dxhat = own_dn * own_gain[None, :]
    grad_in = doubling_all_reduce(jnp.sum(own_dn * own_hat, axis=0), "dp", n_dp)
    d_tokens = cotangent.astype(jnp.float32) + inverse_root_mean * (
        own_dxhat - own_hat * row_inner_product
    )
    grad_out_t_sum = early_sum[:, :inner_loc]
    grad_zx_sum = jnp.concatenate([early_sum[:, inner_loc:], x_sum], axis=1)
    grad_bc_sum = small_sum_all[:, :2 * state_n]
    grad_dt_sum = small_sum_all[:, 2 * state_n:2 * state_n + w_dt.shape[1]]
    small_sum = small_sum_all[:, 2 * state_n + w_dt.shape[1]:].reshape(-1)
    outs_small = []
    pos = 0
    for v in smalls:
        outs_small.append(small_sum[pos:pos + v.size].reshape(v.shape))
        pos += v.size
    grad_zx_out = grad_zx_sum.reshape(chunk, 2, inner_loc)
    return (block_out, d_tokens, grad_zx_out, grad_bc_sum, grad_dt_sum, grad_out_t_sum.T,
            *outs_small, grad_in)


def halving_reduce_scatter(x, n_dev, order=None):
    me = lax.axis_index("dp")
    bits = n_dev.bit_length() - 1
    chunk = x.shape[0] // n_dev
    cur = x.reshape((2,) * bits + (chunk, x.shape[1]))
    axes = list(range(bits - 1, -1, -1))
    for bit in (order if order is not None else range(bits)):
        pos = axes.index(bit)
        mine = (me >> bit) & 1
        keep = lax.dynamic_index_in_dim(cur, mine, axis=pos, keepdims=False)
        send = lax.dynamic_index_in_dim(cur, 1 - mine, axis=pos, keepdims=False)
        got = lax.ppermute(send, "dp", [(i, i ^ (1 << bit)) for i in range(n_dev)])
        cur = keep + got
        axes.pop(pos)
    return cur.reshape(chunk, x.shape[1])


def doubling_all_reduce(x, axis, n_dev):
    bit = 0
    while (1 << bit) < n_dev:
        x = x + lax.ppermute(x, axis, [(i, i ^ (1 << bit)) for i in range(n_dev)])
        bit += 1
    return x


def split_reduce_scatter(x, n_dev):
    bits = n_dev.bit_length() - 1
    half = x.shape[1] // 2
    first = tuple(range(bits))
    second = (0,) + tuple(range(bits - 1, 0, -1))
    return jnp.concatenate([halving_reduce_scatter(x[:, :half], n_dev, first),
                            halving_reduce_scatter(x[:, half:], n_dev, second)], axis=1)


def solution(mesh):
    in_specs = (
        P("dp", "tensor"), P("dp", "tensor"), P("dp", None), P(),
        P(None, None, "tensor"), P(), P(None, "tensor"), P(None, "tensor"), P("tensor"),
        P(), P(), P("tensor"), P("tensor"), P("tensor"), P("tensor"), P("tensor", None),
    )
    out_specs = (
        P("dp", "tensor"), P("dp", "tensor"), P("dp", None, "tensor"), P("dp", None),
        P("dp", "tensor"), P("tensor", "dp"), P(None, "tensor"), P("tensor"), P(), P(),
        P("tensor"), P("tensor"), P("tensor"), P("tensor"), P("tensor"),
    )
    return jax.shard_map(
        per_device_body, mesh=mesh, in_specs=in_specs, out_specs=out_specs, check_vma=False
    )
```

```python
from functools import partial


import jax
import jax.numpy as jnp
from jax import lax
from jax.experimental import pallas as pl
from jax.experimental.pallas import tpu as pltpu

PRECISE = lax.Precision.HIGHEST
HEAD_DIM = 64
PAIR = 2


def _dot(a, b):
    return jnp.dot(a, b, precision=PRECISE, preferred_element_type=jnp.float32)


def _dot_tn(a, b):
    return lax.dot_general(a, b, (((0,), (0,)), ((), ())), precision=PRECISE,
                           preferred_element_type=jnp.float32)


def _dot_nt(a, b):
    return lax.dot_general(a, b, (((1,), (1,)), ((), ())), precision=PRECISE,
                           preferred_element_type=jnp.float32)


def _prologue(c_ref, b_ref, segc_ref, segr_ref, s_scr, neg_scr):
    s_scr[...] = _dot_nt(c_ref[...], b_ref[...])
    rows = s_scr.shape[0]
    row_i = lax.broadcasted_iota(jnp.int32, (rows, rows), 0)
    col_j = lax.broadcasted_iota(jnp.int32, (rows, rows), 1)
    keep = (col_j <= row_i) & (segc_ref[...] == segr_ref[...])
    neg_scr[...] = jnp.where(keep, 0.0, -jnp.inf).astype(jnp.float32)


def _fwd_kernel(c_ref, b_ref, segc_ref, segr_ref, x_ref, cumc_ref, cumr_ref, dtr_ref,
                y_ref, s_scr, neg_scr):
    @pl.when(pl.program_id(0) == 0)
    def _():
        _prologue(c_ref, b_ref, segc_ref, segr_ref, s_scr, neg_scr)

    for k in range(PAIR):
        cc = cumc_ref[0, :, k:k + 1]
        cr = cumr_ref[0, k:k + 1, :]
        dr = dtr_ref[0, k:k + 1, :]
        decays = jnp.exp(cc - cr + neg_scr[...])
        mixing = s_scr[...] * (decays * dr)
        y_ref[:, k * HEAD_DIM:(k + 1) * HEAD_DIM] = _dot(
            mixing, x_ref[:, k * HEAD_DIM:(k + 1) * HEAD_DIM])


def _bwd_kernel(c_ref, b_ref, segc_ref, segr_ref, x_ref, cumc_ref, cumr_ref, dtr_ref, g_ref,
                dx_ref, dcumc_ref, dcumr_ref, ddtr_ref, db_ref, dc_ref,
                s_scr, neg_scr, ds_scr):
    step = pl.program_id(0)

    @pl.when(step == 0)
    def _():
        _prologue(c_ref, b_ref, segc_ref, segr_ref, s_scr, neg_scr)
        ds_scr[...] = jnp.zeros_like(ds_scr)

    for k in range(PAIR):
        cc = cumc_ref[0, :, k:k + 1]
        cr = cumr_ref[0, k:k + 1, :]
        dr = dtr_ref[0, k:k + 1, :]
        decays = jnp.exp(cc - cr + neg_scr[...])
        weights = decays * dr
        scores = s_scr[...]
        mixing = scores * weights
        xh = x_ref[:, k * HEAD_DIM:(k + 1) * HEAD_DIM]
        gh = g_ref[:, k * HEAD_DIM:(k + 1) * HEAD_DIM]
        dx_ref[:, k * HEAD_DIM:(k + 1) * HEAD_DIM] = _dot_tn(mixing, gh)
        d_mix = _dot_nt(gh, xh)
        d_dec = d_mix * decays
        ds_scr[...] += d_dec * dr
        through = d_dec * scores
        d_dt_row = jnp.sum(through, axis=0, keepdims=True)
        q_mat = through * dr
        dcumc_ref[0, :, k:k + 1] = jnp.sum(q_mat, axis=1, keepdims=True)
        dcumr_ref[0, k:k + 1, :] = -(d_dt_row * dr)
        ddtr_ref[0, k:k + 1, :] = d_dt_row

    @pl.when(step == pl.num_programs(0) - 1)
    def _():
        dc_ref[...] = _dot(ds_scr[...], b_ref[...])
        db_ref[...] = _dot_tn(ds_scr[...], c_ref[...])


def _specs(rows, state):
    full = lambda shape: pl.BlockSpec(shape, lambda g: (0,) * len(shape))
    return [
        full((rows, state)),
        full((rows, state)),
        full((rows, 1)),
        full((1, rows)),
        pl.BlockSpec((rows, PAIR * HEAD_DIM), lambda g: (0, g)),
        pl.BlockSpec((1, rows, PAIR), lambda g: (g, 0, 0)),
        pl.BlockSpec((1, PAIR, rows), lambda g: (g, 0, 0)),
        pl.BlockSpec((1, PAIR, rows), lambda g: (g, 0, 0)),
    ]


def _prep(dt, cum, seg):
    rows, heads = dt.shape
    groups = heads // PAIR
    cumr = cum.T.reshape(groups, PAIR, rows)
    cumc = jnp.transpose(cumr, (0, 2, 1))
    dtr = dt.T.reshape(groups, PAIR, rows)
    segc = seg.reshape(rows, 1)
    segr = seg.reshape(1, rows)
    return cumc, cumr, dtr, segc, segr


def _fwd_call(x, dt, cum, b_mat, c_mat, seg):
    rows, inner = x.shape
    heads = dt.shape[1]
    groups = heads // PAIR
    state = b_mat.shape[1]
    cumc, cumr, dtr, segc, segr = _prep(dt, cum, seg)
    flops = 2 * rows * rows * state * 6 + heads * (2 * rows * rows * HEAD_DIM * 6 + 8 * rows * rows)
    return pl.pallas_call(
        _fwd_kernel,
        grid=(groups,),
        in_specs=_specs(rows, state),
        out_specs=pl.BlockSpec((rows, PAIR * HEAD_DIM), lambda g: (0, g)),
        out_shape=jax.ShapeDtypeStruct((rows, inner), jnp.float32),
        scratch_shapes=[pltpu.VMEM((rows, rows), jnp.float32),
                        pltpu.VMEM((rows, rows), jnp.float32)],
        compiler_params=pltpu.CompilerParams(dimension_semantics=("arbitrary",)),
        cost_estimate=pl.CostEstimate(flops=flops, transcendentals=heads * rows * rows,
                                      bytes_accessed=4 * (2 * rows * inner + 2 * rows * state)),
        name="ssd_fwd",
    )(c_mat, b_mat, segc, segr, x, cumc, cumr, dtr)


def _bwd_call(x, dt, cum, b_mat, c_mat, seg, g):
    rows, inner = x.shape
    heads = dt.shape[1]
    groups = heads // PAIR
    state = b_mat.shape[1]
    cumc, cumr, dtr, segc, segr = _prep(dt, cum, seg)
    full = lambda shape: pl.BlockSpec(shape, lambda gi: (0,) * len(shape))
    flops = 2 * rows * rows * state * 6 * 3 + heads * (2 * 2 * rows * rows * HEAD_DIM * 6 + 16 * rows * rows)
    dx, dcumc, dcumr, ddtr, db, dc = pl.pallas_call(
        _bwd_kernel,
        grid=(groups,),
        in_specs=_specs(rows, state) + [pl.BlockSpec((rows, PAIR * HEAD_DIM), lambda gi: (0, gi))],
        out_specs=[
            pl.BlockSpec((rows, PAIR * HEAD_DIM), lambda gi: (0, gi)),
            pl.BlockSpec((1, rows, PAIR), lambda gi: (gi, 0, 0)),
            pl.BlockSpec((1, PAIR, rows), lambda gi: (gi, 0, 0)),
            pl.BlockSpec((1, PAIR, rows), lambda gi: (gi, 0, 0)),
            full((rows, state)),
            full((rows, state)),
        ],
        out_shape=[
            jax.ShapeDtypeStruct((rows, inner), jnp.float32),
            jax.ShapeDtypeStruct((groups, rows, PAIR), jnp.float32),
            jax.ShapeDtypeStruct((groups, PAIR, rows), jnp.float32),
            jax.ShapeDtypeStruct((groups, PAIR, rows), jnp.float32),
            jax.ShapeDtypeStruct((rows, state), jnp.float32),
            jax.ShapeDtypeStruct((rows, state), jnp.float32),
        ],
        scratch_shapes=[pltpu.VMEM((rows, rows), jnp.float32),
                        pltpu.VMEM((rows, rows), jnp.float32),
                        pltpu.VMEM((rows, rows), jnp.float32)],
        compiler_params=pltpu.CompilerParams(dimension_semantics=("arbitrary",)),
        cost_estimate=pl.CostEstimate(flops=flops, transcendentals=heads * rows * rows,
                                      bytes_accessed=4 * (4 * rows * inner + 4 * rows * state)),
        name="ssd_bwd",
    )(c_mat, b_mat, segc, segr, x, cumc, cumr, dtr, g)
    d_cum = jnp.transpose(dcumc, (0, 2, 1)).reshape(heads, rows).T + dcumr.reshape(heads, rows).T
    d_dt = ddtr.reshape(heads, rows).T
    return dx, d_dt, d_cum, db, dc


@jax.custom_vjp
def ssd_core(x, dt, cum, b_mat, c_mat, seg):
    return _fwd_call(x, dt, cum, b_mat, c_mat, seg)


def _ssd_core_fwd(x, dt, cum, b_mat, c_mat, seg):
    return _fwd_call(x, dt, cum, b_mat, c_mat, seg), (x, dt, cum, b_mat, c_mat, seg)


def _ssd_core_bwd(res, g):
    x, dt, cum, b_mat, c_mat, seg = res
    dx, d_dt, d_cum, db, dc = _bwd_call(x, dt, cum, b_mat, c_mat, seg, g)
    return dx, d_dt, d_cum, db, dc, None


ssd_core.defvjp(_ssd_core_fwd, _ssd_core_bwd)

from jax.sharding import PartitionSpec as P
from jax.experimental.layout import Layout, with_layout_constraint

NORM_EPS = 1e-05


def contract_rows(first_op, second_op):
    return lax.dot_general(
        first_op, second_op, (((0,), (0,)), ((), ())), preferred_element_type=jnp.float32
    )


def contract_cols(first_op, second_op):
    return lax.dot_general(
        first_op, second_op, (((1,), (1,)), ((), ())), preferred_element_type=jnp.float32
    )


def segment_ids(lengths, row_count):
    seq_ends = jnp.cumsum(lengths)
    positions = jnp.arange(row_count, dtype=jnp.int32)
    return jnp.sum((positions[:, None] >= seq_ends[None, :]).astype(jnp.int32), axis=1)


def causal_conv(signal, kernel_w, kernel_b, segment):
    kernel_len = kernel_w.shape[0]
    row_count = signal.shape[0]
    summed = kernel_b[None, :] + kernel_w[kernel_len - 1][None, :] * signal
    for lag_steps in range(1, kernel_len):
        shifted = jnp.concatenate(
            [jnp.zeros((lag_steps, signal.shape[1]), jnp.float32), signal[: row_count - lag_steps]],
            axis=0,
        )
        earlier = jnp.concatenate(
            [jnp.full((lag_steps,), -1, jnp.int32), segment[: row_count - lag_steps]]
        )
        same_seq = (earlier == segment).astype(signal.dtype)
        summed = (
            summed + kernel_w[kernel_len - 1 - lag_steps][None, :] * shifted * same_seq[:, None]
        )
    return summed


def mixer_core(z_rows, x_rows, dt_raw, b_conv, c_conv, conv_wx, conv_bx, a_log, dt_bias,
               d_skip, segment=None):
    inner_n = x_rows.shape[1]
    heads_n = a_log.shape[0]
    x_conv = jax.nn.silu(causal_conv(x_rows, conv_wx, conv_bx, segment))
    steps_dt = jax.nn.softplus(dt_raw + dt_bias[None, :])
    decay = steps_dt * (-jnp.exp(a_log))[None, :]
    cum = jnp.cumsum(decay, axis=0)
    scanned = ssd_core(x_conv, steps_dt, cum, b_conv, c_conv, segment)
    skip = jnp.repeat(d_skip, inner_n // heads_n)
    mixed_out = scanned + skip[None, :] * x_conv
    return mixed_out * jax.nn.silu(z_rows)


def bc_core(bc_pre, conv_wbc, conv_bbc, segment=None):
    return jax.nn.silu(causal_conv(bc_pre, conv_wbc, conv_bbc, segment))


def per_device_body(tokens, cotangent, seq_lens, input_norm_gain, w_zx, w_bc, w_dt, conv_wx, conv_bx,
               conv_wbc, conv_bbc, a_log, dt_bias, d_skip, norm_gate, w_out):
    n_dp = lax.axis_size("dp")
    x_full = lax.all_gather(tokens, "tensor", axis=1, tiled=True)
    cot_full = lax.all_gather(cotangent, "tensor", axis=1, tiled=True)
    row_count = tokens.shape[0]
    feat_n = tokens.shape[1]
    d_model = x_full.shape[1]
    feat_start = lax.axis_index("tensor") * feat_n
    state_n = w_bc.shape[1] // 2
    inner_loc = norm_gate.shape[0]
    inner_all = inner_loc * lax.axis_size("tensor")
    segment = segment_ids(seq_lens[0], row_count)
    is_live = (segment < seq_lens.shape[1])[:, None]
    w_zx_flat = w_zx.reshape(d_model, 2 * inner_loc)
    tok_float = x_full.astype(jnp.float32)
    inverse_root_mean = lax.rsqrt(jnp.mean(tok_float * tok_float, axis=1, keepdims=True) + NORM_EPS)
    unit_scaled_input = tok_float * inverse_root_mean
    normed = (unit_scaled_input * input_norm_gain[None, :]).astype(jnp.bfloat16)
    zx_rows = jnp.dot(normed, w_zx_flat, preferred_element_type=jnp.float32)
    bc_pre = jnp.dot(normed, w_bc, preferred_element_type=jnp.float32)
    dt_raw = jnp.dot(normed, w_dt, preferred_element_type=jnp.float32)
    bc_post, bc_back = jax.vjp(partial(bc_core, segment=segment), bc_pre, conv_wbc, conv_bbc)
    gated_rows, core_back = jax.vjp(
        partial(mixer_core, segment=segment),
        zx_rows[:, :inner_loc], zx_rows[:, inner_loc:], dt_raw, bc_post[:, :state_n],
        bc_post[:, state_n:],
        conv_wx, conv_bx, a_log, dt_bias, d_skip,
    )
    cot_live = jnp.where(is_live, cot_full, jnp.zeros_like(cot_full))
    d_gate = contract_cols(cot_live, w_out)
    d_hat = d_gate * norm_gate[None, :]
    stats = doubling_all_reduce(
        jnp.concatenate([jnp.sum(gated_rows * gated_rows, axis=1, keepdims=True),
                         jnp.sum(d_hat * gated_rows, axis=1, keepdims=True)], axis=1),
        "tensor", lax.axis_size("tensor"))
    squares, cross_sum = stats[:, 0:1], stats[:, 1:2]
    r_gate = lax.rsqrt(squares / inner_all + NORM_EPS)
    gate_hat = gated_rows * r_gate
    gate_out = (gate_hat * norm_gate[None, :]).astype(jnp.bfloat16)
    branch_part = jnp.dot(gate_out, w_out, preferred_element_type=jnp.float32)
    grad_gate = jnp.sum(d_gate * gate_hat, axis=0)
    d_gated = r_gate * d_hat - gated_rows * (r_gate * r_gate * r_gate * cross_sum / inner_all)
    d_gated, branch_part = lax.optimization_barrier((d_gated, branch_part))
    branch = lax.psum_scatter(branch_part, "tensor", scatter_dimension=1, tiled=True)
    own_float = tokens.astype(jnp.float32)
    block_out = (own_float + jnp.where(is_live, branch, 0.0)).astype(jnp.bfloat16)
    d_z, d_x, d_dt, d_b, d_c, grad_conv_wx, grad_conv_bx, grad_a_log, grad_dt_bias, grad_d_skip = (
        core_back(d_gated)
    )
    n_tp = lax.axis_size("tensor")
    chunk = d_model // n_dp
    row_major = Layout(major_to_minor=(0, 1))
    d_z_half = d_z.astype(jnp.bfloat16)
    grads_early = with_layout_constraint(jnp.concatenate(
        [with_layout_constraint(contract_rows(cot_live, gate_out), row_major),
         with_layout_constraint(contract_rows(normed, d_z_half), row_major)],
        axis=1), row_major)
    d_x, d_dt, block_out = lax.optimization_barrier((d_x, d_dt, block_out))
    d_zx_half = jnp.concatenate([d_z_half, d_x.astype(jnp.bfloat16)], axis=1)
    d_dt_half = d_dt.astype(jnp.bfloat16)
    early_sum = split_reduce_scatter(grads_early, n_dp)
    grads_x = with_layout_constraint(contract_rows(normed, d_zx_half[:, inner_loc:]), row_major)
    x_sum = split_reduce_scatter(grads_x, n_dp)
    d_bc_part = jnp.concatenate([d_b, d_c], axis=1)
    partial_in = contract_cols(d_zx_half, w_zx_flat) + contract_cols(d_dt_half, w_dt)
    hat_gain = unit_scaled_input * input_norm_gain[None, :]
    row_part = jnp.sum(partial_in * hat_gain, axis=1, keepdims=True)
    d_bc_post = lax.psum(d_bc_part, "tensor")
    row_sum = doubling_all_reduce(row_part, "tensor", n_tp)
    d_bc, grad_conv_wbc, grad_conv_bbc = bc_back(d_bc_post)
    d_bc_half = d_bc.astype(jnp.bfloat16)
    bc_full = contract_cols(d_bc_half, w_bc)
    row_inner_product = (row_sum + jnp.sum(bc_full * hat_gain, axis=1, keepdims=True)) / d_model
    smalls = (grad_conv_wx, grad_conv_bx, grad_conv_wbc, grad_conv_bbc, grad_a_log,
              grad_dt_bias, grad_d_skip, grad_gate)
    flat_small = jnp.concatenate([v.reshape(-1) for v in smalls])
    small_cols = -(-flat_small.shape[0] // chunk)
    small_block = jnp.pad(flat_small, (0, small_cols * chunk - flat_small.shape[0])).reshape(
        chunk, small_cols)
    grads_small = with_layout_constraint(jnp.concatenate(
        [with_layout_constraint(
            contract_rows(normed, jnp.concatenate([d_bc_half, d_dt_half], axis=1)), row_major),
         jnp.tile(small_block, (n_dp, 1))], axis=1), row_major)
    small_sum_all = halving_reduce_scatter(grads_small, n_dp)
    own_part = lax.psum_scatter(partial_in, "tensor", scatter_dimension=1, tiled=True)
    own_hat = lax.dynamic_slice_in_dim(unit_scaled_input, feat_start, feat_n, 1)
    own_gain = lax.dynamic_slice_in_dim(input_norm_gain, feat_start, feat_n, 0)
    own_dn = own_part + lax.dynamic_slice_in_dim(bc_full, feat_start, feat_n, 1)
    own_dxhat = own_dn * own_gain[None, :]
    grad_in = doubling_all_reduce(jnp.sum(own_dn * own_hat, axis=0), "dp", n_dp)
    d_tokens = cotangent.astype(jnp.float32) + inverse_root_mean * (
        own_dxhat - own_hat * row_inner_product
    )
    grad_out_t_sum = early_sum[:, :inner_loc]
    grad_zx_sum = jnp.concatenate([early_sum[:, inner_loc:], x_sum], axis=1)
    grad_bc_sum = small_sum_all[:, :2 * state_n]
    grad_dt_sum = small_sum_all[:, 2 * state_n:2 * state_n + w_dt.shape[1]]
    small_sum = small_sum_all[:, 2 * state_n + w_dt.shape[1]:].reshape(-1)
    outs_small = []
    pos = 0
    for v in smalls:
        outs_small.append(small_sum[pos:pos + v.size].reshape(v.shape))
        pos += v.size
    grad_zx_out = grad_zx_sum.reshape(chunk, 2, inner_loc)
    return (block_out, d_tokens, grad_zx_out, grad_bc_sum, grad_dt_sum, grad_out_t_sum.T,
            *outs_small, grad_in)


def halving_reduce_scatter(x, n_dev, order=None):
    me = lax.axis_index("dp")
    bits = n_dev.bit_length() - 1
    chunk = x.shape[0] // n_dev
    cur = x.reshape((2,) * bits + (chunk, x.shape[1]))
    axes = list(range(bits - 1, -1, -1))
    for bit in (order if order is not None else range(bits)):
        pos = axes.index(bit)
        mine = (me >> bit) & 1
        keep = lax.dynamic_index_in_dim(cur, mine, axis=pos, keepdims=False)
        send = lax.dynamic_index_in_dim(cur, 1 - mine, axis=pos, keepdims=False)
        got = lax.ppermute(send, "dp", [(i, i ^ (1 << bit)) for i in range(n_dev)])
        cur = keep + got
        axes.pop(pos)
    return cur.reshape(chunk, x.shape[1])


def doubling_all_reduce(x, axis, n_dev):
    bit = 0
    while (1 << bit) < n_dev:
        x = x + lax.ppermute(x, axis, [(i, i ^ (1 << bit)) for i in range(n_dev)])
        bit += 1
    return x


def split_reduce_scatter(x, n_dev):
    bits = n_dev.bit_length() - 1
    half = x.shape[1] // 2
    first = tuple(range(bits))
    second = (0,) + tuple(range(bits - 1, 0, -1))
    return jnp.concatenate([halving_reduce_scatter(x[:, :half], n_dev, first),
                            halving_reduce_scatter(x[:, half:], n_dev, second)], axis=1)


def solution(mesh):
    in_specs = (
        P("dp", "tensor"), P("dp", "tensor"), P("dp", None), P(),
        P(None, None, "tensor"), P(), P(None, "tensor"), P(None, "tensor"), P("tensor"),
        P(), P(), P("tensor"), P("tensor"), P("tensor"), P("tensor"), P("tensor", None),
    )
    out_specs = (
        P("dp", "tensor"), P("dp", "tensor"), P("dp", None, "tensor"), P("dp", None),
        P("dp", "tensor"), P("tensor", "dp"), P(None, "tensor"), P("tensor"), P(), P(),
        P("tensor"), P("tensor"), P("tensor"), P("tensor"), P("tensor"),
    )
    return jax.shard_map(
        per_device_body, mesh=mesh, in_specs=in_specs, out_specs=out_specs, check_vma=False
    )
```

```python
from functools import partial


import jax
import jax.numpy as jnp
from jax import lax
from jax.experimental import pallas as pl
from jax.experimental.pallas import tpu as pltpu

PRECISE = lax.Precision.HIGHEST
HEAD_DIM = 64
PAIR = 2


def _dot(a, b):
    return jnp.dot(a, b, precision=PRECISE, preferred_element_type=jnp.float32)


def _dot_tn(a, b):
    return lax.dot_general(a, b, (((0,), (0,)), ((), ())), precision=PRECISE,
                           preferred_element_type=jnp.float32)


def _dot_nt(a, b):
    return lax.dot_general(a, b, (((1,), (1,)), ((), ())), precision=PRECISE,
                           preferred_element_type=jnp.float32)


def _prologue(c_ref, b_ref, segc_ref, segr_ref, s_scr, neg_scr):
    s_scr[...] = _dot_nt(c_ref[...], b_ref[...])
    rows = s_scr.shape[0]
    row_i = lax.broadcasted_iota(jnp.int32, (rows, rows), 0)
    col_j = lax.broadcasted_iota(jnp.int32, (rows, rows), 1)
    keep = (col_j <= row_i) & (segc_ref[...] == segr_ref[...])
    neg_scr[...] = jnp.where(keep, 0.0, -jnp.inf).astype(jnp.float32)


def _fwd_kernel(c_ref, b_ref, segc_ref, segr_ref, x_ref, cumc_ref, cumr_ref, dtr_ref,
                y_ref, s_scr, neg_scr):
    @pl.when(pl.program_id(0) == 0)
    def _():
        _prologue(c_ref, b_ref, segc_ref, segr_ref, s_scr, neg_scr)

    rows = s_scr.shape[0]
    half = rows // 2
    for k in range(PAIR):
        lanes = slice(k * HEAD_DIM, (k + 1) * HEAD_DIM)
        for r0, r1, c1 in ((0, half, half), (half, rows, rows)):
            cc = cumc_ref[0, r0:r1, k:k + 1]
            cr = cumr_ref[0, k:k + 1, 0:c1]
            dr = dtr_ref[0, k:k + 1, 0:c1]
            decays = jnp.exp(cc - cr + neg_scr[r0:r1, 0:c1])
            mixing = s_scr[r0:r1, 0:c1] * (decays * dr)
            y_ref[r0:r1, lanes] = _dot(mixing, x_ref[0:c1, lanes])


def _bwd_kernel(c_ref, b_ref, segc_ref, segr_ref, x_ref, cumc_ref, cumr_ref, dtr_ref, g_ref,
                dx_ref, dcumc_ref, dcumr_ref, ddtr_ref, db_ref, dc_ref,
                s_scr, neg_scr, ds_scr):
    step = pl.program_id(0)

    @pl.when(step == 0)
    def _():
        _prologue(c_ref, b_ref, segc_ref, segr_ref, s_scr, neg_scr)
        ds_scr[...] = jnp.zeros_like(ds_scr)

    rows = s_scr.shape[0]
    half = rows // 2
    for k in range(PAIR):
        lanes = slice(k * HEAD_DIM, (k + 1) * HEAD_DIM)
        xh = x_ref[:, lanes]
        gh = g_ref[:, lanes]
        parts = []
        for r0, r1, c1 in ((0, half, half), (half, rows, rows)):
            cc = cumc_ref[0, r0:r1, k:k + 1]
            cr = cumr_ref[0, k:k + 1, 0:c1]
            dr = dtr_ref[0, k:k + 1, 0:c1]
            decays = jnp.exp(cc - cr + neg_scr[r0:r1, 0:c1])
            scores = s_scr[r0:r1, 0:c1]
            mixing = scores * (decays * dr)
            g_blk = gh[r0:r1]
            dx_part = _dot_tn(mixing, g_blk)
            d_mix = _dot_nt(g_blk, xh[0:c1])
            d_dec = d_mix * decays
            ds_scr[r0:r1, 0:c1] += d_dec * dr
            through = d_dec * scores
            col_part = jnp.sum(through, axis=0, keepdims=True)
            dcumc_ref[0, r0:r1, k:k + 1] = jnp.sum(through * dr, axis=1, keepdims=True)
            parts.append((dx_part, col_part))
        (dx_top, col_top), (dx_all, col_all) = parts
        dx_ref[0:half, lanes] = dx_all[0:half] + dx_top
        dx_ref[half:rows, lanes] = dx_all[half:rows]
        dr_full = dtr_ref[0, k:k + 1, :]
        d_dt_lo = col_all[:, 0:half] + col_top
        d_dt_hi = col_all[:, half:rows]
        ddtr_ref[0, k:k + 1, 0:half] = d_dt_lo
        ddtr_ref[0, k:k + 1, half:rows] = d_dt_hi
        dcumr_ref[0, k:k + 1, 0:half] = -(d_dt_lo * dr_full[:, 0:half])
        dcumr_ref[0, k:k + 1, half:rows] = -(d_dt_hi * dr_full[:, half:rows])

    @pl.when(step == pl.num_programs(0) - 1)
    def _():
        dc_ref[...] = _dot(ds_scr[...], b_ref[...])
        db_ref[...] = _dot_tn(ds_scr[...], c_ref[...])


def _specs(rows, state):
    full = lambda shape: pl.BlockSpec(shape, lambda g: (0,) * len(shape))
    return [
        full((rows, state)),
        full((rows, state)),
        full((rows, 1)),
        full((1, rows)),
        pl.BlockSpec((rows, PAIR * HEAD_DIM), lambda g: (0, g)),
        pl.BlockSpec((1, rows, PAIR), lambda g: (g, 0, 0)),
        pl.BlockSpec((1, PAIR, rows), lambda g: (g, 0, 0)),
        pl.BlockSpec((1, PAIR, rows), lambda g: (g, 0, 0)),
    ]


def _prep(dt, cum, seg):
    rows, heads = dt.shape
    groups = heads // PAIR
    cumr = cum.T.reshape(groups, PAIR, rows)
    cumc = jnp.transpose(cumr, (0, 2, 1))
    dtr = dt.T.reshape(groups, PAIR, rows)
    segc = seg.reshape(rows, 1)
    segr = seg.reshape(1, rows)
    return cumc, cumr, dtr, segc, segr


def _fwd_call(x, dt, cum, b_mat, c_mat, seg):
    rows, inner = x.shape
    heads = dt.shape[1]
    groups = heads // PAIR
    state = b_mat.shape[1]
    cumc, cumr, dtr, segc, segr = _prep(dt, cum, seg)
    flops = 2 * rows * rows * state * 6 + heads * (2 * rows * rows * HEAD_DIM * 6 + 8 * rows * rows)
    return pl.pallas_call(
        _fwd_kernel,
        grid=(groups,),
        in_specs=_specs(rows, state),
        out_specs=pl.BlockSpec((rows, PAIR * HEAD_DIM), lambda g: (0, g)),
        out_shape=jax.ShapeDtypeStruct((rows, inner), jnp.float32),
        scratch_shapes=[pltpu.VMEM((rows, rows), jnp.float32),
                        pltpu.VMEM((rows, rows), jnp.float32)],
        compiler_params=pltpu.CompilerParams(dimension_semantics=("arbitrary",)),
        cost_estimate=pl.CostEstimate(flops=flops, transcendentals=heads * rows * rows,
                                      bytes_accessed=4 * (2 * rows * inner + 2 * rows * state)),
        name="ssd_fwd",
    )(c_mat, b_mat, segc, segr, x, cumc, cumr, dtr)


def _bwd_call(x, dt, cum, b_mat, c_mat, seg, g):
    rows, inner = x.shape
    heads = dt.shape[1]
    groups = heads // PAIR
    state = b_mat.shape[1]
    cumc, cumr, dtr, segc, segr = _prep(dt, cum, seg)
    full = lambda shape: pl.BlockSpec(shape, lambda gi: (0,) * len(shape))
    flops = 2 * rows * rows * state * 6 * 3 + heads * (2 * 2 * rows * rows * HEAD_DIM * 6 + 16 * rows * rows)
    dx, dcumc, dcumr, ddtr, db, dc = pl.pallas_call(
        _bwd_kernel,
        grid=(groups,),
        in_specs=_specs(rows, state) + [pl.BlockSpec((rows, PAIR * HEAD_DIM), lambda gi: (0, gi))],
        out_specs=[
            pl.BlockSpec((rows, PAIR * HEAD_DIM), lambda gi: (0, gi)),
            pl.BlockSpec((1, rows, PAIR), lambda gi: (gi, 0, 0)),
            pl.BlockSpec((1, PAIR, rows), lambda gi: (gi, 0, 0)),
            pl.BlockSpec((1, PAIR, rows), lambda gi: (gi, 0, 0)),
            full((rows, state)),
            full((rows, state)),
        ],
        out_shape=[
            jax.ShapeDtypeStruct((rows, inner), jnp.float32),
            jax.ShapeDtypeStruct((groups, rows, PAIR), jnp.float32),
            jax.ShapeDtypeStruct((groups, PAIR, rows), jnp.float32),
            jax.ShapeDtypeStruct((groups, PAIR, rows), jnp.float32),
            jax.ShapeDtypeStruct((rows, state), jnp.float32),
            jax.ShapeDtypeStruct((rows, state), jnp.float32),
        ],
        scratch_shapes=[pltpu.VMEM((rows, rows), jnp.float32),
                        pltpu.VMEM((rows, rows), jnp.float32),
                        pltpu.VMEM((rows, rows), jnp.float32)],
        compiler_params=pltpu.CompilerParams(dimension_semantics=("arbitrary",)),
        cost_estimate=pl.CostEstimate(flops=flops, transcendentals=heads * rows * rows,
                                      bytes_accessed=4 * (4 * rows * inner + 4 * rows * state)),
        name="ssd_bwd",
    )(c_mat, b_mat, segc, segr, x, cumc, cumr, dtr, g)
    d_cum = jnp.transpose(dcumc, (0, 2, 1)).reshape(heads, rows).T + dcumr.reshape(heads, rows).T
    d_dt = ddtr.reshape(heads, rows).T
    return dx, d_dt, d_cum, db, dc


@jax.custom_vjp
def ssd_core(x, dt, cum, b_mat, c_mat, seg):
    return _fwd_call(x, dt, cum, b_mat, c_mat, seg)


def _ssd_core_fwd(x, dt, cum, b_mat, c_mat, seg):
    return _fwd_call(x, dt, cum, b_mat, c_mat, seg), (x, dt, cum, b_mat, c_mat, seg)


def _ssd_core_bwd(res, g):
    x, dt, cum, b_mat, c_mat, seg = res
    dx, d_dt, d_cum, db, dc = _bwd_call(x, dt, cum, b_mat, c_mat, seg, g)
    return dx, d_dt, d_cum, db, dc, None


ssd_core.defvjp(_ssd_core_fwd, _ssd_core_bwd)

from jax.sharding import PartitionSpec as P
from jax.experimental.layout import Layout, with_layout_constraint

NORM_EPS = 1e-05


def contract_rows(first_op, second_op):
    return lax.dot_general(
        first_op, second_op, (((0,), (0,)), ((), ())), preferred_element_type=jnp.float32
    )


def contract_cols(first_op, second_op):
    return lax.dot_general(
        first_op, second_op, (((1,), (1,)), ((), ())), preferred_element_type=jnp.float32
    )


def segment_ids(lengths, row_count):
    seq_ends = jnp.cumsum(lengths)
    positions = jnp.arange(row_count, dtype=jnp.int32)
    return jnp.sum((positions[:, None] >= seq_ends[None, :]).astype(jnp.int32), axis=1)


def causal_conv(signal, kernel_w, kernel_b, segment):
    kernel_len = kernel_w.shape[0]
    row_count = signal.shape[0]
    summed = kernel_b[None, :] + kernel_w[kernel_len - 1][None, :] * signal
    for lag_steps in range(1, kernel_len):
        shifted = jnp.concatenate(
            [jnp.zeros((lag_steps, signal.shape[1]), jnp.float32), signal[: row_count - lag_steps]],
            axis=0,
        )
        earlier = jnp.concatenate(
            [jnp.full((lag_steps,), -1, jnp.int32), segment[: row_count - lag_steps]]
        )
        same_seq = (earlier == segment).astype(signal.dtype)
        summed = (
            summed + kernel_w[kernel_len - 1 - lag_steps][None, :] * shifted * same_seq[:, None]
        )
    return summed


def mixer_core(z_rows, x_rows, dt_raw, b_conv, c_conv, conv_wx, conv_bx, a_log, dt_bias,
               d_skip, segment=None):
    inner_n = x_rows.shape[1]
    heads_n = a_log.shape[0]
    x_conv = jax.nn.silu(causal_conv(x_rows, conv_wx, conv_bx, segment))
    steps_dt = jax.nn.softplus(dt_raw + dt_bias[None, :])
    decay = steps_dt * (-jnp.exp(a_log))[None, :]
    cum = jnp.cumsum(decay, axis=0)
    scanned = ssd_core(x_conv, steps_dt, cum, b_conv, c_conv, segment)
    skip = jnp.repeat(d_skip, inner_n // heads_n)
    mixed_out = scanned + skip[None, :] * x_conv
    return mixed_out * jax.nn.silu(z_rows)


def bc_core(bc_pre, conv_wbc, conv_bbc, segment=None):
    return jax.nn.silu(causal_conv(bc_pre, conv_wbc, conv_bbc, segment))


def per_device_body(tokens, cotangent, seq_lens, input_norm_gain, w_zx, w_bc, w_dt, conv_wx, conv_bx,
               conv_wbc, conv_bbc, a_log, dt_bias, d_skip, norm_gate, w_out):
    n_dp = lax.axis_size("dp")
    x_full = lax.all_gather(tokens, "tensor", axis=1, tiled=True)
    cot_full = lax.all_gather(cotangent, "tensor", axis=1, tiled=True)
    row_count = tokens.shape[0]
    feat_n = tokens.shape[1]
    d_model = x_full.shape[1]
    feat_start = lax.axis_index("tensor") * feat_n
    state_n = w_bc.shape[1] // 2
    inner_loc = norm_gate.shape[0]
    inner_all = inner_loc * lax.axis_size("tensor")
    segment = segment_ids(seq_lens[0], row_count)
    is_live = (segment < seq_lens.shape[1])[:, None]
    w_zx_flat = w_zx.reshape(d_model, 2 * inner_loc)
    tok_float = x_full.astype(jnp.float32)
    inverse_root_mean = lax.rsqrt(jnp.mean(tok_float * tok_float, axis=1, keepdims=True) + NORM_EPS)
    unit_scaled_input = tok_float * inverse_root_mean
    normed = (unit_scaled_input * input_norm_gain[None, :]).astype(jnp.bfloat16)
    zx_rows = jnp.dot(normed, w_zx_flat, preferred_element_type=jnp.float32)
    bc_pre = jnp.dot(normed, w_bc, preferred_element_type=jnp.float32)
    dt_raw = jnp.dot(normed, w_dt, preferred_element_type=jnp.float32)
    bc_post, bc_back = jax.vjp(partial(bc_core, segment=segment), bc_pre, conv_wbc, conv_bbc)
    gated_rows, core_back = jax.vjp(
        partial(mixer_core, segment=segment),
        zx_rows[:, :inner_loc], zx_rows[:, inner_loc:], dt_raw, bc_post[:, :state_n],
        bc_post[:, state_n:],
        conv_wx, conv_bx, a_log, dt_bias, d_skip,
    )
    cot_live = jnp.where(is_live, cot_full, jnp.zeros_like(cot_full))
    d_gate = contract_cols(cot_live, w_out)
    d_hat = d_gate * norm_gate[None, :]
    squares = doubling_all_reduce(jnp.sum(gated_rows * gated_rows, axis=1, keepdims=True),
                                  "tensor", lax.axis_size("tensor"))
    cross_sum = doubling_all_reduce(jnp.sum(d_hat * gated_rows, axis=1, keepdims=True),
                                    "tensor", lax.axis_size("tensor"))
    r_gate = lax.rsqrt(squares / inner_all + NORM_EPS)
    gate_hat = gated_rows * r_gate
    gate_out = (gate_hat * norm_gate[None, :]).astype(jnp.bfloat16)
    branch_part = jnp.dot(gate_out, w_out, preferred_element_type=jnp.float32)
    grad_gate = jnp.sum(d_gate * gate_hat, axis=0)
    d_gated = r_gate * d_hat - gated_rows * (r_gate * r_gate * r_gate * cross_sum / inner_all)
    d_gated, branch_part = lax.optimization_barrier((d_gated, branch_part))
    branch = lax.psum_scatter(branch_part, "tensor", scatter_dimension=1, tiled=True)
    own_float = tokens.astype(jnp.float32)
    block_out = (own_float + jnp.where(is_live, branch, 0.0)).astype(jnp.bfloat16)
    d_z, d_x, d_dt, d_b, d_c, grad_conv_wx, grad_conv_bx, grad_a_log, grad_dt_bias, grad_d_skip = (
        core_back(d_gated)
    )
    n_tp = lax.axis_size("tensor")
    chunk = d_model // n_dp
    row_major = Layout(major_to_minor=(0, 1))
    d_z_half = d_z.astype(jnp.bfloat16)
    grads_early = with_layout_constraint(jnp.concatenate(
        [with_layout_constraint(contract_rows(cot_live, gate_out), row_major),
         with_layout_constraint(contract_rows(normed, d_z_half), row_major)],
        axis=1), row_major)
    d_x, d_dt, block_out = lax.optimization_barrier((d_x, d_dt, block_out))
    d_zx_half = jnp.concatenate([d_z_half, d_x.astype(jnp.bfloat16)], axis=1)
    d_dt_half = d_dt.astype(jnp.bfloat16)
    early_sum = split_reduce_scatter(grads_early, n_dp)
    grads_x = with_layout_constraint(contract_rows(normed, d_zx_half[:, inner_loc:]), row_major)
    x_sum = split_reduce_scatter(grads_x, n_dp)
    d_bc_part = jnp.concatenate([d_b, d_c], axis=1)
    partial_in = contract_cols(d_zx_half, w_zx_flat) + contract_cols(d_dt_half, w_dt)
    hat_gain = unit_scaled_input * input_norm_gain[None, :]
    row_part = jnp.sum(lax.optimization_barrier(partial_in) * hat_gain, axis=1, keepdims=True)
    d_bc_post = lax.psum(d_bc_part, "tensor")
    row_sum = doubling_all_reduce(row_part, "tensor", n_tp)
    d_bc, grad_conv_wbc, grad_conv_bbc = bc_back(d_bc_post)
    d_bc_half = d_bc.astype(jnp.bfloat16)
    bc_full = contract_cols(d_bc_half, w_bc)
    row_inner_product = (row_sum + jnp.sum(bc_full * hat_gain, axis=1, keepdims=True)) / d_model
    smalls = (grad_conv_wx, grad_conv_bx, grad_conv_wbc, grad_conv_bbc, grad_a_log,
              grad_dt_bias, grad_d_skip, grad_gate)
    flat_small = jnp.concatenate([v.reshape(-1) for v in smalls])
    small_cols = -(-flat_small.shape[0] // chunk)
    small_block = jnp.pad(flat_small, (0, small_cols * chunk - flat_small.shape[0])).reshape(
        chunk, small_cols)
    grads_small = with_layout_constraint(jnp.concatenate(
        [with_layout_constraint(
            contract_rows(normed, jnp.concatenate([d_bc_half, d_dt_half], axis=1)), row_major),
         jnp.tile(small_block, (n_dp, 1))], axis=1), row_major)
    small_sum_all = halving_reduce_scatter(grads_small, n_dp)
    own_part = lax.psum_scatter(partial_in, "tensor", scatter_dimension=1, tiled=True)
    own_hat = lax.dynamic_slice_in_dim(unit_scaled_input, feat_start, feat_n, 1)
    own_gain = lax.dynamic_slice_in_dim(input_norm_gain, feat_start, feat_n, 0)
    own_dn = own_part + lax.dynamic_slice_in_dim(bc_full, feat_start, feat_n, 1)
    own_dxhat = own_dn * own_gain[None, :]
    grad_in = doubling_all_reduce(jnp.sum(own_dn * own_hat, axis=0), "dp", n_dp)
    d_tokens = cotangent.astype(jnp.float32) + inverse_root_mean * (
        own_dxhat - own_hat * row_inner_product
    )
    grad_out_t_sum = early_sum[:, :inner_loc]
    grad_zx_sum = jnp.concatenate([early_sum[:, inner_loc:], x_sum], axis=1)
    grad_bc_sum = small_sum_all[:, :2 * state_n]
    grad_dt_sum = small_sum_all[:, 2 * state_n:2 * state_n + w_dt.shape[1]]
    small_sum = small_sum_all[:, 2 * state_n + w_dt.shape[1]:].reshape(-1)
    outs_small = []
    pos = 0
    for v in smalls:
        outs_small.append(small_sum[pos:pos + v.size].reshape(v.shape))
        pos += v.size
    grad_zx_out = grad_zx_sum.reshape(chunk, 2, inner_loc)
    return (block_out, d_tokens, grad_zx_out, grad_bc_sum, grad_dt_sum, grad_out_t_sum.T,
            *outs_small, grad_in)


def halving_reduce_scatter(x, n_dev, order=None):
    me = lax.axis_index("dp")
    bits = n_dev.bit_length() - 1
    chunk = x.shape[0] // n_dev
    cur = x.reshape((2,) * bits + (chunk, x.shape[1]))
    axes = list(range(bits - 1, -1, -1))
    for bit in (order if order is not None else range(bits)):
        pos = axes.index(bit)
        mine = (me >> bit) & 1
        keep = lax.dynamic_index_in_dim(cur, mine, axis=pos, keepdims=False)
        send = lax.dynamic_index_in_dim(cur, 1 - mine, axis=pos, keepdims=False)
        got = lax.ppermute(send, "dp", [(i, i ^ (1 << bit)) for i in range(n_dev)])
        cur = keep + got
        axes.pop(pos)
    return cur.reshape(chunk, x.shape[1])


def doubling_all_reduce(x, axis, n_dev):
    bit = 0
    while (1 << bit) < n_dev:
        x = x + lax.ppermute(x, axis, [(i, i ^ (1 << bit)) for i in range(n_dev)])
        bit += 1
    return x


def split_reduce_scatter(x, n_dev):
    bits = n_dev.bit_length() - 1
    half = x.shape[1] // 2
    first = tuple(range(bits))
    second = (0,) + tuple(range(bits - 1, 0, -1))
    return jnp.concatenate([halving_reduce_scatter(x[:, :half], n_dev, first),
                            halving_reduce_scatter(x[:, half:], n_dev, second)], axis=1)


def solution(mesh):
    in_specs = (
        P("dp", "tensor"), P("dp", "tensor"), P("dp", None), P(),
        P(None, None, "tensor"), P(), P(None, "tensor"), P(None, "tensor"), P("tensor"),
        P(), P(), P("tensor"), P("tensor"), P("tensor"), P("tensor"), P("tensor", None),
    )
    out_specs = (
        P("dp", "tensor"), P("dp", "tensor"), P("dp", None, "tensor"), P("dp", None),
        P("dp", "tensor"), P("tensor", "dp"), P(None, "tensor"), P("tensor"), P(), P(),
        P("tensor"), P("tensor"), P("tensor"), P("tensor"), P("tensor"),
    )
    return jax.shard_map(
        per_device_body, mesh=mesh, in_specs=in_specs, out_specs=out_specs, check_vma=False
    )
```

```python
from functools import partial


import jax
import jax.numpy as jnp
from jax import lax
from jax.experimental import pallas as pl
from jax.experimental.pallas import tpu as pltpu

PRECISE = lax.Precision.HIGHEST
HEAD_DIM = 64
PAIR = 2


def _dot(a, b):
    return jnp.dot(a, b, precision=PRECISE, preferred_element_type=jnp.float32)


def _dot_tn(a, b):
    return lax.dot_general(a, b, (((0,), (0,)), ((), ())), precision=PRECISE,
                           preferred_element_type=jnp.float32)


def _dot_nt(a, b):
    return lax.dot_general(a, b, (((1,), (1,)), ((), ())), precision=PRECISE,
                           preferred_element_type=jnp.float32)


def _prologue(c_ref, b_ref, segc_ref, segr_ref, s_scr, neg_scr):
    s_scr[...] = _dot_nt(c_ref[...], b_ref[...])
    rows = s_scr.shape[0]
    row_i = lax.broadcasted_iota(jnp.int32, (rows, rows), 0)
    col_j = lax.broadcasted_iota(jnp.int32, (rows, rows), 1)
    keep = (col_j <= row_i) & (segc_ref[...] == segr_ref[...])
    neg_scr[...] = jnp.where(keep, 0.0, -jnp.inf).astype(jnp.float32)


def _fwd_kernel(c_ref, b_ref, segc_ref, segr_ref, x_ref, cumc_ref, cumr_ref, dtr_ref,
                y_ref, s_scr, neg_scr):
    @pl.when(pl.program_id(0) == 0)
    def _():
        _prologue(c_ref, b_ref, segc_ref, segr_ref, s_scr, neg_scr)

    rows = s_scr.shape[0]
    half = rows // 2
    for k in range(PAIR):
        lanes = slice(k * HEAD_DIM, (k + 1) * HEAD_DIM)
        for r0, r1, c1 in ((0, half, half), (half, rows, rows)):
            cc = cumc_ref[0, r0:r1, k:k + 1]
            cr = cumr_ref[0, k:k + 1, 0:c1]
            dr = dtr_ref[0, k:k + 1, 0:c1]
            decays = jnp.exp(cc - cr + neg_scr[r0:r1, 0:c1])
            mixing = s_scr[r0:r1, 0:c1] * (decays * dr)
            y_ref[r0:r1, lanes] = _dot(mixing, x_ref[0:c1, lanes])


def _bwd_kernel(c_ref, b_ref, segc_ref, segr_ref, x_ref, cumc_ref, cumr_ref, dtr_ref, g_ref,
                dx_ref, dcumc_ref, dcumr_ref, ddtr_ref, db_ref, dc_ref,
                s_scr, neg_scr, ds_scr):
    step = pl.program_id(0)

    @pl.when(step == 0)
    def _():
        _prologue(c_ref, b_ref, segc_ref, segr_ref, s_scr, neg_scr)
        ds_scr[...] = jnp.zeros_like(ds_scr)

    rows = s_scr.shape[0]
    half = rows // 2
    for k in range(PAIR):
        lanes = slice(k * HEAD_DIM, (k + 1) * HEAD_DIM)
        xh = x_ref[:, lanes]
        gh = g_ref[:, lanes]
        parts = []
        for r0, r1, c1 in ((0, half, half), (half, rows, rows)):
            cc = cumc_ref[0, r0:r1, k:k + 1]
            cr = cumr_ref[0, k:k + 1, 0:c1]
            dr = dtr_ref[0, k:k + 1, 0:c1]
            decays = jnp.exp(cc - cr + neg_scr[r0:r1, 0:c1])
            scores = s_scr[r0:r1, 0:c1]
            mixing = scores * (decays * dr)
            g_blk = gh[r0:r1]
            dx_part = _dot_tn(mixing, g_blk)
            d_mix = _dot_nt(g_blk, xh[0:c1])
            d_dec = d_mix * decays
            ds_scr[r0:r1, 0:c1] += d_dec * dr
            through = d_dec * scores
            col_part = jnp.sum(through, axis=0, keepdims=True)
            dcumc_ref[0, r0:r1, k:k + 1] = jnp.sum(through * dr, axis=1, keepdims=True)
            parts.append((dx_part, col_part))
        (dx_top, col_top), (dx_all, col_all) = parts
        dx_ref[0:half, lanes] = dx_all[0:half] + dx_top
        dx_ref[half:rows, lanes] = dx_all[half:rows]
        dr_full = dtr_ref[0, k:k + 1, :]
        d_dt_lo = col_all[:, 0:half] + col_top
        d_dt_hi = col_all[:, half:rows]
        ddtr_ref[0, k:k + 1, 0:half] = d_dt_lo
        ddtr_ref[0, k:k + 1, half:rows] = d_dt_hi
        dcumr_ref[0, k:k + 1, 0:half] = -(d_dt_lo * dr_full[:, 0:half])
        dcumr_ref[0, k:k + 1, half:rows] = -(d_dt_hi * dr_full[:, half:rows])

    @pl.when(step == pl.num_programs(0) - 1)
    def _():
        dc_ref[...] = _dot(ds_scr[...], b_ref[...])
        db_ref[...] = _dot_tn(ds_scr[...], c_ref[...])


def _specs(rows, state):
    full = lambda shape: pl.BlockSpec(shape, lambda g: (0,) * len(shape))
    return [
        full((rows, state)),
        full((rows, state)),
        full((rows, 1)),
        full((1, rows)),
        pl.BlockSpec((rows, PAIR * HEAD_DIM), lambda g: (0, g)),
        pl.BlockSpec((1, rows, PAIR), lambda g: (g, 0, 0)),
        pl.BlockSpec((1, PAIR, rows), lambda g: (g, 0, 0)),
        pl.BlockSpec((1, PAIR, rows), lambda g: (g, 0, 0)),
    ]


def _prep(dt, cum, seg):
    rows, heads = dt.shape
    groups = heads // PAIR
    cumr = cum.T.reshape(groups, PAIR, rows)
    cumc = jnp.transpose(cumr, (0, 2, 1))
    dtr = dt.T.reshape(groups, PAIR, rows)
    segc = seg.reshape(rows, 1)
    segr = seg.reshape(1, rows)
    return cumc, cumr, dtr, segc, segr


def _fwd_call(x, dt, cum, b_mat, c_mat, seg):
    rows, inner = x.shape
    heads = dt.shape[1]
    groups = heads // PAIR
    state = b_mat.shape[1]
    cumc, cumr, dtr, segc, segr = _prep(dt, cum, seg)
    flops = 2 * rows * rows * state * 6 + heads * (2 * rows * rows * HEAD_DIM * 6 + 8 * rows * rows)
    return pl.pallas_call(
        _fwd_kernel,
        grid=(groups,),
        in_specs=_specs(rows, state),
        out_specs=pl.BlockSpec((rows, PAIR * HEAD_DIM), lambda g: (0, g)),
        out_shape=jax.ShapeDtypeStruct((rows, inner), jnp.float32),
        scratch_shapes=[pltpu.VMEM((rows, rows), jnp.float32),
                        pltpu.VMEM((rows, rows), jnp.float32)],
        compiler_params=pltpu.CompilerParams(dimension_semantics=("arbitrary",)),
        cost_estimate=pl.CostEstimate(flops=flops, transcendentals=heads * rows * rows,
                                      bytes_accessed=4 * (2 * rows * inner + 2 * rows * state)),
        name="ssd_fwd",
    )(c_mat, b_mat, segc, segr, x, cumc, cumr, dtr)


def _bwd_call(x, dt, cum, b_mat, c_mat, seg, g):
    rows, inner = x.shape
    heads = dt.shape[1]
    groups = heads // PAIR
    state = b_mat.shape[1]
    cumc, cumr, dtr, segc, segr = _prep(dt, cum, seg)
    full = lambda shape: pl.BlockSpec(shape, lambda gi: (0,) * len(shape))
    flops = 2 * rows * rows * state * 6 * 3 + heads * (2 * 2 * rows * rows * HEAD_DIM * 6 + 16 * rows * rows)
    dx, dcumc, dcumr, ddtr, db, dc = pl.pallas_call(
        _bwd_kernel,
        grid=(groups,),
        in_specs=_specs(rows, state) + [pl.BlockSpec((rows, PAIR * HEAD_DIM), lambda gi: (0, gi))],
        out_specs=[
            pl.BlockSpec((rows, PAIR * HEAD_DIM), lambda gi: (0, gi)),
            pl.BlockSpec((1, rows, PAIR), lambda gi: (gi, 0, 0)),
            pl.BlockSpec((1, PAIR, rows), lambda gi: (gi, 0, 0)),
            pl.BlockSpec((1, PAIR, rows), lambda gi: (gi, 0, 0)),
            full((rows, state)),
            full((rows, state)),
        ],
        out_shape=[
            jax.ShapeDtypeStruct((rows, inner), jnp.float32),
            jax.ShapeDtypeStruct((groups, rows, PAIR), jnp.float32),
            jax.ShapeDtypeStruct((groups, PAIR, rows), jnp.float32),
            jax.ShapeDtypeStruct((groups, PAIR, rows), jnp.float32),
            jax.ShapeDtypeStruct((rows, state), jnp.float32),
            jax.ShapeDtypeStruct((rows, state), jnp.float32),
        ],
        scratch_shapes=[pltpu.VMEM((rows, rows), jnp.float32),
                        pltpu.VMEM((rows, rows), jnp.float32),
                        pltpu.VMEM((rows, rows), jnp.float32)],
        compiler_params=pltpu.CompilerParams(dimension_semantics=("arbitrary",)),
        cost_estimate=pl.CostEstimate(flops=flops, transcendentals=heads * rows * rows,
                                      bytes_accessed=4 * (4 * rows * inner + 4 * rows * state)),
        name="ssd_bwd",
    )(c_mat, b_mat, segc, segr, x, cumc, cumr, dtr, g)
    d_cum = jnp.transpose(dcumc, (0, 2, 1)).reshape(heads, rows).T + dcumr.reshape(heads, rows).T
    d_dt = ddtr.reshape(heads, rows).T
    return dx, d_dt, d_cum, db, dc


@jax.custom_vjp
def ssd_core(x, dt, cum, b_mat, c_mat, seg):
    return _fwd_call(x, dt, cum, b_mat, c_mat, seg)


def _ssd_core_fwd(x, dt, cum, b_mat, c_mat, seg):
    return _fwd_call(x, dt, cum, b_mat, c_mat, seg), (x, dt, cum, b_mat, c_mat, seg)


def _ssd_core_bwd(res, g):
    x, dt, cum, b_mat, c_mat, seg = res
    dx, d_dt, d_cum, db, dc = _bwd_call(x, dt, cum, b_mat, c_mat, seg, g)
    return dx, d_dt, d_cum, db, dc, None


ssd_core.defvjp(_ssd_core_fwd, _ssd_core_bwd)

from jax.sharding import PartitionSpec as P
from jax.experimental.layout import Layout, with_layout_constraint

NORM_EPS = 1e-05


def contract_rows(first_op, second_op):
    return lax.dot_general(
        first_op, second_op, (((0,), (0,)), ((), ())), preferred_element_type=jnp.float32
    )


def contract_cols(first_op, second_op):
    return lax.dot_general(
        first_op, second_op, (((1,), (1,)), ((), ())), preferred_element_type=jnp.float32
    )


def segment_ids(lengths, row_count):
    seq_ends = jnp.cumsum(lengths)
    positions = jnp.arange(row_count, dtype=jnp.int32)
    return jnp.sum((positions[:, None] >= seq_ends[None, :]).astype(jnp.int32), axis=1)


def causal_conv(signal, kernel_w, kernel_b, segment):
    kernel_len = kernel_w.shape[0]
    row_count = signal.shape[0]
    summed = kernel_b[None, :] + kernel_w[kernel_len - 1][None, :] * signal
    for lag_steps in range(1, kernel_len):
        shifted = jnp.concatenate(
            [jnp.zeros((lag_steps, signal.shape[1]), jnp.float32), signal[: row_count - lag_steps]],
            axis=0,
        )
        earlier = jnp.concatenate(
            [jnp.full((lag_steps,), -1, jnp.int32), segment[: row_count - lag_steps]]
        )
        same_seq = (earlier == segment).astype(signal.dtype)
        summed = (
            summed + kernel_w[kernel_len - 1 - lag_steps][None, :] * shifted * same_seq[:, None]
        )
    return summed


def mixer_core(z_rows, x_rows, dt_raw, b_conv, c_conv, conv_wx, conv_bx, a_log, dt_bias,
               d_skip, segment=None):
    inner_n = x_rows.shape[1]
    heads_n = a_log.shape[0]
    x_conv = jax.nn.silu(causal_conv(x_rows, conv_wx, conv_bx, segment))
    steps_dt = jax.nn.softplus(dt_raw + dt_bias[None, :])
    decay = steps_dt * (-jnp.exp(a_log))[None, :]
    cum = jnp.cumsum(decay, axis=0)
    scanned = ssd_core(x_conv, steps_dt, cum, b_conv, c_conv, segment)
    skip = jnp.repeat(d_skip, inner_n // heads_n)
    mixed_out = scanned + skip[None, :] * x_conv
    return mixed_out * jax.nn.silu(z_rows)


def bc_core(bc_pre, conv_wbc, conv_bbc, segment=None):
    return jax.nn.silu(causal_conv(bc_pre, conv_wbc, conv_bbc, segment))


def per_device_body(tokens, cotangent, seq_lens, input_norm_gain, w_zx, w_bc, w_dt, conv_wx, conv_bx,
               conv_wbc, conv_bbc, a_log, dt_bias, d_skip, norm_gate, w_out):
    n_dp = lax.axis_size("dp")
    x_full = lax.all_gather(tokens, "tensor", axis=1, tiled=True)
    cot_full = lax.all_gather(cotangent, "tensor", axis=1, tiled=True)
    row_count = tokens.shape[0]
    feat_n = tokens.shape[1]
    d_model = x_full.shape[1]
    feat_start = lax.axis_index("tensor") * feat_n
    state_n = w_bc.shape[1] // 2
    inner_loc = norm_gate.shape[0]
    inner_all = inner_loc * lax.axis_size("tensor")
    segment = segment_ids(seq_lens[0], row_count)
    is_live = (segment < seq_lens.shape[1])[:, None]
    w_zx_flat = w_zx.reshape(d_model, 2 * inner_loc)
    tok_float = x_full.astype(jnp.float32)
    inverse_root_mean = lax.rsqrt(jnp.mean(tok_float * tok_float, axis=1, keepdims=True) + NORM_EPS)
    unit_scaled_input = tok_float * inverse_root_mean
    normed = (unit_scaled_input * input_norm_gain[None, :]).astype(jnp.bfloat16)
    zx_rows = jnp.dot(normed, w_zx_flat, preferred_element_type=jnp.float32)
    bc_pre = jnp.dot(normed, w_bc, preferred_element_type=jnp.float32)
    dt_raw = jnp.dot(normed, w_dt, preferred_element_type=jnp.float32)
    bc_post, bc_back = jax.vjp(partial(bc_core, segment=segment), bc_pre, conv_wbc, conv_bbc)
    gated_rows, core_back = jax.vjp(
        partial(mixer_core, segment=segment),
        zx_rows[:, :inner_loc], zx_rows[:, inner_loc:], dt_raw, bc_post[:, :state_n],
        bc_post[:, state_n:],
        conv_wx, conv_bx, a_log, dt_bias, d_skip,
    )
    cot_live = jnp.where(is_live, cot_full, jnp.zeros_like(cot_full))
    d_gate = contract_cols(cot_live, w_out)
    d_hat = d_gate * norm_gate[None, :]
    stats = doubling_all_reduce(
        jnp.concatenate([jnp.sum(gated_rows * gated_rows, axis=1, keepdims=True),
                         jnp.sum(d_hat * gated_rows, axis=1, keepdims=True)], axis=1),
        "tensor", lax.axis_size("tensor"))
    squares, cross_sum = stats[:, 0:1], stats[:, 1:2]
    r_gate = lax.rsqrt(squares / inner_all + NORM_EPS)
    gate_hat = gated_rows * r_gate
    gate_out = (gate_hat * norm_gate[None, :]).astype(jnp.bfloat16)
    branch_part = jnp.dot(gate_out, w_out, preferred_element_type=jnp.float32)
    grad_gate = jnp.sum(d_gate * gate_hat, axis=0)
    d_gated = r_gate * d_hat - gated_rows * (r_gate * r_gate * r_gate * cross_sum / inner_all)
    d_gated, branch_part = lax.optimization_barrier((d_gated, branch_part))
    branch = lax.psum_scatter(branch_part, "tensor", scatter_dimension=1, tiled=True)
    own_float = tokens.astype(jnp.float32)
    block_out = (own_float + jnp.where(is_live, branch, 0.0)).astype(jnp.bfloat16)
    d_z, d_x, d_dt, d_b, d_c, grad_conv_wx, grad_conv_bx, grad_a_log, grad_dt_bias, grad_d_skip = (
        core_back(d_gated)
    )
    n_tp = lax.axis_size("tensor")
    chunk = d_model // n_dp
    row_major = Layout(major_to_minor=(0, 1))
    d_z_half = d_z.astype(jnp.bfloat16)
    grads_early = with_layout_constraint(jnp.concatenate(
        [with_layout_constraint(contract_rows(cot_live, gate_out), row_major),
         with_layout_constraint(contract_rows(normed, d_z_half), row_major)],
        axis=1), row_major)
    d_x, d_dt, block_out = lax.optimization_barrier((d_x, d_dt, block_out))
    d_zx_half = jnp.concatenate([d_z_half, d_x.astype(jnp.bfloat16)], axis=1)
    d_dt_half = d_dt.astype(jnp.bfloat16)
    early_sum = split_reduce_scatter(grads_early, n_dp)
    grads_x = with_layout_constraint(contract_rows(normed, d_zx_half[:, inner_loc:]), row_major)
    x_sum = split_reduce_scatter(grads_x, n_dp)
    d_bc_part = jnp.concatenate([d_b, d_c], axis=1)
    partial_in = contract_cols(d_zx_half, w_zx_flat) + contract_cols(d_dt_half, w_dt)
    hat_gain = unit_scaled_input * input_norm_gain[None, :]
    row_part = jnp.sum(lax.optimization_barrier(partial_in) * hat_gain, axis=1, keepdims=True)
    d_bc_post = lax.psum(d_bc_part, "tensor")
    row_sum = doubling_all_reduce(row_part, "tensor", n_tp)
    d_bc, grad_conv_wbc, grad_conv_bbc = bc_back(d_bc_post)
    d_bc_half = d_bc.astype(jnp.bfloat16)
    bc_full = contract_cols(d_bc_half, w_bc)
    row_inner_product = (row_sum + jnp.sum(bc_full * hat_gain, axis=1, keepdims=True)) / d_model
    smalls = (grad_conv_wx, grad_conv_bx, grad_conv_wbc, grad_conv_bbc, grad_a_log,
              grad_dt_bias, grad_d_skip, grad_gate)
    flat_small = jnp.concatenate([v.reshape(-1) for v in smalls])
    small_cols = -(-flat_small.shape[0] // chunk)
    small_block = jnp.pad(flat_small, (0, small_cols * chunk - flat_small.shape[0])).reshape(
        chunk, small_cols)
    grads_small = with_layout_constraint(jnp.concatenate(
        [with_layout_constraint(
            contract_rows(normed, jnp.concatenate([d_bc_half, d_dt_half], axis=1)), row_major),
         jnp.tile(small_block, (n_dp, 1))], axis=1), row_major)
    small_sum_all = halving_reduce_scatter(grads_small, n_dp)
    own_part = lax.psum_scatter(partial_in, "tensor", scatter_dimension=1, tiled=True)
    own_hat = lax.dynamic_slice_in_dim(unit_scaled_input, feat_start, feat_n, 1)
    own_gain = lax.dynamic_slice_in_dim(input_norm_gain, feat_start, feat_n, 0)
    own_dn = own_part + lax.dynamic_slice_in_dim(bc_full, feat_start, feat_n, 1)
    own_dxhat = own_dn * own_gain[None, :]
    grad_in = doubling_all_reduce(jnp.sum(own_dn * own_hat, axis=0), "dp", n_dp)
    d_tokens = cotangent.astype(jnp.float32) + inverse_root_mean * (
        own_dxhat - own_hat * row_inner_product
    )
    grad_out_t_sum = early_sum[:, :inner_loc]
    grad_zx_sum = jnp.concatenate([early_sum[:, inner_loc:], x_sum], axis=1)
    grad_bc_sum = small_sum_all[:, :2 * state_n]
    grad_dt_sum = small_sum_all[:, 2 * state_n:2 * state_n + w_dt.shape[1]]
    small_sum = small_sum_all[:, 2 * state_n + w_dt.shape[1]:].reshape(-1)
    outs_small = []
    pos = 0
    for v in smalls:
        outs_small.append(small_sum[pos:pos + v.size].reshape(v.shape))
        pos += v.size
    grad_zx_out = grad_zx_sum.reshape(chunk, 2, inner_loc)
    return (block_out, d_tokens, grad_zx_out, grad_bc_sum, grad_dt_sum, grad_out_t_sum.T,
            *outs_small, grad_in)


def halving_reduce_scatter(x, n_dev, order=None):
    me = lax.axis_index("dp")
    bits = n_dev.bit_length() - 1
    chunk = x.shape[0] // n_dev
    cur = x.reshape((2,) * bits + (chunk, x.shape[1]))
    axes = list(range(bits - 1, -1, -1))
    for bit in (order if order is not None else range(bits)):
        pos = axes.index(bit)
        mine = (me >> bit) & 1
        keep = lax.dynamic_index_in_dim(cur, mine, axis=pos, keepdims=False)
        send = lax.dynamic_index_in_dim(cur, 1 - mine, axis=pos, keepdims=False)
        got = lax.ppermute(send, "dp", [(i, i ^ (1 << bit)) for i in range(n_dev)])
        cur = keep + got
        axes.pop(pos)
    return cur.reshape(chunk, x.shape[1])


def doubling_all_reduce(x, axis, n_dev):
    bit = 0
    while (1 << bit) < n_dev:
        x = x + lax.ppermute(x, axis, [(i, i ^ (1 << bit)) for i in range(n_dev)])
        bit += 1
    return x


def split_reduce_scatter(x, n_dev):
    bits = n_dev.bit_length() - 1
    half = x.shape[1] // 2
    first = tuple(range(bits))
    second = (0,) + tuple(range(bits - 1, 0, -1))
    return jnp.concatenate([halving_reduce_scatter(x[:, :half], n_dev, first),
                            halving_reduce_scatter(x[:, half:], n_dev, second)], axis=1)


def solution(mesh):
    in_specs = (
        P("dp", "tensor"), P("dp", "tensor"), P("dp", None), P(),
        P(None, None, "tensor"), P(), P(None, "tensor"), P(None, "tensor"), P("tensor"),
        P(), P(), P("tensor"), P("tensor"), P("tensor"), P("tensor"), P("tensor", None),
    )
    out_specs = (
        P("dp", "tensor"), P("dp", "tensor"), P("dp", None, "tensor"), P("dp", None),
        P("dp", "tensor"), P("tensor", "dp"), P(None, "tensor"), P("tensor"), P(), P(),
        P("tensor"), P("tensor"), P("tensor"), P("tensor"), P("tensor"),
    )
    return jax.shard_map(
        per_device_body, mesh=mesh, in_specs=in_specs, out_specs=out_specs, check_vma=False
    )
```

```python
from functools import partial


import jax
import jax.numpy as jnp
from jax import lax
from jax.experimental import pallas as pl
from jax.experimental.pallas import tpu as pltpu

PRECISE = lax.Precision.HIGHEST
HEAD_DIM = 64
PAIR = 2


def _dot(a, b):
    return jnp.dot(a, b, precision=PRECISE, preferred_element_type=jnp.float32)


def _dot_tn(a, b):
    return lax.dot_general(a, b, (((0,), (0,)), ((), ())), precision=PRECISE,
                           preferred_element_type=jnp.float32)


def _dot_nt(a, b):
    return lax.dot_general(a, b, (((1,), (1,)), ((), ())), precision=PRECISE,
                           preferred_element_type=jnp.float32)


def _prologue(c_ref, b_ref, segc_ref, segr_ref, s_scr, neg_scr):
    s_scr[...] = _dot_nt(c_ref[...], b_ref[...])
    rows = s_scr.shape[0]
    row_i = lax.broadcasted_iota(jnp.int32, (rows, rows), 0)
    col_j = lax.broadcasted_iota(jnp.int32, (rows, rows), 1)
    keep = (col_j <= row_i) & (segc_ref[...] == segr_ref[...])
    neg_scr[...] = jnp.where(keep, 0.0, -jnp.inf).astype(jnp.float32)


def _fwd_kernel(c_ref, b_ref, segc_ref, segr_ref, x_ref, cumc_ref, cumr_ref, dtr_ref,
                y_ref, s_scr, neg_scr):
    @pl.when(pl.program_id(0) == 0)
    def _():
        _prologue(c_ref, b_ref, segc_ref, segr_ref, s_scr, neg_scr)

    rows = s_scr.shape[0]
    half = rows // 2
    for k in range(PAIR):
        lanes = slice(k * HEAD_DIM, (k + 1) * HEAD_DIM)
        for r0, r1, c1 in ((0, half, half), (half, rows, rows)):
            cc = cumc_ref[0, r0:r1, k:k + 1]
            cr = cumr_ref[0, k:k + 1, 0:c1]
            dr = dtr_ref[0, k:k + 1, 0:c1]
            decays = jnp.exp(cc - cr + neg_scr[r0:r1, 0:c1])
            mixing = s_scr[r0:r1, 0:c1] * (decays * dr)
            y_ref[r0:r1, lanes] = _dot(mixing, x_ref[0:c1, lanes])


def _bwd_kernel(c_ref, b_ref, segc_ref, segr_ref, x_ref, cumc_ref, cumr_ref, dtr_ref, g_ref,
                dx_ref, dcumc_ref, dcumr_ref, ddtr_ref, db_ref, dc_ref,
                s_scr, neg_scr, ds_scr):
    step = pl.program_id(0)

    @pl.when(step == 0)
    def _():
        _prologue(c_ref, b_ref, segc_ref, segr_ref, s_scr, neg_scr)
        ds_scr[...] = jnp.zeros_like(ds_scr)

    rows = s_scr.shape[0]
    half = rows // 2
    for k in range(PAIR):
        lanes = slice(k * HEAD_DIM, (k + 1) * HEAD_DIM)
        xh = x_ref[:, lanes]
        gh = g_ref[:, lanes]
        parts = []
        for r0, r1, c1 in ((0, half, half), (half, rows, rows)):
            cc = cumc_ref[0, r0:r1, k:k + 1]
            cr = cumr_ref[0, k:k + 1, 0:c1]
            dr = dtr_ref[0, k:k + 1, 0:c1]
            decays = jnp.exp(cc - cr + neg_scr[r0:r1, 0:c1])
            scores = s_scr[r0:r1, 0:c1]
            mixing = scores * (decays * dr)
            g_blk = gh[r0:r1]
            dx_part = _dot_tn(mixing, g_blk)
            d_mix = _dot_nt(g_blk, xh[0:c1])
            d_dec = d_mix * decays
            ds_scr[r0:r1, 0:c1] += d_dec * dr
            through = d_dec * scores
            col_part = jnp.sum(through, axis=0, keepdims=True)
            dcumc_ref[0, r0:r1, k:k + 1] = jnp.sum(through * dr, axis=1, keepdims=True)
            parts.append((dx_part, col_part))
        (dx_top, col_top), (dx_all, col_all) = parts
        dx_ref[0:half, lanes] = dx_all[0:half] + dx_top
        dx_ref[half:rows, lanes] = dx_all[half:rows]
        dr_full = dtr_ref[0, k:k + 1, :]
        d_dt_lo = col_all[:, 0:half] + col_top
        d_dt_hi = col_all[:, half:rows]
        ddtr_ref[0, k:k + 1, 0:half] = d_dt_lo
        ddtr_ref[0, k:k + 1, half:rows] = d_dt_hi
        dcumr_ref[0, k:k + 1, 0:half] = -(d_dt_lo * dr_full[:, 0:half])
        dcumr_ref[0, k:k + 1, half:rows] = -(d_dt_hi * dr_full[:, half:rows])

    @pl.when(step == pl.num_programs(0) - 1)
    def _():
        dc_ref[...] = _dot(ds_scr[...], b_ref[...])
        db_ref[...] = _dot_tn(ds_scr[...], c_ref[...])


def _specs(rows, state):
    full = lambda shape: pl.BlockSpec(shape, lambda g: (0,) * len(shape))
    return [
        full((rows, state)),
        full((rows, state)),
        full((rows, 1)),
        full((1, rows)),
        pl.BlockSpec((rows, PAIR * HEAD_DIM), lambda g: (0, g)),
        pl.BlockSpec((1, rows, PAIR), lambda g: (g, 0, 0)),
        pl.BlockSpec((1, PAIR, rows), lambda g: (g, 0, 0)),
        pl.BlockSpec((1, PAIR, rows), lambda g: (g, 0, 0)),
    ]


def _prep(dt, cum, seg):
    rows, heads = dt.shape
    groups = heads // PAIR
    cumr = cum.T.reshape(groups, PAIR, rows)
    cumc = jnp.transpose(cumr, (0, 2, 1))
    dtr = dt.T.reshape(groups, PAIR, rows)
    segc = seg.reshape(rows, 1)
    segr = seg.reshape(1, rows)
    return cumc, cumr, dtr, segc, segr


def _fwd_call(x, dt, cum, b_mat, c_mat, seg):
    rows, inner = x.shape
    heads = dt.shape[1]
    groups = heads // PAIR
    state = b_mat.shape[1]
    cumc, cumr, dtr, segc, segr = _prep(dt, cum, seg)
    flops = 2 * rows * rows * state * 6 + heads * (2 * rows * rows * HEAD_DIM * 6 + 8 * rows * rows)
    return pl.pallas_call(
        _fwd_kernel,
        grid=(groups,),
        in_specs=_specs(rows, state),
        out_specs=pl.BlockSpec((rows, PAIR * HEAD_DIM), lambda g: (0, g)),
        out_shape=jax.ShapeDtypeStruct((rows, inner), jnp.float32),
        scratch_shapes=[pltpu.VMEM((rows, rows), jnp.float32),
                        pltpu.VMEM((rows, rows), jnp.float32)],
        compiler_params=pltpu.CompilerParams(dimension_semantics=("arbitrary",)),
        cost_estimate=pl.CostEstimate(flops=flops, transcendentals=heads * rows * rows,
                                      bytes_accessed=4 * (2 * rows * inner + 2 * rows * state)),
        name="ssd_fwd",
    )(c_mat, b_mat, segc, segr, x, cumc, cumr, dtr)


def _bwd_call(x, dt, cum, b_mat, c_mat, seg, g):
    rows, inner = x.shape
    heads = dt.shape[1]
    groups = heads // PAIR
    state = b_mat.shape[1]
    cumc, cumr, dtr, segc, segr = _prep(dt, cum, seg)
    full = lambda shape: pl.BlockSpec(shape, lambda gi: (0,) * len(shape))
    flops = 2 * rows * rows * state * 6 * 3 + heads * (2 * 2 * rows * rows * HEAD_DIM * 6 + 16 * rows * rows)
    dx, dcumc, dcumr, ddtr, db, dc = pl.pallas_call(
        _bwd_kernel,
        grid=(groups,),
        in_specs=_specs(rows, state) + [pl.BlockSpec((rows, PAIR * HEAD_DIM), lambda gi: (0, gi))],
        out_specs=[
            pl.BlockSpec((rows, PAIR * HEAD_DIM), lambda gi: (0, gi)),
            pl.BlockSpec((1, rows, PAIR), lambda gi: (gi, 0, 0)),
            pl.BlockSpec((1, PAIR, rows), lambda gi: (gi, 0, 0)),
            pl.BlockSpec((1, PAIR, rows), lambda gi: (gi, 0, 0)),
            full((rows, state)),
            full((rows, state)),
        ],
        out_shape=[
            jax.ShapeDtypeStruct((rows, inner), jnp.float32),
            jax.ShapeDtypeStruct((groups, rows, PAIR), jnp.float32),
            jax.ShapeDtypeStruct((groups, PAIR, rows), jnp.float32),
            jax.ShapeDtypeStruct((groups, PAIR, rows), jnp.float32),
            jax.ShapeDtypeStruct((rows, state), jnp.float32),
            jax.ShapeDtypeStruct((rows, state), jnp.float32),
        ],
        scratch_shapes=[pltpu.VMEM((rows, rows), jnp.float32),
                        pltpu.VMEM((rows, rows), jnp.float32),
                        pltpu.VMEM((rows, rows), jnp.float32)],
        compiler_params=pltpu.CompilerParams(dimension_semantics=("arbitrary",)),
        cost_estimate=pl.CostEstimate(flops=flops, transcendentals=heads * rows * rows,
                                      bytes_accessed=4 * (4 * rows * inner + 4 * rows * state)),
        name="ssd_bwd",
    )(c_mat, b_mat, segc, segr, x, cumc, cumr, dtr, g)
    d_cum = jnp.transpose(dcumc, (0, 2, 1)).reshape(heads, rows).T + dcumr.reshape(heads, rows).T
    d_dt = ddtr.reshape(heads, rows).T
    return dx, d_dt, d_cum, db, dc


@jax.custom_vjp
def ssd_core(x, dt, cum, b_mat, c_mat, seg):
    return _fwd_call(x, dt, cum, b_mat, c_mat, seg)


def _ssd_core_fwd(x, dt, cum, b_mat, c_mat, seg):
    return _fwd_call(x, dt, cum, b_mat, c_mat, seg), (x, dt, cum, b_mat, c_mat, seg)


def _ssd_core_bwd(res, g):
    x, dt, cum, b_mat, c_mat, seg = res
    dx, d_dt, d_cum, db, dc = _bwd_call(x, dt, cum, b_mat, c_mat, seg, g)
    return dx, d_dt, d_cum, db, dc, None


ssd_core.defvjp(_ssd_core_fwd, _ssd_core_bwd)

from jax.sharding import PartitionSpec as P
from jax.experimental.layout import Layout, with_layout_constraint

NORM_EPS = 1e-05


def contract_rows(first_op, second_op):
    return lax.dot_general(
        first_op, second_op, (((0,), (0,)), ((), ())), preferred_element_type=jnp.float32
    )


def contract_cols(first_op, second_op):
    return lax.dot_general(
        first_op, second_op, (((1,), (1,)), ((), ())), preferred_element_type=jnp.float32
    )


def segment_ids(lengths, row_count):
    seq_ends = jnp.cumsum(lengths)
    positions = jnp.arange(row_count, dtype=jnp.int32)
    return jnp.sum((positions[:, None] >= seq_ends[None, :]).astype(jnp.int32), axis=1)


def causal_conv(signal, kernel_w, kernel_b, segment):
    kernel_len = kernel_w.shape[0]
    row_count = signal.shape[0]
    summed = kernel_b[None, :] + kernel_w[kernel_len - 1][None, :] * signal
    for lag_steps in range(1, kernel_len):
        shifted = jnp.concatenate(
            [jnp.zeros((lag_steps, signal.shape[1]), jnp.float32), signal[: row_count - lag_steps]],
            axis=0,
        )
        earlier = jnp.concatenate(
            [jnp.full((lag_steps,), -1, jnp.int32), segment[: row_count - lag_steps]]
        )
        same_seq = (earlier == segment).astype(signal.dtype)
        summed = (
            summed + kernel_w[kernel_len - 1 - lag_steps][None, :] * shifted * same_seq[:, None]
        )
    return summed


def mixer_core(z_rows, x_rows, dt_raw, b_conv, c_conv, conv_wx, conv_bx, a_log, dt_bias,
               d_skip, segment=None):
    inner_n = x_rows.shape[1]
    heads_n = a_log.shape[0]
    x_conv = jax.nn.silu(causal_conv(x_rows, conv_wx, conv_bx, segment))
    steps_dt = jax.nn.softplus(dt_raw + dt_bias[None, :])
    decay = steps_dt * (-jnp.exp(a_log))[None, :]
    cum = jnp.cumsum(decay, axis=0)
    scanned = ssd_core(x_conv, steps_dt, cum, b_conv, c_conv, segment)
    skip = jnp.repeat(d_skip, inner_n // heads_n)
    mixed_out = scanned + skip[None, :] * x_conv
    return mixed_out * jax.nn.silu(z_rows)


def bc_core(bc_pre, conv_wbc, conv_bbc, segment=None):
    return jax.nn.silu(causal_conv(bc_pre, conv_wbc, conv_bbc, segment))


def per_device_body(tokens, cotangent, seq_lens, input_norm_gain, w_zx, w_bc, w_dt, conv_wx, conv_bx,
               conv_wbc, conv_bbc, a_log, dt_bias, d_skip, norm_gate, w_out):
    n_dp = lax.axis_size("dp")
    x_full = lax.all_gather(tokens, "tensor", axis=1, tiled=True)
    cot_full = lax.all_gather(cotangent, "tensor", axis=1, tiled=True)
    row_count = tokens.shape[0]
    feat_n = tokens.shape[1]
    d_model = x_full.shape[1]
    feat_start = lax.axis_index("tensor") * feat_n
    state_n = w_bc.shape[1] // 2
    inner_loc = norm_gate.shape[0]
    inner_all = inner_loc * lax.axis_size("tensor")
    segment = segment_ids(seq_lens[0], row_count)
    is_live = (segment < seq_lens.shape[1])[:, None]
    w_zx_flat = w_zx.reshape(d_model, 2 * inner_loc)
    tok_float = x_full.astype(jnp.float32)
    inverse_root_mean = lax.rsqrt(jnp.mean(tok_float * tok_float, axis=1, keepdims=True) + NORM_EPS)
    unit_scaled_input = tok_float * inverse_root_mean
    normed = (unit_scaled_input * input_norm_gain[None, :]).astype(jnp.bfloat16)
    zx_rows = jnp.dot(normed, w_zx_flat, preferred_element_type=jnp.float32)
    bc_pre = jnp.dot(normed, w_bc, preferred_element_type=jnp.float32)
    dt_raw = jnp.dot(normed, w_dt, preferred_element_type=jnp.float32)
    bc_post, bc_back = jax.vjp(partial(bc_core, segment=segment), bc_pre, conv_wbc, conv_bbc)
    gated_rows, core_back = jax.vjp(
        partial(mixer_core, segment=segment),
        zx_rows[:, :inner_loc], zx_rows[:, inner_loc:], dt_raw, bc_post[:, :state_n],
        bc_post[:, state_n:],
        conv_wx, conv_bx, a_log, dt_bias, d_skip,
    )
    cot_live = jnp.where(is_live, cot_full, jnp.zeros_like(cot_full))
    d_gate = contract_cols(cot_live, w_out)
    d_hat = d_gate * norm_gate[None, :]
    stats = doubling_all_reduce(
        jnp.concatenate([jnp.sum(gated_rows * gated_rows, axis=1, keepdims=True),
                         jnp.sum(d_hat * gated_rows, axis=1, keepdims=True)], axis=1),
        "tensor", lax.axis_size("tensor"))
    squares, cross_sum = stats[:, 0:1], stats[:, 1:2]
    r_gate = lax.rsqrt(squares / inner_all + NORM_EPS)
    gate_hat = gated_rows * r_gate
    gate_out = (gate_hat * norm_gate[None, :]).astype(jnp.bfloat16)
    branch_part = jnp.dot(gate_out, w_out, preferred_element_type=jnp.float32)
    grad_gate = jnp.sum(d_gate * gate_hat, axis=0)
    d_gated = r_gate * d_hat - gated_rows * (r_gate * r_gate * r_gate * cross_sum / inner_all)
    d_gated, branch_part = lax.optimization_barrier((d_gated, branch_part))
    branch = lax.psum_scatter(branch_part, "tensor", scatter_dimension=1, tiled=True)
    own_float = tokens.astype(jnp.float32)
    block_out = (own_float + jnp.where(is_live, branch, 0.0)).astype(jnp.bfloat16)
    d_z, d_x, d_dt, d_b, d_c, grad_conv_wx, grad_conv_bx, grad_a_log, grad_dt_bias, grad_d_skip = (
        core_back(d_gated)
    )
    n_tp = lax.axis_size("tensor")
    chunk = d_model // n_dp
    row_major = Layout(major_to_minor=(0, 1))
    d_z_half = d_z.astype(jnp.bfloat16)
    grads_early = with_layout_constraint(jnp.concatenate(
        [with_layout_constraint(contract_rows(cot_live, gate_out), row_major),
         with_layout_constraint(contract_rows(normed, d_z_half), row_major)],
        axis=1), row_major)
    d_x, d_dt, block_out = lax.optimization_barrier((d_x, d_dt, block_out))
    d_zx_half = jnp.concatenate([d_z_half, d_x.astype(jnp.bfloat16)], axis=1)
    d_dt_half = d_dt.astype(jnp.bfloat16)
    early_sum = split_reduce_scatter(grads_early, n_dp)
    grads_x = with_layout_constraint(contract_rows(normed, d_zx_half[:, inner_loc:]), row_major)
    x_sum = split_reduce_scatter(grads_x, n_dp)
    d_bc_part = jnp.concatenate([d_b, d_c], axis=1)
    partial_in = contract_cols(d_zx_half, w_zx_flat) + contract_cols(d_dt_half, w_dt)
    hat_gain = unit_scaled_input * input_norm_gain[None, :]
    row_part = jnp.sum(lax.optimization_barrier(partial_in) * hat_gain, axis=1, keepdims=True)
    d_bc_post = lax.psum(d_bc_part, "tensor")
    row_sum = doubling_all_reduce(row_part, "tensor", n_tp)
    d_bc, grad_conv_wbc, grad_conv_bbc = bc_back(d_bc_post)
    d_bc_half = d_bc.astype(jnp.bfloat16)
    bc_full = contract_cols(d_bc_half, w_bc)
    gin_heads = doubling_all_reduce(
        jnp.sum(lax.optimization_barrier(partial_in) * unit_scaled_input, axis=0),
        "tensor", n_tp)
    gin_sum = doubling_all_reduce(
        gin_heads + jnp.sum(bc_full * unit_scaled_input, axis=0), "dp", n_dp)
    row_inner_product = (row_sum + jnp.sum(bc_full * hat_gain, axis=1, keepdims=True)) / d_model
    smalls = (grad_conv_wx, grad_conv_bx, grad_conv_wbc, grad_conv_bbc, grad_a_log,
              grad_dt_bias, grad_d_skip, grad_gate)
    flat_small = jnp.concatenate([v.reshape(-1) for v in smalls])
    small_cols = -(-flat_small.shape[0] // chunk)
    small_block = jnp.pad(flat_small, (0, small_cols * chunk - flat_small.shape[0])).reshape(
        chunk, small_cols)
    grads_small = with_layout_constraint(jnp.concatenate(
        [with_layout_constraint(
            contract_rows(normed, jnp.concatenate([d_bc_half, d_dt_half], axis=1)), row_major),
         jnp.tile(small_block, (n_dp, 1))], axis=1), row_major)
    small_sum_all = halving_reduce_scatter(grads_small, n_dp)
    own_part = lax.psum_scatter(partial_in, "tensor", scatter_dimension=1, tiled=True)
    own_hat = lax.dynamic_slice_in_dim(unit_scaled_input, feat_start, feat_n, 1)
    own_gain = lax.dynamic_slice_in_dim(input_norm_gain, feat_start, feat_n, 0)
    own_dn = own_part + lax.dynamic_slice_in_dim(bc_full, feat_start, feat_n, 1)
    own_dxhat = own_dn * own_gain[None, :]
    grad_in = lax.dynamic_slice_in_dim(gin_sum, feat_start, feat_n, 0)
    d_tokens = cotangent.astype(jnp.float32) + inverse_root_mean * (
        own_dxhat - own_hat * row_inner_product
    )
    grad_out_t_sum = early_sum[:, :inner_loc]
    grad_zx_sum = jnp.concatenate([early_sum[:, inner_loc:], x_sum], axis=1)
    grad_bc_sum = small_sum_all[:, :2 * state_n]
    grad_dt_sum = small_sum_all[:, 2 * state_n:2 * state_n + w_dt.shape[1]]
    small_sum = small_sum_all[:, 2 * state_n + w_dt.shape[1]:].reshape(-1)
    outs_small = []
    pos = 0
    for v in smalls:
        outs_small.append(small_sum[pos:pos + v.size].reshape(v.shape))
        pos += v.size
    grad_zx_out = grad_zx_sum.reshape(chunk, 2, inner_loc)
    return (block_out, d_tokens, grad_zx_out, grad_bc_sum, grad_dt_sum, grad_out_t_sum.T,
            *outs_small, grad_in)


def halving_reduce_scatter(x, n_dev, order=None):
    me = lax.axis_index("dp")
    bits = n_dev.bit_length() - 1
    chunk = x.shape[0] // n_dev
    cur = x.reshape((2,) * bits + (chunk, x.shape[1]))
    axes = list(range(bits - 1, -1, -1))
    for bit in (order if order is not None else range(bits)):
        pos = axes.index(bit)
        mine = (me >> bit) & 1
        keep = lax.dynamic_index_in_dim(cur, mine, axis=pos, keepdims=False)
        send = lax.dynamic_index_in_dim(cur, 1 - mine, axis=pos, keepdims=False)
        got = lax.ppermute(send, "dp", [(i, i ^ (1 << bit)) for i in range(n_dev)])
        cur = keep + got
        axes.pop(pos)
    return cur.reshape(chunk, x.shape[1])


def doubling_all_reduce(x, axis, n_dev):
    bit = 0
    while (1 << bit) < n_dev:
        x = x + lax.ppermute(x, axis, [(i, i ^ (1 << bit)) for i in range(n_dev)])
        bit += 1
    return x


def split_reduce_scatter(x, n_dev):
    bits = n_dev.bit_length() - 1
    half = x.shape[1] // 2
    first = tuple(range(bits))
    second = (0,) + tuple(range(bits - 1, 0, -1))
    return jnp.concatenate([halving_reduce_scatter(x[:, :half], n_dev, first),
                            halving_reduce_scatter(x[:, half:], n_dev, second)], axis=1)


def solution(mesh):
    in_specs = (
        P("dp", "tensor"), P("dp", "tensor"), P("dp", None), P(),
        P(None, None, "tensor"), P(), P(None, "tensor"), P(None, "tensor"), P("tensor"),
        P(), P(), P("tensor"), P("tensor"), P("tensor"), P("tensor"), P("tensor", None),
    )
    out_specs = (
        P("dp", "tensor"), P("dp", "tensor"), P("dp", None, "tensor"), P("dp", None),
        P("dp", "tensor"), P("tensor", "dp"), P(None, "tensor"), P("tensor"), P(), P(),
        P("tensor"), P("tensor"), P("tensor"), P("tensor"), P("tensor"),
    )
    return jax.shard_map(
        per_device_body, mesh=mesh, in_specs=in_specs, out_specs=out_specs, check_vma=False
    )
```
